32 devices in a mesh: grp: 4 (over z), slab: 8 (over y, x, core).
Axes of the slice: x: 2, y: 2, z: 4, core: 2. Of those that a mesh axis runs over, the one named last changes fastest.
Arguments:
- orbitals: float32 [8, 96, 9216], P('grp', 'slab'), may hold values from -6 to 6
- occupation: int32 [8], P('grp'), may hold values from 1 to 4
- kernel_hat: float32 [192, 36864], P('slab'), may hold values from 0.02 to 1200, as said below
- pair_mask: int32 [1], replicated, may hold values from 1 to 3
Outputs:
- exchange_terms: float32 [8, 96, 9216], P('grp', 'slab')
The draws below stay inside these ranges and needn't reach their ends.
Inputs may be any that keep to these rules, and one draw needn't show every extreme that they name: In this round group g is paired with group g XOR pair_mask. kernel_hat is positive, and unchanged when each frequency index k is replaced by (192 - k) mod 192 in all three dimensions at once.
All inputs are finite; a program needn't handle non-finite values.
Results may differ from the reference program's by a relative error of at most 0.0001.
Values sent between devices are 32-bit elements; how exact they have to be, the bound alone decides.
A program may use at most 64 MiB of HBM per device.

```python
import math
import jax
import jax.numpy as jnp
from jax import lax

G = 96
P_SIZE = 192
ORBS = 2
ORBITALS = 8
N_GRP = 4


screening = 0.0025


def draw_kernel_hat(key, part):
    factors = jax.random.uniform(key, (P_SIZE, P_SIZE, P_SIZE), jnp.float32, 0.5, 1.5)
    mirrored = jnp.roll(jnp.flip(factors, (0, 1, 2)), 1, (0, 1, 2))
    even_factors = 0.5 * (factors + mirrored)
    wave_index = jnp.arange(P_SIZE, dtype=jnp.int32)
    folded = jnp.minimum(wave_index, P_SIZE - wave_index).astype(jnp.float32)
    eigen_line = 4.0 * jnp.sin(math.pi * folded / P_SIZE) ** 2
    eigen_sum = eigen_line[:, None, None] + eigen_line[None, :, None] + eigen_line[None, None, :]
    return (even_factors / (eigen_sum + screening)).reshape(P_SIZE, P_SIZE * P_SIZE)


def plant(entries, own_key, smallest, largest):
    spot = [jax.random.randint(jax.random.fold_in(own_key, axis), (), 0, length) for axis, length in enumerate(entries.shape)]
    main_axis = entries.shape.index(max(entries.shape))
    neighbour = spot[:main_axis] + [(spot[main_axis] + 1) % entries.shape[main_axis]] + spot[main_axis + 1:]
    return entries.at[tuple(spot)].set(smallest).at[tuple(neighbour)].set(largest)


def shard_levels(rng, dims, split, least, top_value):
    def one(position, blocks):
        steps = jax.random.uniform(jax.random.fold_in(jax.random.fold_in(rng, 6), position), (blocks,), jnp.float32, least / len(split), top_value / len(split))
        return jnp.repeat(jnp.exp(steps), dims[position] // blocks).reshape((-1,) + (1,) * (len(dims) - position - 1))

    loudness = one(*split[0])
    for cut in split[1:]:
        loudness = loudness * one(*cut)
    return loudness


def scatter_about(rng, dims, scale, reach, cuts=(), kind=jnp.bfloat16):
    level = shard_levels(rng, dims, cuts, -0.22, 0.18) if cuts else 1.0
    array = jax.random.normal(rng, dims, jnp.float32) * scale * level
    return jnp.minimum(jnp.maximum(array, -reach), reach).astype(kind)


def setup_inputs(seed: int = 0) -> dict:
    key_of = jax.random.split(jax.random.key(seed), 5)
    return {
        "orbitals": scatter_about(key_of[0], (ORBITALS, G, G * G), 1.0, 6.0, ((0, 4), (1, 8)), jnp.float32),
        "occupation": plant(jax.random.randint(key_of[1], (ORBITALS,), 1, 5), jax.random.fold_in(key_of[1], 1), 1, 4).astype(jnp.int32),
        "kernel_hat": draw_kernel_hat(jax.random.fold_in(key_of[4], 71), 0),
        "pair_mask": jax.random.randint(key_of[3], (1,), 1, N_GRP).astype(jnp.int32),
    }


def pair_potential(density, kernel_half):
    padded = jnp.pad(density, ((0, G), (0, G), (0, G)))
    spectrum = jnp.fft.rfftn(padded)
    field = jnp.fft.irfftn(spectrum * kernel_half, s=(P_SIZE, P_SIZE, P_SIZE))
    return field[:G, :G, :G]


def reference(orbitals, occupation, kernel_hat, pair_mask):
    fields = orbitals.reshape(N_GRP, ORBS, G, G, G)
    weights = (0.25 * occupation.astype(jnp.float32)).reshape(N_GRP, ORBS)
    kernel_cube = kernel_hat.reshape(P_SIZE, P_SIZE, P_SIZE)
    kernel_half = jnp.transpose(kernel_cube, (2, 1, 0))[:, :, : P_SIZE // 2 + 1]
    pair_bits = pair_mask[0].astype(jnp.int32)
    high_bit = jnp.zeros((), jnp.int32)
    for shift_level in range(1, 31):
        high_bit = high_bit + (jnp.right_shift(pair_bits, shift_level) > 0).astype(jnp.int32)
    low_bits = jnp.left_shift(jnp.ones((), jnp.int32), high_bit) - 1

    def pair_step(flat_index, sums):
        flat_index = flat_index.astype(jnp.int32)
        pair_index = flat_index // (ORBS * ORBS)
        first = (flat_index // ORBS) % ORBS
        second = flat_index % ORBS
        lower_group = jnp.bitwise_or(
            jnp.left_shift(jnp.right_shift(pair_index, high_bit), high_bit + 1),
            jnp.bitwise_and(pair_index, low_bits))
        upper_group = jnp.bitwise_xor(lower_group, pair_bits)
        left_field = fields[lower_group, first]
        right_field = fields[upper_group, second]
        potential = pair_potential(left_field * right_field, kernel_half)
        sums = sums.at[lower_group, first].add(-weights[upper_group, second] * potential * right_field)
        sums = sums.at[upper_group, second].add(-weights[lower_group, first] * potential * left_field)
        return sums

    total_pairs = (N_GRP // 2) * ORBS * ORBS
    sums = lax.fori_loop(0, total_pairs, pair_step, jnp.zeros((N_GRP, ORBS, G, G, G), jnp.float32))
    return sums.reshape(N_GRP * ORBS, G, G * G)
```

```python
import math

import jax
import jax.numpy as jnp
import ml_dtypes
import numpy as np
from jax import lax
from jax.experimental import pallas as pl
from jax.experimental.pallas import tpu as pltpu
from jax.sharding import PartitionSpec as P

LANE = 128
SUB = 8
F32 = jnp.float32


def halves(table):
    high = table.astype(np.float32).astype(ml_dtypes.bfloat16)
    low = (table - high.astype(np.float64)).astype(ml_dtypes.bfloat16)
    return np.stack([high, low])


def padded(size, unit):
    return -(-size // unit) * unit


class Plan:
    def __init__(self, planes, plane_cells, slabs, freqs):
        self.planes, self.slabs, self.freqs = planes, slabs, freqs
        self.grid = math.isqrt(plane_cells)
        self.period = 2 * self.grid
        self.group = math.lcm(self.grid, LANE)
        self.fold = self.group // self.grid
        self.quads = self.grid // self.fold
        self.tiles = self.group // LANE
        self.rows = planes * self.quads
        self.chunks = -(-planes // self.fold)
        self.wide = padded(self.period, LANE)
        self.lanes = self.fold * self.period
        self.parts = -(-freqs // SUB)
        self.columns = padded(self.parts * slabs * SUB, LANE)
        self.line_rows = planes * 2 * slabs * SUB
        self.cell_starts = self.windows(self.grid, self.group)
        self.pair_starts = self.windows(self.period, self.lanes)
        assert self.period % LANE == LANE // 2 and LANE % (slabs * SUB) == 0

    def windows(self, step, lanes):
        return [min(j * step // LANE * LANE, lanes - self.wide) for j in range(self.fold)]

    def sizes(self, chunk):
        return min(self.fold, self.planes - chunk * self.fold)

    def wave(self, left, right):
        angle = 2.0 * math.pi / self.period * (np.outer(left, right) % self.period)
        return np.cos(angle), np.sin(angle)

    def tables(self):
        grid, period, fold, wide = self.grid, self.period, self.fold, self.wide
        columns = self.columns
        freq = np.zeros(columns, int)
        live = np.zeros(columns, bool)
        for n in range(self.parts * self.slabs * SUB):
            part, rest = divmod(n, self.slabs * SUB)
            own = part * SUB + rest % SUB
            freq[n] = rest // SUB * self.freqs + own
            live[n] = own < self.freqs
        cells = np.arange(grid)
        zc, zs = self.wave(cells, np.where(live, freq, 0))
        zc, zs = zc * live, zs * live
        offsets = [j * grid - self.cell_starts[j] for j in range(fold)]
        reach = max(offsets)
        self.cell_slides = [reach - offset for offset in offsets]
        zf = np.zeros((2, reach + wide, 2 * columns))
        at = slice(reach, reach + grid)
        zf[0, at, :columns], zf[0, at, columns:] = zc, -zs
        zf[1, at, :columns], zf[1, at, columns:] = zs, zc
        zi = np.zeros((fold, 2 * columns, 2 * wide))
        for j in range(fold):
            first, second = offsets[j], wide + offsets[j]
            zi[j, :columns, first : first + grid] = zc.T / period
            zi[j, columns:, first : first + grid] = -zs.T / period
            zi[j, :columns, second : second + grid] = zs.T / period
            zi[j, columns:, second : second + grid] = zc.T / period
        y_order = np.array([fold * q + j for j in range(fold) for q in range(self.quads)])
        ky_order = np.concatenate([np.arange(0, period, 2), np.arange(1, period, 2)])
        yc, ys = self.wave(y_order, ky_order)
        offsets = [j * period - self.pair_starts[j] for j in range(fold)]
        reach = max(offsets)
        self.pair_slides = [reach - offset for offset in offsets]
        self.pair_kinds = sorted(set(offsets))
        self.pair_kind = [self.pair_kinds.index(offset) for offset in offsets]
        yf = np.zeros((reach + wide, 2 * wide))
        re, im = slice(reach, reach + grid), slice(reach + grid, reach + period)
        yf[re, :period], yf[re, wide : wide + period] = yc, -ys
        yf[im, :period], yf[im, wide : wide + period] = ys, yc
        yi = np.zeros((len(self.pair_kinds), 2 * wide, wide))
        for n, offset in enumerate(self.pair_kinds):
            re, im = slice(offset, offset + grid), slice(offset + grid, offset + period)
            yi[n, :period, re], yi[n, :period, im] = yc.T / period, ys.T / period
            yi[n, wide : wide + period, re] = -ys.T / period
            yi[n, wide : wide + period, im] = yc.T / period
        row = [
            (c, s * self.planes + x)
            for x in range(self.planes)
            for c in range(2)
            for s in range(self.slabs)
        ]
        side = np.array([r[0] for r in row])
        cos, sin = self.wave(np.arange(period), np.array([r[1] for r in row]))
        xf = np.concatenate([np.where(side == 0, cos, sin), np.where(side == 0, -sin, cos)])
        xi = np.concatenate([np.where(side == 0, cos, sin), np.where(side == 0, -sin, cos)])
        return {
            "zf": halves(zf),
            "zi": halves(zi),
            "yf": halves(yf),
            "yi": halves(yi),
            "xf": halves(xf),
            "xi": halves(xi.T / period),
        }


def mm(left, right):
    return jnp.dot(left, right, preferred_element_type=F32)


def split(value):
    high = value.astype(jnp.bfloat16)
    low = (value - high.astype(F32)).astype(jnp.bfloat16)
    return high, low


def right_mul(value, high, low):
    vh, vl = value
    return mm(vh, high) + mm(vh, low) + mm(vl, high)


def left_mul(high, low, value):
    vh, vl = value
    return mm(high, vh) + mm(low, vh) + mm(high, vl)


NAMES = ("zf", "yf", "xf", "xi", "yi", "zi")


def core(plan, mask, *refs):
    occ_ref, orb_hbm, kern_hbm, *table_hbm = refs[:9]
    out_ref = refs[9]
    raw, flat, zf, yf, xf, xi, yi, zi = refs[10:18]
    bank, terms, back, cube, turned, going, coming, leaving, landing, lines = refs[18:28]
    load_sem, zs, zr, fs, fr, bs, br, rs, rr = refs[28:]
    slabs, parts, planes, period = plan.slabs, plan.parts, plan.planes, plan.period
    grid, quads, fold, wide, tiles = plan.grid, plan.quads, plan.fold, plan.wide, plan.tiles
    columns = plan.columns

    loads = [
        pltpu.make_async_copy(source, dest, load_sem.at[n])
        for n, (source, dest) in enumerate(
            zip([orb_hbm, kern_hbm, *table_hbm], [raw, flat, zf, yf, xf, xi, yi, zi])
        )
    ]
    for load in loads:
        load.start()

    me = lax.axis_index("slab")
    g = lax.axis_index("grp")
    top = 1 << (mask.bit_length() - 1)
    quad = mask % 2 == 0
    owner = (g % 2) == ((g // top) % 2 if quad else 0)
    helper = jnp.logical_not(owner)
    mate = 1 if quad else mask
    steps = sorted(range(1, slabs), key=lambda step: -step)
    others = sorted({mate, mask, mask ^ 1} if quad else {mask})
    barrier = pltpu.get_barrier_semaphore()
    mesh_id = pl.DeviceIdType.MESH
    for other in others:
        pl.semaphore_signal(barrier, 1, device_id={"grp": g ^ other}, device_id_type=mesh_id)
    for step in steps:
        pl.semaphore_signal(barrier, 1, device_id={"slab": me ^ step}, device_id_type=mesh_id)

    def hop(source, dest, send_sem, recv_sem, other):
        return pltpu.make_async_remote_copy(
            src_ref=source,
            dst_ref=dest,
            send_sem=send_sem,
            recv_sem=recv_sem,
            device_id={"grp": g ^ other},
            device_id_type=mesh_id,
        )

    def block(chunk):
        return slice(chunk * fold * quads, (chunk * fold + plan.sizes(chunk)) * quads)

    def ahead(chunk, source, slot, other):
        at = block(chunk)
        n = slot - 2
        return hop(
            bank.at[source, at], bank.at[slot, at], zs.at[source, chunk], zr.at[n, chunk], other
        )

    def answer(chunk, source, slot, other):
        at = block(chunk)
        return hop(
            terms.at[source, at], back.at[slot, at], rs.at[source, chunk], rr.at[slot, chunk], other
        )

    def sends_ahead(chunk):
        mine = [ahead(chunk, 0, 2, mate), ahead(chunk, 1, 3, mate)]
        theirs = [ahead(chunk, 0, 4, mask)] + ([ahead(chunk, 1, 4, mask ^ 1)] if quad else [])
        return mine, theirs

    def sends_back(chunk):
        mine = [answer(chunk, 2, 0, mask)]
        theirs = [answer(chunk, 0, 0, mate), answer(chunk, 1, 1, mate)]
        return mine, theirs + ([answer(chunk, 2, 1, mask ^ 1)] if quad else [])

    def both(pair, act):
        for role, copies in zip((owner, helper), pair):

            @pl.when(role)
            def _(copies=copies):
                for copy in copies:
                    act(copy)

    def spread(way, chunk, step, arriving):
        source, dest, ss, sr = ((going, coming, fs, fr), (leaving, landing, bs, br))[way]
        peer = me ^ step
        return pltpu.make_async_remote_copy(
            src_ref=source.at[chunk, :, peer],
            dst_ref=dest.at[chunk, :, peer if arriving else me],
            send_sem=ss.at[chunk, step],
            recv_sem=sr.at[chunk, step],
            device_id={"slab": peer},
            device_id_type=mesh_id,
        )

    def spread_out(way, chunk):
        for step in steps:
            spread(way, chunk, step, False).start()
        source, dest = ((going, coming), (leaving, landing))[way]
        dest[chunk, :, pl.ds(me, 1)] = source[chunk, :, pl.ds(me, 1)]

    def spread_in(way, chunk):
        for step in steps:
            spread(way, chunk, step, True).wait_recv()

    scale = [jnp.sqrt(0.25 * jnp.full((1, LANE), occ_ref[i], jnp.int32).astype(F32)) for i in range(2)]

    def cells(ref, x, i, r):
        return pl.ds((x * quads * tiles + r) * 2 + i, quads, stride=2 * tiles)

    loads[0].wait()
    for chunk in range(plan.chunks):
        for x in range(chunk * fold, chunk * fold + plan.sizes(chunk)):
            for i in range(2):
                for r in range(tiles):
                    bank[i, x * quads : (x + 1) * quads, r * LANE : (r + 1) * LANE] = (
                        raw[cells(raw, x, i, r), :] * scale[i]
                    )
        if chunk == 0:
            pl.semaphore_wait(barrier, len(others) + len(steps))
        both(sends_ahead(chunk), lambda copy: copy.start())

    loads[1].wait()
    pairs = period // 2
    per = 2 * period // LANE
    if plan.freqs % SUB == 0:
        unit = SUB
        plane_start = lambda k: k // SUB * (period * period // LANE * SUB) + k % SUB
    else:
        unit = plan.freqs
        plane_start = lambda k: k

    def one_cube(k, carry):
        first = plane_start(k)
        got = [flat[pl.ds(first + m * unit, pairs, stride=per * unit), :] for m in range(per)]
        n = per // 2
        swapped = [pltpu.roll(v, LANE // 2, 1) for v in got[n:]]
        lane = lax.broadcasted_iota(jnp.int32, (pairs, LANE), 1)
        spare = jnp.zeros((wide - period, LANE), F32)
        for t in range(n + 1):
            odd = swapped[t]
            if t < n:
                odd = jnp.where(lane < LANE // 2, odd, swapped[t + 1])
            rows = jnp.concatenate([got[t], odd, spare], axis=0).T
            depth = min(LANE, period - t * LANE)
            cube[k, t * LANE : t * LANE + depth, :] = rows[:depth]
        return carry

    lax.fori_loop(0, plan.freqs, one_cube, 0)

    left = [jnp.where(owner, i, 2 + i) for i in range(2)]
    right = jnp.where(owner, 4, 4 if quad else 1)
    for load in loads[2:]:
        load.wait()

    for chunk in range(plan.chunks):
        heard = ([ahead(chunk, 0, 4, mask)], [ahead(chunk, 0, 2, mate), ahead(chunk, 1, 3, mate)])
        if quad:
            heard[1].append(ahead(chunk, 1, 4, mask ^ 1))
        both(heard, lambda copy: copy.wait_recv())
        at, count = block(chunk), plan.sizes(chunk)
        partner = bank[right, at]
        pieces = [split(bank[left[i], at] * partner) for i in range(2)]
        if count < fold:
            turned[count * period :, :] = jnp.zeros(((fold - count) * period, columns), F32)
        for j in range(fold):
            lane = slice(plan.cell_starts[j], plan.cell_starts[j] + wide)
            rows = slice(plan.cell_slides[j], plan.cell_slides[j] + wide)
            total = None
            for i in range(2):
                piece = tuple(part[:, lane] for part in pieces[i])
                term = right_mul(piece, zf[0, i, rows], zf[1, i, rows])
                total = term if total is None else total + term
            for x in range(count):
                for c in range(2):
                    first = x * period + c * grid + j * quads
                    turned[first : first + quads, :] = total[
                        x * quads : (x + 1) * quads, c * columns : (c + 1) * columns
                    ]
        share = LANE // (slabs * SUB)
        for col in range(0, columns, LANE):
            for r in range(0, plan.lanes, LANE):
                flip = turned[r : r + LANE, col : col + LANE].T.reshape(share, slabs, SUB, LANE)
                for n in range(min(share, parts - col // LANE * share)):
                    going[chunk, col // LANE * share + n, :, :, r : r + LANE] = flip[n]
        spread_out(0, chunk)

    many = parts * slabs * SUB
    for chunk in range(plan.chunks):
        spread_in(0, chunk)
        for j in range(plan.sizes(chunk)):
            x = chunk * fold + j
            lane = slice(plan.pair_starts[j], plan.pair_starts[j] + wide)
            rows = slice(plan.pair_slides[j], plan.pair_slides[j] + wide)
            piece = split(coming[chunk, :, :, :, lane].reshape(many, wide))
            field = right_mul(piece, yf[0, rows], yf[1, rows])
            for part in range(parts):
                own = slice(part * slabs * SUB, (part + 1) * slabs * SUB)
                for c in range(2):
                    first = ((part * planes + x) * 2 + c) * slabs * SUB
                    for t in range(wide // LANE):
                        spot = c * wide + t * LANE
                        lines[t, first : first + slabs * SUB, :] = field[own, spot : spot + LANE]

    def one_plane(part, k):
        rows = pl.ds(part * plan.line_rows + k, planes * 2 * slabs, stride=SUB)
        field = jnp.concatenate([lines[t, rows, :] for t in range(wide // LANE)], axis=1)
        spectra = left_mul(xf[0], xf[1], split(field))
        kernel = cube[part * SUB + k]
        spectra = jnp.concatenate(
            [spectra[:period] * kernel, spectra[period:] * kernel], axis=0
        )
        field = left_mul(xi[0], xi[1], split(spectra))
        for t in range(wide // LANE):
            lines[t, rows, :] = field[:, t * LANE : (t + 1) * LANE]

    step_by = 2 if plan.freqs % 2 == 0 else 1

    def some_planes(n, carry):
        for k in range(step_by):
            at = n * step_by + k
            one_plane(at // SUB, at % SUB)
        return carry

    lax.fori_loop(0, plan.freqs // step_by, some_planes, 0)

    for chunk in range(plan.chunks):
        total = [None] * (plan.lanes // LANE)
        for j in range(plan.sizes(chunk)):
            x = chunk * fold + j
            kind = plan.pair_kind[j]
            field = []
            for part in range(parts):
                field.append([])
                for c in range(2):
                    first = ((part * planes + x) * 2 + c) * slabs * SUB
                    for t in range(wide // LANE):
                        field[-1].append(lines[t, first : first + slabs * SUB, :])
            field = jnp.concatenate([jnp.concatenate(f, axis=1) for f in field], axis=0)
            field = right_mul(split(field), yi[0, kind], yi[1, kind])
            for t in range(wide // LANE):
                spot = plan.pair_starts[j] // LANE + t
                term = field[:, t * LANE : (t + 1) * LANE]
                total[spot] = term if total[spot] is None else total[spot] + term
        for t, term in enumerate(total):
            if term is None:
                term = jnp.zeros((many, LANE), F32)
            leaving[chunk, :, :, :, t * LANE : (t + 1) * LANE] = term.reshape(
                parts, slabs, SUB, LANE
            )
        spread_out(1, chunk)

    for chunk in range(plan.chunks):
        spread_in(1, chunk)
        at, count = block(chunk), plan.sizes(chunk)
        share = LANE // (slabs * SUB)
        for col in range(0, columns, LANE):
            for r in range(0, plan.lanes, LANE):
                got = []
                for n in range(share):
                    part = col // LANE * share + n
                    if part < parts:
                        one = landing[chunk, part, :, :, r : r + LANE].reshape(slabs * SUB, LANE)
                    else:
                        one = jnp.zeros((slabs * SUB, LANE), F32)
                    got.append(one)
                got = jnp.concatenate(got, axis=0) if share > 1 else got[0]
                turned[r : r + LANE, col : col + LANE] = got.T
        total = [[None] * tiles for _ in range(2)]
        for j in range(fold):
            rows = []
            for x in range(count):
                firsts = [x * period + c * grid + j * quads for c in range(2)]
                rows.append(
                    jnp.concatenate([turned[f : f + quads, :] for f in firsts], axis=1)
                )
            rows = jnp.concatenate(rows, axis=0)
            field = right_mul(split(rows), zi[0, j], zi[1, j])
            for i in range(2):
                for t in range(wide // LANE):
                    spot = plan.cell_starts[j] // LANE + t
                    first = i * wide + t * LANE
                    term = field[:, first : first + LANE]
                    known = total[i][spot]
                    total[i][spot] = term if known is None else known + term
        far = None
        partner = bank[right, at]
        for i in range(2):
            field = jnp.concatenate(total[i], axis=1)
            terms[i, at] = field * partner
            term = field * bank[left[i], at]
            far = term if far is None else far + term
        terms[2, at] = far
        both(sends_back(chunk), lambda copy: copy.start())

    weight = [-1.0 / s for s in scale]
    for chunk in range(plan.chunks):
        heard = ([answer(chunk, 0, 0, mate), answer(chunk, 1, 1, mate)], [answer(chunk, 2, 0, mask)])
        if quad:
            heard[1].append(answer(chunk, 2, 1, mask ^ 1))
        both(heard, lambda copy: copy.wait_recv())

        def put(i, value, chunk=chunk):
            for x in range(plan.sizes(chunk)):
                for r in range(tiles):
                    out_ref[cells(out_ref, chunk * fold + x, i, r), :] = (
                        value[x * quads : (x + 1) * quads, r * LANE : (r + 1) * LANE] * weight[i]
                    )

        @pl.when(owner)
        def _(chunk=chunk, put=put):
            for i in range(2):
                put(i, terms[i, block(chunk)] + back[i, block(chunk)])

        @pl.when(helper)
        def _(chunk=chunk, put=put):
            put(0, back[0, block(chunk)])
            put(1, back[1, block(chunk)] if quad else terms[2, block(chunk)])

    for chunk in range(plan.chunks):
        both(sends_ahead(chunk), lambda copy: copy.wait_send())
        both(sends_back(chunk), lambda copy: copy.wait_send())
        for way in range(2):
            for step in steps:
                spread(way, chunk, step, False).wait_send()


def run_core(plan, mask, occupation, orbitals, kernel, tables):
    operands = [orbitals, kernel] + [tables[name] for name in NAMES]
    out = jax.ShapeDtypeStruct(orbitals.shape, F32)
    wire = pltpu.VMEM((plan.chunks, plan.parts, plan.slabs, SUB, plan.lanes), F32)
    dma = pltpu.SemaphoreType.DMA
    return pl.pallas_call(
        lambda *refs: core(plan, mask, *refs),
        out_shape=out,
        in_specs=[pl.BlockSpec(memory_space=pltpu.SMEM)]
        + [pl.BlockSpec(memory_space=pl.ANY)] * len(operands),
        out_specs=pl.BlockSpec(memory_space=pltpu.VMEM),
        scratch_shapes=[pltpu.VMEM(op.shape, op.dtype) for op in operands]
        + [
            pltpu.VMEM((5, plan.rows, plan.group), F32),
            pltpu.VMEM((3, plan.rows, plan.group), F32),
            pltpu.VMEM((2, plan.rows, plan.group), F32),
            pltpu.VMEM((plan.freqs, plan.period, plan.wide), F32),
            pltpu.VMEM((plan.lanes, plan.columns), F32),
            wire,
            wire,
            wire,
            wire,
            pltpu.VMEM((plan.wide // LANE, plan.parts * plan.line_rows, LANE), F32),
            dma((len(operands),)),
            dma((2, plan.chunks)),
            dma((3, plan.chunks)),
        ]
        + [dma((plan.chunks, plan.slabs))] * 4
        + [dma((3, plan.chunks)), dma((2, plan.chunks))],
        compiler_params=pltpu.CompilerParams(
            collective_id=mask, has_side_effects=True, vmem_limit_bytes=62 * 2**20
        ),
    )(occupation, *operands)


def local(orbitals, occupation, kernel_hat, pair_mask):
    orbit_count, planes, plane_cells = orbitals.shape
    assert orbit_count == 2 and plane_cells % LANE == 0
    slabs = lax.axis_size("slab")
    groups = lax.axis_size("grp")
    freqs, columns = kernel_hat.shape
    plan = Plan(planes, plane_cells, slabs, freqs)
    tables = {name: jnp.asarray(t) for name, t in plan.tables().items()}
    tiles = plane_cells // LANE
    flat = orbitals.reshape(2, planes, tiles, LANE).transpose(1, 2, 0, 3).reshape(-1, LANE)
    if freqs % SUB == 0:
        kernel = kernel_hat.reshape(freqs // SUB, SUB, columns // LANE, LANE)
        kernel = kernel.transpose(0, 2, 1, 3).reshape(-1, LANE)
    else:
        kernel = kernel_hat.reshape(freqs, columns // LANE, LANE)
        kernel = kernel.transpose(1, 0, 2).reshape(-1, LANE)

    def branch(mask):
        return lambda *args: run_core(plan, mask, *args, tables)

    branches = [branch(mask) for mask in range(1, groups)]
    out = lax.switch(pair_mask[0] - 1, branches, occupation, flat, kernel)
    return out.reshape(planes, tiles, 2, LANE).transpose(2, 0, 1, 3).reshape(2, planes, plane_cells)


def solution(mesh):
    return jax.shard_map(
        local,
        mesh=mesh,
        in_specs=(P("grp", "slab", None), P("grp"), P("slab", None), P()),
        out_specs=P("grp", "slab", None),
        check_vma=False,
    )
```

```python
import math

import jax
import jax.numpy as jnp
import ml_dtypes
import numpy as np
from jax import lax
from jax.experimental import pallas as pl
from jax.experimental.pallas import tpu as pltpu
from jax.sharding import PartitionSpec as P

LANE = 128
SUB = 8
F32 = jnp.float32


def halves(table):
    high = table.astype(np.float32).astype(ml_dtypes.bfloat16)
    low = (table - high.astype(np.float64)).astype(ml_dtypes.bfloat16)
    return np.stack([high, low])


def padded(size, unit):
    return -(-size // unit) * unit


class Plan:
    def __init__(self, planes, plane_cells, slabs, freqs):
        self.planes, self.slabs, self.freqs = planes, slabs, freqs
        self.grid = math.isqrt(plane_cells)
        self.period = 2 * self.grid
        self.group = math.lcm(self.grid, LANE)
        self.fold = self.group // self.grid
        self.quads = self.grid // self.fold
        self.tiles = self.group // LANE
        self.rows = planes * self.quads
        self.chunks = -(-planes // self.fold)
        self.wide = padded(self.period, LANE)
        self.lanes = self.fold * self.period
        self.parts = -(-freqs // SUB)
        self.columns = padded(self.parts * slabs * SUB, LANE)
        self.line_rows = planes * 2 * slabs * SUB
        self.cell_starts = self.windows(self.grid, self.group)
        self.pair_starts = self.windows(self.period, self.lanes)
        assert self.period % LANE == LANE // 2 and LANE % (slabs * SUB) == 0

    def windows(self, step, lanes):
        return [min(j * step // LANE * LANE, lanes - self.wide) for j in range(self.fold)]

    def sizes(self, chunk):
        return self.fold if self.planes % self.fold == 0 else min(self.fold, self.planes - chunk * self.fold)

    def wave(self, left, right):
        angle = 2.0 * math.pi / self.period * (np.outer(left, right) % self.period)
        return np.cos(angle), np.sin(angle)

    def tables(self):
        grid, period, fold, wide = self.grid, self.period, self.fold, self.wide
        columns = self.columns
        freq = np.zeros(columns, int)
        live = np.zeros(columns, bool)
        for n in range(self.parts * self.slabs * SUB):
            part, rest = divmod(n, self.slabs * SUB)
            own = part * SUB + rest % SUB
            freq[n] = rest // SUB * self.freqs + own
            live[n] = own < self.freqs
        cells = np.arange(grid)
        zc, zs = self.wave(cells, np.where(live, freq, 0))
        zc, zs = zc * live, zs * live
        offsets = [j * grid - self.cell_starts[j] for j in range(fold)]
        reach = max(offsets)
        self.cell_slides = [reach - offset for offset in offsets]
        zf = np.zeros((2, reach + wide, 2 * columns))
        at = slice(reach, reach + grid)
        zf[0, at, :columns], zf[0, at, columns:] = zc, -zs
        zf[1, at, :columns], zf[1, at, columns:] = zs, zc
        zi = np.zeros((fold, 2 * columns, 2 * wide))
        for j in range(fold):
            first, second = offsets[j], wide + offsets[j]
            zi[j, :columns, first : first + grid] = zc.T / period
            zi[j, columns:, first : first + grid] = -zs.T / period
            zi[j, :columns, second : second + grid] = zs.T / period
            zi[j, columns:, second : second + grid] = zc.T / period
        y_order = np.array([fold * q + j for j in range(fold) for q in range(self.quads)])
        ky_order = np.concatenate([np.arange(0, period, 2), np.arange(1, period, 2)])
        yc, ys = self.wave(y_order, ky_order)
        offsets = [j * period - self.pair_starts[j] for j in range(fold)]
        reach = max(offsets)
        self.pair_slides = [reach - offset for offset in offsets]
        self.pair_kinds = sorted(set(offsets))
        self.pair_kind = [self.pair_kinds.index(offset) for offset in offsets]
        yf = np.zeros((reach + wide, 2 * wide))
        re, im = slice(reach, reach + grid), slice(reach + grid, reach + period)
        yf[re, :period], yf[re, wide : wide + period] = yc, -ys
        yf[im, :period], yf[im, wide : wide + period] = ys, yc
        yi = np.zeros((len(self.pair_kinds), 2 * wide, wide))
        for n, offset in enumerate(self.pair_kinds):
            re, im = slice(offset, offset + grid), slice(offset + grid, offset + period)
            yi[n, :period, re], yi[n, :period, im] = yc.T / period, ys.T / period
            yi[n, wide : wide + period, re] = -ys.T / period
            yi[n, wide : wide + period, im] = yc.T / period
        row = [
            (c, s * self.planes + x)
            for x in range(self.planes)
            for c in range(2)
            for s in range(self.slabs)
        ]
        side = np.array([r[0] for r in row])
        cos, sin = self.wave(np.arange(period), np.array([r[1] for r in row]))
        xf = np.concatenate([np.where(side == 0, cos, sin), np.where(side == 0, -sin, cos)])
        xi = np.concatenate([np.where(side == 0, cos, sin), np.where(side == 0, -sin, cos)])
        return {
            "zf": halves(zf),
            "zi": halves(zi),
            "yf": halves(yf),
            "yi": halves(yi),
            "xf": halves(xf),
            "xi": halves(xi.T / period),
        }


def mm(left, right):
    return jnp.dot(left, right, preferred_element_type=F32)


def split(value):
    high = value.astype(jnp.bfloat16)
    low = (value - high.astype(F32)).astype(jnp.bfloat16)
    return high, low


def right_mul(value, high, low):
    vh, vl = value
    return mm(vh, high) + mm(vh, low) + mm(vl, high)


def left_mul(high, low, value):
    vh, vl = value
    return mm(high, vh) + mm(low, vh) + mm(high, vl)


def each(count, body, looped):
    if looped and count > 1:
        lax.fori_loop(0, count, lambda n, carry: (body(n), carry)[1], 0)
    else:
        for n in range(count):
            body(n)


NAMES = ("zf", "yf", "xf", "xi", "yi", "zi")


def core(plan, mask, *refs):
    occ_ref, orb_hbm, kern_hbm, *table_hbm = refs[:9]
    out_ref = refs[9]
    raw, flat, zf, yf, xf, xi, yi, zi = refs[10:18]
    bank, terms, back, cube, turned, going, coming, leaving, landing, lines = refs[18:28]
    load_sem, zs, zr, fs, fr, bs, br, rs, rr = refs[28:]
    slabs, parts, planes, period = plan.slabs, plan.parts, plan.planes, plan.period
    grid, quads, fold, wide, tiles = plan.grid, plan.quads, plan.fold, plan.wide, plan.tiles
    columns = plan.columns

    loads = [
        pltpu.make_async_copy(source, dest, load_sem.at[n])
        for n, (source, dest) in enumerate(
            zip([orb_hbm, kern_hbm, *table_hbm], [raw, flat, zf, yf, xf, xi, yi, zi])
        )
    ]
    loads[0].start()

    me = lax.axis_index("slab")
    g = lax.axis_index("grp")
    top = 1 << (mask.bit_length() - 1)
    quad = mask % 2 == 0
    owner = (g % 2) == ((g // top) % 2 if quad else 0)
    helper = jnp.logical_not(owner)
    mate = 1 if quad else mask
    steps = sorted(range(1, slabs), key=lambda step: -step)
    others = sorted({mate, mask, mask ^ 1} if quad else {mask})
    barrier = pltpu.get_barrier_semaphore()
    mesh_id = pl.DeviceIdType.MESH
    for other in others:
        pl.semaphore_signal(barrier, 1, device_id={"grp": g ^ other}, device_id_type=mesh_id)
    for step in steps:
        pl.semaphore_signal(barrier, 1, device_id={"slab": me ^ step}, device_id_type=mesh_id)

    def hop(source, dest, send_sem, recv_sem, other):
        return pltpu.make_async_remote_copy(
            src_ref=source,
            dst_ref=dest,
            send_sem=send_sem,
            recv_sem=recv_sem,
            device_id={"grp": g ^ other},
            device_id_type=mesh_id,
        )

    even = planes % fold == 0
    last_chunk, last_part = plan.chunks - 1, parts - 1

    def aligned(start, size):
        return pl.ds(start if isinstance(start, int) else pl.multiple_of(start, SUB), size)

    def block(chunk):
        return aligned(chunk * (fold * quads), plan.sizes(chunk) * quads)

    def when(condition, act):
        if isinstance(condition, bool):
            if condition:
                act()
        else:
            pl.when(condition)(act)

    def ahead(chunk, source, slot, other):
        at = block(chunk)
        n = slot - 2
        return hop(
            bank.at[source, at], bank.at[slot, at], zs.at[source, chunk], zr.at[n, chunk], other
        )

    def answer(chunk, source, slot, other):
        at = block(chunk)
        return hop(
            terms.at[source, at], back.at[slot, at], rs.at[source, chunk], rr.at[slot, chunk], other
        )

    def sends_ahead(chunk):
        mine = [ahead(chunk, 0, 2, mate), ahead(chunk, 1, 3, mate)]
        theirs = [ahead(chunk, 0, 4, mask)] + ([ahead(chunk, 1, 4, mask ^ 1)] if quad else [])
        return mine, theirs

    def sends_back(chunk):
        mine = [answer(chunk, 2, 0, mask)]
        theirs = [answer(chunk, 0, 0, mate), answer(chunk, 1, 1, mate)]
        return mine, theirs + ([answer(chunk, 2, 1, mask ^ 1)] if quad else [])

    def both(pair, act):
        for role, copies in zip((owner, helper), pair):

            @pl.when(role)
            def _(copies=copies):
                for copy in copies:
                    act(copy)

    every = slice(None)
    ways = ((going, coming, fs, fr), (leaving, landing, bs, br))

    def whole(chunk):
        return 0, chunk, every, chunk

    def tail(part):
        return 0, last_chunk, part, last_chunk + part

    def early(part):
        return 1, slice(0, last_chunk), part, part

    def late(chunk):
        return 1, chunk, last_part, last_part + chunk

    rest = 1, last_chunk, every, last_part + last_chunk
    pieces = [whole(chunk) for chunk in range(last_chunk)] + [tail(part) for part in range(parts)]
    if last_chunk:
        pieces += [early(part) for part in range(last_part)]
    pieces += [late(chunk) for chunk in range(last_chunk)] + [rest]

    def spread(piece, step, arriving):
        way, chunk, part, sem = piece
        source, dest, ss, sr = ways[way]
        peer = me ^ step
        return pltpu.make_async_remote_copy(
            src_ref=source.at[chunk, part, peer],
            dst_ref=dest.at[chunk, part, peer if arriving else me],
            send_sem=ss.at[sem, step],
            recv_sem=sr.at[sem, step],
            device_id={"slab": peer},
            device_id_type=mesh_id,
        )

    def spread_out(piece):
        for step in steps:
            spread(piece, step, False).start()
        way, chunk, part, _ = piece
        source, dest = ways[way][:2]
        dest[chunk, part, pl.ds(me, 1)] = source[chunk, part, pl.ds(me, 1)]

    def spread_in(piece):
        for step in steps:
            spread(piece, step, True).wait_recv()

    scale = [jnp.sqrt(0.25 * jnp.full((1, LANE), occ_ref[i], jnp.int32).astype(F32)) for i in range(2)]

    def cells(x, i, r):
        return pl.ds((x * quads * tiles + r) * 2 + i, quads, stride=2 * tiles)

    with jax.named_scope("w_raw"):
        loads[0].wait()

    def own_chunk(chunk):
        for n in range(plan.sizes(chunk)):
            x = chunk * fold + n
            for i in range(2):
                for r in range(tiles):
                    bank[i, aligned(x * quads, quads), r * LANE : (r + 1) * LANE] = (
                        raw[cells(x, i, r), :] * scale[i]
                    )

        def meet():
            with jax.named_scope("w_barrier"):
                pl.semaphore_wait(barrier, len(others) + len(steps))

        when(chunk == 0, meet)
        both(sends_ahead(chunk), lambda copy: copy.start())

    own_chunk(0)
    for load in loads[1:]:
        load.start()
    for chunk in range(1, plan.chunks):
        own_chunk(chunk)

    with jax.named_scope("w_kern"):
        loads[1].wait()
    pairs = period // 2
    per = 2 * period // LANE
    if plan.freqs % SUB == 0:
        unit = SUB
        plane_start = lambda k: k // SUB * (period * period // LANE * SUB) + k % SUB
    else:
        unit = plan.freqs
        plane_start = lambda k: k

    def one_cube(k, carry):
        first = plane_start(k)
        got = [flat[pl.ds(first + m * unit, pairs, stride=per * unit), :] for m in range(per)]
        n = per // 2
        swapped = [pltpu.roll(v, LANE // 2, 1) for v in got[n:]]
        lane = lax.broadcasted_iota(jnp.int32, (pairs, LANE), 1)
        spare = jnp.zeros((wide - period, LANE), F32)
        for t in range(n + 1):
            odd = swapped[t]
            if t < n:
                odd = jnp.where(lane < LANE // 2, odd, swapped[t + 1])
            rows = jnp.concatenate([got[t], odd, spare], axis=0).T
            depth = min(LANE, period - t * LANE)
            cube[k, t * LANE : t * LANE + depth, :] = rows[:depth]
        return carry

    with jax.named_scope("p_cube"):
        lax.fori_loop(0, plan.freqs, one_cube, 0)

    left = [jnp.where(owner, i, 2 + i) for i in range(2)]
    right = jnp.where(owner, 4, 4 if quad else 1)
    for load in loads[2:]:
        load.wait()

    share = LANE // (slabs * SUB)

    def forward_z(chunk):
        heard = ([ahead(chunk, 0, 4, mask)], [ahead(chunk, 0, 2, mate), ahead(chunk, 1, 3, mate)])
        if quad:
            heard[1].append(ahead(chunk, 1, 4, mask ^ 1))
        with jax.named_scope("w_ahead"):
            both(heard, lambda copy: copy.wait_recv())
        at, count = block(chunk), plan.sizes(chunk)
        partner = bank[right, at]
        densities = [split(bank[left[i], at] * partner) for i in range(2)]
        if count < fold:
            turned[count * period :, :] = jnp.zeros(((fold - count) * period, columns), F32)
        for j in range(fold):
            lane = slice(plan.cell_starts[j], plan.cell_starts[j] + wide)
            rows = slice(plan.cell_slides[j], plan.cell_slides[j] + wide)
            total = None
            for i in range(2):
                piece = tuple(part[:, lane] for part in densities[i])
                term = right_mul(piece, zf[0, i, rows], zf[1, i, rows])
                total = term if total is None else total + term
            for x in range(count):
                for c in range(2):
                    first = x * period + c * grid + j * quads
                    turned[first : first + quads, :] = total[
                        x * quads : (x + 1) * quads, c * columns : (c + 1) * columns
                    ]
        for col in range(0, columns, LANE):
            for r in range(0, plan.lanes, LANE):
                flip = turned[r : r + LANE, col : col + LANE].T.reshape(share, slabs, SUB, LANE)
                for n in range(min(share, parts - col // LANE * share)):
                    going[chunk, col // LANE * share + n, :, :, r : r + LANE] = flip[n]

        def by_part():
            each(parts, lambda part: spread_out(tail(part)), True)

        when(chunk < last_chunk, lambda: spread_out(whole(chunk)))
        when(chunk == last_chunk, by_part)

    each(plan.chunks, forward_z, even)

    size = slabs * SUB
    halves_of = range(wide // LANE)

    def line(part, x, c):
        return aligned(part * plan.line_rows + (x * 2 + c) * size, size)

    def forward_y(chunk, some):
        for kind, offset in enumerate(plan.pair_kinds):
            own = [j for j in range(plan.sizes(chunk)) if plan.pair_kind[j] == kind]
            piece = []
            for j in own:
                lane = slice(plan.pair_starts[j], plan.pair_starts[j] + wide)
                for part in some:
                    piece.append(coming[chunk, part, :, :, lane].reshape(size, wide))
            slide = plan.pair_kinds[-1] - offset
            rows = slice(slide, slide + wide)
            piece = jnp.concatenate(piece, axis=0) if len(piece) > 1 else piece[0]
            field = right_mul(split(piece), yf[0, rows], yf[1, rows])
            for n, (j, part) in enumerate((j, part) for j in own for part in some):
                for c in range(2):
                    for t in halves_of:
                        spot = c * wide + t * LANE
                        lines[t, line(part, chunk * fold + j, c), :] = field[
                            n * size : (n + 1) * size, spot : spot + LANE
                        ]

    def some_planes(part, k, count):
        rows = [
            pl.ds(part * plan.line_rows + k + n, planes * 2 * slabs, stride=SUB)
            for n in range(count)
        ]
        field = jnp.concatenate([lines[t, r, :] for r in rows for t in halves_of], axis=1)
        spectra = left_mul(xf[0], xf[1], split(field))
        kernel = jnp.concatenate([cube[part * SUB + k + n] for n in range(count)], axis=1)
        spectra = jnp.concatenate(
            [spectra[:period] * kernel, spectra[period:] * kernel], axis=0
        )
        field = left_mul(xi[0], xi[1], split(spectra))
        for n, r in enumerate(rows):
            for t in halves_of:
                first = n * wide + t * LANE
                lines[t, r, :] = field[:, first : first + LANE]

    def inverse_y(part):
        total = {}
        for kind in range(len(plan.pair_kinds)):
            own = [x for x in range(planes) if plan.pair_kind[x % fold] == kind]
            field = [
                jnp.concatenate(
                    [lines[t, line(part, x, c), :] for c in range(2) for t in halves_of], axis=1
                )
                for x in own
            ]
            field = jnp.concatenate(field, axis=0) if len(field) > 1 else field[0]
            field = right_mul(split(field), yi[0, kind], yi[1, kind])
            for n, x in enumerate(own):
                for t in halves_of:
                    spot = (x // fold, plan.pair_starts[x % fold] // LANE + t)
                    term = field[n * size : (n + 1) * size, t * LANE : (t + 1) * LANE]
                    total[spot] = total[spot] + term if spot in total else term
        for chunk in range(plan.chunks):
            for t in range(plan.lanes // LANE):
                term = total.get((chunk, t))
                if term is None:
                    term = jnp.zeros((size, LANE), F32)
                leaving[chunk, part, :, :, t * LANE : (t + 1) * LANE] = term.reshape(
                    slabs, SUB, LANE
                )

    def y_chunk(chunk):
        with jax.named_scope("w_in0"):
            spread_in(whole(chunk))
        with jax.named_scope("p_y"):
            forward_y(chunk, range(parts))

    def one_part(part):
        with jax.named_scope("w_in0p"):
            spread_in(tail(part))
        with jax.named_scope("p_y1"):
            forward_y(last_chunk, [part])
        with jax.named_scope("p_x"):
            live = SUB if plan.freqs % SUB == 0 else min(SUB, plan.freqs - part * SUB)
            count = next(n for n in (4, 2, 1) if live % n == 0)
            each(live // count, lambda n: some_planes(part, n * count, count), True)
        with jax.named_scope("p_yi"):
            inverse_y(part)

            def final():
                each(last_chunk, lambda chunk: spread_out(late(chunk)), True)
                spread_out(rest)

            if last_chunk:
                when(part < last_part, lambda: spread_out(early(part)))
            when(part == last_part, final)

    each(last_chunk, y_chunk, even)
    each(parts, one_part, plan.freqs % SUB == 0)

    def inverse_z(chunk):
        with jax.named_scope("w_in1"):
            when(chunk < last_chunk, lambda: spread_in(late(chunk)))
            when(chunk == last_chunk, lambda: spread_in(rest))
        at, count = block(chunk), plan.sizes(chunk)
        for col in range(0, columns, LANE):
            for r in range(0, plan.lanes, LANE):
                got = []
                for n in range(share):
                    part = col // LANE * share + n
                    if part < parts:
                        one = landing[chunk, part, :, :, r : r + LANE].reshape(slabs * SUB, LANE)
                    else:
                        one = jnp.zeros((slabs * SUB, LANE), F32)
                    got.append(one)
                got = jnp.concatenate(got, axis=0) if share > 1 else got[0]
                turned[r : r + LANE, col : col + LANE] = got.T
        total = [[None] * tiles for _ in range(2)]
        for j in range(fold):
            rows = []
            for x in range(count):
                firsts = [x * period + c * grid + j * quads for c in range(2)]
                rows.append(
                    jnp.concatenate([turned[f : f + quads, :] for f in firsts], axis=1)
                )
            rows = jnp.concatenate(rows, axis=0)
            field = right_mul(split(rows), zi[0, j], zi[1, j])
            for i in range(2):
                for t in range(wide // LANE):
                    spot = plan.cell_starts[j] // LANE + t
                    first = i * wide + t * LANE
                    term = field[:, first : first + LANE]
                    known = total[i][spot]
                    total[i][spot] = term if known is None else known + term
        far = None
        partner = bank[right, at]
        for i in range(2):
            field = jnp.concatenate(total[i], axis=1)
            terms[i, at] = field * partner
            term = field * bank[left[i], at]
            far = term if far is None else far + term
        terms[2, at] = far
        both(sends_back(chunk), lambda copy: copy.start())

    with jax.named_scope("w_in1"):
        if last_chunk:
            each(last_part, lambda part: spread_in(early(part)), True)
    each(plan.chunks, inverse_z, even)

    weight = [-1.0 / s for s in scale]

    def finish(chunk):
        heard = ([answer(chunk, 0, 0, mate), answer(chunk, 1, 1, mate)], [answer(chunk, 2, 0, mask)])
        if quad:
            heard[1].append(answer(chunk, 2, 1, mask ^ 1))
        with jax.named_scope("w_back"):
            both(heard, lambda copy: copy.wait_recv())

        def put(i, value):
            for n in range(plan.sizes(chunk)):
                for r in range(tiles):
                    out_ref[cells(chunk * fold + n, i, r), :] = (
                        value[n * quads : (n + 1) * quads, r * LANE : (r + 1) * LANE] * weight[i]
                    )

        @pl.when(owner)
        def _():
            for i in range(2):
                put(i, terms[i, block(chunk)] + back[i, block(chunk)])

        @pl.when(helper)
        def _():
            put(0, back[0, block(chunk)])
            put(1, back[1, block(chunk)] if quad else terms[2, block(chunk)])

    each(plan.chunks, finish, even)

    def drain(chunk):
        both(sends_ahead(chunk), lambda copy: copy.wait_send())
        both(sends_back(chunk), lambda copy: copy.wait_send())

    each(plan.chunks, drain, even)
    for piece in pieces:
        for step in steps:
            spread(piece, step, False).wait_send()


def run_core(plan, mask, occupation, orbitals, kernel, tables):
    operands = [orbitals, kernel] + [tables[name] for name in NAMES]
    out = jax.ShapeDtypeStruct(orbitals.shape, F32)
    wire = pltpu.VMEM((plan.chunks, plan.parts, plan.slabs, SUB, plan.lanes), F32)
    dma = pltpu.SemaphoreType.DMA
    return pl.pallas_call(
        lambda *refs: core(plan, mask, *refs),
        out_shape=out,
        in_specs=[pl.BlockSpec(memory_space=pltpu.SMEM)]
        + [pl.BlockSpec(memory_space=pl.ANY)] * len(operands),
        out_specs=pl.BlockSpec(memory_space=pltpu.VMEM),
        scratch_shapes=[pltpu.VMEM(op.shape, op.dtype) for op in operands]
        + [
            pltpu.VMEM((5, plan.rows, plan.group), F32),
            pltpu.VMEM((3, plan.rows, plan.group), F32),
            pltpu.VMEM((2, plan.rows, plan.group), F32),
            pltpu.VMEM((plan.freqs, plan.period, plan.wide), F32),
            pltpu.VMEM((plan.lanes, plan.columns), F32),
            wire,
            wire,
            wire,
            wire,
            pltpu.VMEM((plan.wide // LANE, plan.parts * plan.line_rows, LANE), F32),
            dma((len(operands),)),
            dma((2, plan.chunks)),
            dma((3, plan.chunks)),
        ]
        + [dma((plan.chunks + plan.parts - 1, plan.slabs))] * 4
        + [dma((3, plan.chunks)), dma((2, plan.chunks))],
        compiler_params=pltpu.CompilerParams(
            collective_id=mask, has_side_effects=True, vmem_limit_bytes=62 * 2**20
        ),
    )(occupation, *operands)


def local(orbitals, occupation, kernel_hat, pair_mask):
    orbit_count, planes, plane_cells = orbitals.shape
    assert orbit_count == 2 and plane_cells % LANE == 0
    slabs = lax.axis_size("slab")
    groups = lax.axis_size("grp")
    freqs, columns = kernel_hat.shape
    plan = Plan(planes, plane_cells, slabs, freqs)
    tables = {name: jnp.asarray(t) for name, t in plan.tables().items()}
    tiles = plane_cells // LANE
    flat = orbitals.reshape(2, planes, tiles, LANE).transpose(1, 2, 0, 3).reshape(-1, LANE)
    if freqs % SUB == 0:
        kernel = kernel_hat.reshape(freqs // SUB, SUB, columns // LANE, LANE)
        kernel = kernel.transpose(0, 2, 1, 3).reshape(-1, LANE)
    else:
        kernel = kernel_hat.reshape(freqs, columns // LANE, LANE)
        kernel = kernel.transpose(1, 0, 2).reshape(-1, LANE)

    def branch(mask):
        return lambda *args: run_core(plan, mask, *args, tables)

    branches = [branch(mask) for mask in range(1, groups)]
    out = lax.switch(pair_mask[0] - 1, branches, occupation, flat, kernel)
    return out.reshape(planes, tiles, 2, LANE).transpose(2, 0, 1, 3).reshape(2, planes, plane_cells)


def solution(mesh):
    return jax.shard_map(
        local,
        mesh=mesh,
        in_specs=(P("grp", "slab", None), P("grp"), P("slab", None), P()),
        out_specs=P("grp", "slab", None),
        check_vma=False,
    )
```

```python
import math

import jax
import jax.numpy as jnp
import ml_dtypes
import numpy as np
from jax import lax
from jax.experimental import pallas as pl
from jax.experimental.pallas import tpu as pltpu
from jax.sharding import PartitionSpec as P

LANE = 128
EARLY = (4, 2)
LATER = 3
SUB = 8
F32 = jnp.float32


def halves(table):
    high = table.astype(np.float32).astype(ml_dtypes.bfloat16)
    low = (table - high.astype(np.float64)).astype(ml_dtypes.bfloat16)
    return np.stack([high, low])


def padded(size, unit):
    return -(-size // unit) * unit


class Plan:
    def __init__(self, planes, plane_cells, slabs, freqs):
        self.planes, self.slabs, self.freqs = planes, slabs, freqs
        self.grid = math.isqrt(plane_cells)
        self.period = 2 * self.grid
        self.group = math.lcm(self.grid, LANE)
        self.fold = self.group // self.grid
        self.quads = self.grid // self.fold
        self.tiles = self.group // LANE
        self.rows = planes * self.quads
        self.per = math.lcm(self.period, LANE) // self.period
        self.chunks = -(-planes // self.per)
        self.wide = padded(self.period, LANE)
        self.lanes = self.per * self.period
        self.parts = -(-freqs // SUB)
        self.columns = padded(self.parts * slabs * SUB, LANE)
        self.line_rows = planes * 2 * slabs * SUB
        self.pair_starts = self.windows(self.per, self.period, self.lanes)
        assert self.period % LANE == LANE // 2 and LANE % (slabs * SUB) == 0

    def windows(self, count, step, lanes):
        return [min(j * step // LANE * LANE, lanes - self.wide) for j in range(count)]

    def sizes(self, chunk):
        even = self.planes % self.per == 0
        return self.per if even else min(self.per, self.planes - chunk * self.per)

    def wave(self, left, right):
        angle = 2.0 * math.pi / self.period * (np.outer(left, right) % self.period)
        return np.cos(angle), np.sin(angle)

    def tables(self):
        grid, period, fold, wide = self.grid, self.period, self.fold, self.wide
        columns = self.columns
        freq = np.zeros(columns, int)
        live = np.zeros(columns, bool)
        for n in range(self.parts * self.slabs * SUB):
            part, rest = divmod(n, self.slabs * SUB)
            own = part * SUB + rest % SUB
            freq[n] = rest // SUB * self.freqs + own
            live[n] = own < self.freqs
        cells = np.arange(grid)
        zc, zs = self.wave(cells, np.where(live, freq, 0))
        zc, zs = zc * live, zs * live
        zf = np.zeros((wide, 2 * columns))
        zf[:grid, :columns], zf[:grid, columns:] = zc, -zs
        zf[grid:period, :columns], zf[grid:period, columns:] = zs, zc
        zi = np.zeros((2 * columns, wide))
        zi[:columns, :grid], zi[:columns, grid:period] = zc.T / period, zs.T / period
        zi[columns:, :grid], zi[columns:, grid:period] = -zs.T / period, zc.T / period
        y_order = np.array([fold * q + j for j in range(fold) for q in range(self.quads)])
        ky_order = np.concatenate([np.arange(0, period, 2), np.arange(1, period, 2)])
        yc, ys = self.wave(y_order, ky_order)
        offsets = [j * period - self.pair_starts[j] for j in range(self.per)]
        reach = max(offsets)
        self.pair_slides = [reach - offset for offset in offsets]
        self.pair_kinds = sorted(set(offsets))
        self.pair_kind = [self.pair_kinds.index(offset) for offset in offsets]
        yf = np.zeros((reach + wide, 2 * wide))
        re, im = slice(reach, reach + grid), slice(reach + grid, reach + period)
        yf[re, :period], yf[re, wide : wide + period] = yc, -ys
        yf[im, :period], yf[im, wide : wide + period] = ys, yc
        yi = np.zeros((len(self.pair_kinds), 2 * wide, wide))
        for n, offset in enumerate(self.pair_kinds):
            re, im = slice(offset, offset + grid), slice(offset + grid, offset + period)
            yi[n, :period, re], yi[n, :period, im] = yc.T / period, ys.T / period
            yi[n, wide : wide + period, re] = -ys.T / period
            yi[n, wide : wide + period, im] = yc.T / period
        row = [
            (c, s * self.planes + x)
            for x in range(self.planes)
            for c in range(2)
            for s in range(self.slabs)
        ]
        side = np.array([r[0] for r in row])
        cos, sin = self.wave(np.arange(period), np.array([r[1] for r in row]))
        xf = np.concatenate([np.where(side == 0, cos, sin), np.where(side == 0, -sin, cos)])
        xi = np.concatenate([np.where(side == 0, cos, sin), np.where(side == 0, -sin, cos)])
        return {
            "zf": halves(zf),
            "zi": halves(zi),
            "yf": halves(yf),
            "yi": halves(yi),
            "xf": halves(xf),
            "xi": np.concatenate([halves(xi.T / period)[n] for n in (0, 1, 0)], axis=1),
        }


def mm(left, right):
    return jnp.dot(left, right, preferred_element_type=F32)


def split(value):
    high = value.astype(jnp.bfloat16)
    low = (value - high.astype(F32)).astype(jnp.bfloat16)
    return high, low


def right_mul(value, high, low):
    vh, vl = value
    return mm(vh, high) + mm(vh, low) + mm(vl, high)


def left_mul(high, low, value):
    vh, vl = value
    return mm(high, vh) + mm(low, vh) + mm(high, vl)


def each(count, body, looped):
    if looped and count > 1:
        lax.fori_loop(0, count, lambda n, carry: (body(n), carry)[1], 0)
    else:
        for n in range(count):
            body(n)


def lane_of(value):
    return lax.broadcasted_iota(jnp.int32, value.shape, 1)


def place(tiles, start, dest, index):
    shift = (dest - start) % LANE
    base = index + (start - dest + shift) // LANE
    if shift == 0:
        return tiles[base]
    below, above = (
        pltpu.roll(tiles[n], shift, 1) if 0 <= n < len(tiles) else None for n in (base - 1, base)
    )
    if below is None or above is None:
        return above if below is None else below
    return jnp.where(lane_of(above) < shift, below, above)


def join(first, second, at, index):
    low, high = index * LANE, (index + 1) * LANE
    if at <= low:
        return second(index)
    if at >= high:
        return first(index)
    value = first(index)
    return jnp.where(lane_of(value) < at - low, value, second(index))


NAMES = ("zf", "yf", "xf", "xi", "yi", "zi")


def core(plan, mask, *refs):
    occ_ref, orb_hbm, kern_hbm, *table_hbm = refs[:9]
    out_ref = refs[9]
    raw, flat, zf, yf, xf, xi, yi, zi = refs[10:18]
    bank, terms, back, cube, turned, going, coming, leaving, landing, lines = refs[18:28]
    load_sem, zs, zr, fs, fr, bs, br, rs, rr = refs[28:]
    slabs, parts, planes, period = plan.slabs, plan.parts, plan.planes, plan.period
    grid, quads, fold, wide, tiles = plan.grid, plan.quads, plan.fold, plan.wide, plan.tiles
    columns = plan.columns

    loads = [
        pltpu.make_async_copy(source, dest, load_sem.at[n])
        for n, (source, dest) in enumerate(
            zip([orb_hbm, kern_hbm, *table_hbm], [raw, flat, zf, yf, xf, xi, yi, zi])
        )
    ]
    loads[0].start()

    me = lax.axis_index("slab")
    g = lax.axis_index("grp")
    top = 1 << (mask.bit_length() - 1)
    quad = mask % 2 == 0
    owner = (g % 2) == ((g // top) % 2 if quad else 0)
    helper = jnp.logical_not(owner)
    mate = 1 if quad else mask
    steps = sorted(range(1, slabs), key=lambda step: -step)
    others = sorted({mate, mask, mask ^ 1} if quad else {mask})
    barrier = pltpu.get_barrier_semaphore()
    mesh_id = pl.DeviceIdType.MESH
    for other in others:
        pl.semaphore_signal(barrier, 1, device_id={"grp": g ^ other}, device_id_type=mesh_id)
    for step in steps:
        pl.semaphore_signal(barrier, 1, device_id={"slab": me ^ step}, device_id_type=mesh_id)

    def hop(source, dest, send_sem, recv_sem, other):
        return pltpu.make_async_remote_copy(
            src_ref=source,
            dst_ref=dest,
            send_sem=send_sem,
            recv_sem=recv_sem,
            device_id={"grp": g ^ other},
            device_id_type=mesh_id,
        )

    per = plan.per
    even = planes % per == 0
    last_chunk, last_part = plan.chunks - 1, parts - 1

    def aligned(start, size):
        return pl.ds(start if isinstance(start, int) else pl.multiple_of(start, SUB), size)

    def block(chunk):
        return aligned(chunk * (per * quads), plan.sizes(chunk) * quads)

    def when(condition, act):
        if isinstance(condition, bool):
            if condition:
                act()
        else:
            pl.when(condition)(act)

    def ahead(chunk, source, slot, other):
        at = block(chunk)
        n = slot - 2
        return hop(
            bank.at[source, at], bank.at[slot, at], zs.at[source, chunk], zr.at[n, chunk], other
        )

    def answer(chunk, source, slot, other):
        at = block(chunk)
        return hop(
            terms.at[source, at], back.at[slot, at], rs.at[source, chunk], rr.at[slot, chunk], other
        )

    def sends_ahead(chunk):
        mine = [ahead(chunk, 0, 2, mate), ahead(chunk, 1, 3, mate)]
        theirs = [ahead(chunk, 0, 4, mask)] + ([ahead(chunk, 1, 4, mask ^ 1)] if quad else [])
        return mine, theirs

    crossing = False

    def sends_ahead_now(chunk):
        mine, theirs = sends_ahead(chunk)
        return mine, ([] if crossing else theirs)

    def sends_ahead_later(chunk):
        if not crossing:
            return

        @pl.when(helper)
        def _():
            when(chunk >= LATER, lambda: ahead(chunk - LATER, 0, 4, mask).start())

            def others_left():
                for n in range(max(0, plan.chunks - LATER), plan.chunks):
                    ahead(n, 0, 4, mask).start()

            when(chunk == last_chunk, others_left)

    def sends_back(chunk):
        mine = [answer(chunk, 2, 0, mask)]
        theirs = [answer(chunk, 0, 0, mate), answer(chunk, 1, 1, mate)]
        return mine, theirs + ([answer(chunk, 2, 1, mask ^ 1)] if quad else [])

    def both(pair, act):
        for role, copies in zip((owner, helper), pair):

            @pl.when(role)
            def _(copies=copies):
                for copy in copies:
                    act(copy)

    every = slice(None)
    ways = ((going, coming, fs, fr), (leaving, landing, bs, br))

    def whole(chunk):
        return 0, chunk, every, chunk

    def tail(part):
        return 0, last_chunk, part, last_chunk + part

    early_chunks = [last_chunk * EARLY[min(p, 1)] // 6 for p in range(last_part)]
    kept = [sum(chunk < count for count in early_chunks) for chunk in range(plan.chunks)]

    def early(part, count):
        return 1, slice(0, count), part, part

    def late(chunk, done):
        return 1, chunk, slice(done, parts), last_part + chunk

    hold = last_chunk - 1
    held = (0, hold, slice(0, last_part), hold), (0, hold, last_part, last_chunk + parts)
    pieces = [whole(chunk) for chunk in range(hold)] + [tail(part) for part in range(parts)]
    pieces += list(held)
    pieces += [early(part, count) for part, count in enumerate(early_chunks) if count]
    pieces += [late(chunk, kept[chunk]) for chunk in range(plan.chunks)]

    def with_kept(chunk, act):
        for done in sorted(set(kept)):
            own = [n for n in range(plan.chunks) if kept[n] == done]
            if isinstance(chunk, int):
                if chunk in own:
                    act(late(chunk, done))
            else:
                inside = jnp.logical_and(chunk >= own[0], chunk <= own[-1])
                pl.when(inside)(lambda done=done: act(late(chunk, done)))

    def spread(piece, step, arriving):
        way, chunk, part, sem = piece
        source, dest, ss, sr = ways[way]
        peer = me ^ step
        return pltpu.make_async_remote_copy(
            src_ref=source.at[chunk, part, peer],
            dst_ref=dest.at[chunk, part, peer if arriving else me],
            send_sem=ss.at[sem, step],
            recv_sem=sr.at[sem, step],
            device_id={"slab": peer},
            device_id_type=mesh_id,
        )

    def spread_out(piece):
        for step in steps:
            spread(piece, step, False).start()
        way, chunk, part, _ = piece
        source, dest = ways[way][:2]
        dest[chunk, part, pl.ds(me, 1)] = source[chunk, part, pl.ds(me, 1)]

    def spread_in(piece):
        for step in steps:
            spread(piece, step, True).wait_recv()

    scale = [jnp.sqrt(0.25 * jnp.full((1, LANE), occ_ref[i], jnp.int32).astype(F32)) for i in range(2)]

    def cells(x, i, r):
        return pl.ds((x * quads * tiles + r) * 2 + i, quads, stride=2 * tiles)

    with jax.named_scope("w_raw"):
        loads[0].wait()

    def own_chunk(chunk):
        for n in range(plan.sizes(chunk)):
            x = chunk * per + n
            for i in range(2):
                for r in range(tiles):
                    bank[i, aligned(x * quads, quads), r * LANE : (r + 1) * LANE] = (
                        raw[cells(x, i, r), :] * scale[i]
                    )

        def meet():
            with jax.named_scope("w_barrier"):
                pl.semaphore_wait(barrier, len(others) + len(steps))

        when(chunk == 0, meet)
        both(sends_ahead_now(chunk), lambda copy: copy.start())

    own_chunk(0)
    for load in loads[1:]:
        load.start()
    for chunk in range(1, plan.chunks):
        own_chunk(chunk)

    with jax.named_scope("w_kern"):
        loads[1].wait()
    pairs = period // 2
    pitch = 2 * period // LANE
    if plan.freqs % SUB == 0:
        unit = SUB
        plane_start = lambda k: k // SUB * (period * period // LANE * SUB) + k % SUB
    else:
        unit = plan.freqs
        plane_start = lambda k: k

    def cube_side(k, side):
        first = plane_start(k)
        got = [flat[pl.ds(first + m * unit, pairs, stride=pitch * unit), :] for m in range(pitch)]
        n = pitch // 2
        swapped = [pltpu.roll(v, LANE // 2, 1) for v in got[n:]]
        spare = jnp.zeros((wide - period, LANE), F32)
        result = []
        for t in range(n + 1):
            odd = swapped[t]
            if t < n:
                odd = jnp.where(lane_of(odd) < LANE // 2, odd, swapped[t + 1])
            rows = [got[t], odd, spare] if side == 0 else [spare, got[t], odd]
            result.append(jnp.concatenate(rows, axis=0).T[: min(LANE, period - t * LANE)])
        return result

    def cube_pair(pair, carry):
        low, high = cube_side(2 * pair, 0), cube_side(2 * pair + 1, 1)
        meet = period // LANE * LANE
        for t, (one, two) in enumerate(zip(low, high)):
            rows = slice(t * LANE, t * LANE + one.shape[0])
            cube[pair, rows, :meet] = one[:, :meet]
            cube[pair, rows, meet:wide] = one[:, meet:] + two[:, :LANE]
            cube[pair, rows, wide:] = two[:, LANE:]
        return carry

    with jax.named_scope("p_cube"):
        lax.fori_loop(0, plan.freqs // 2, cube_pair, 0)

    left = [jnp.where(owner, i, 2 + i) for i in range(2)]
    right = jnp.where(owner, 4, 4 if quad else 1)
    for load in loads[2:]:
        load.wait()

    share = LANE // (slabs * SUB)

    def forward_z(chunk):
        heard = ([ahead(chunk, 0, 4, mask)], [ahead(chunk, 0, 2, mate), ahead(chunk, 1, 3, mate)])
        if quad:
            heard[1].append(ahead(chunk, 1, 4, mask ^ 1))
        with jax.named_scope("w_ahead"):
            both(heard, lambda copy: copy.wait_recv())
        sends_ahead_later(chunk)
        at, count = block(chunk), plan.sizes(chunk)
        partner = bank[right, at]
        densities = [bank[left[i], at] * partner for i in range(2)]
        if count < per:
            turned[count * period :, :] = jnp.zeros(((per - count) * period, columns), F32)
        fields = []
        for j in range(fold):
            one, two = ([d[:, t * LANE : (t + 1) * LANE] for t in range(tiles)] for d in densities)
            fields.append(
                jnp.concatenate(
                    [
                        join(
                            lambda n: place(one, j * grid, 0, n),
                            lambda n: place(two, j * grid, grid, n),
                            grid,
                            n,
                        )
                        for n in range(wide // LANE)
                    ],
                    axis=1,
                )
            )
        total = right_mul(split(jnp.concatenate(fields, axis=0)), zf[0], zf[1])
        for j in range(fold):
            for x in range(count):
                for c in range(2):
                    first = x * period + c * grid + j * quads
                    row = (j * count + x) * quads
                    turned[first : first + quads, :] = total[
                        row : row + quads, c * columns : (c + 1) * columns
                    ]
        for col in range(0, columns, LANE):
            for r in range(0, plan.lanes, LANE):
                flip = turned[r : r + LANE, col : col + LANE].T.reshape(share, slabs, SUB, LANE)
                for n in range(min(share, parts - col // LANE * share)):
                    going[chunk, col // LANE * share + n, :, :, r : r + LANE] = flip[n]

        def by_part():
            each(last_part, lambda part: spread_out(tail(part)), True)
            spread_out(held[1])
            spread_out(tail(last_part))

        when(chunk < hold, lambda: spread_out(whole(chunk)))
        when(chunk == hold, lambda: spread_out(held[0]))
        when(chunk == last_chunk, by_part)

    each(plan.chunks, forward_z, even)

    size = slabs * SUB
    halves_of = range(wide // LANE)

    def line(part, x, c):
        return aligned(part * plan.line_rows + (x * 2 + c) * size, size)

    def forward_y(some_chunks, some):
        for kind, offset in enumerate(plan.pair_kinds):
            own = [
                (chunk, j, part)
                for chunk in some_chunks
                for j in range(plan.sizes(chunk))
                if plan.pair_kind[j] == kind
                for part in some
            ]
            piece = []
            for chunk, j, part in own:
                lane = slice(plan.pair_starts[j], plan.pair_starts[j] + wide)
                piece.append(coming[chunk, part, :, :, lane].reshape(size, wide))
            slide = plan.pair_kinds[-1] - offset
            rows = slice(slide, slide + wide)
            piece = jnp.concatenate(piece, axis=0) if len(piece) > 1 else piece[0]
            field = right_mul(split(piece), yf[0, rows], yf[1, rows])
            for n, (chunk, j, part) in enumerate(own):
                for c in range(2):
                    for t in halves_of:
                        spot = c * wide + t * LANE
                        lines[t, line(part, chunk * per + j, c), :] = field[
                            n * size : (n + 1) * size, spot : spot + LANE
                        ]

    def some_planes(part, k, count):
        rows = [
            pl.ds(part * plan.line_rows + k + n, planes * 2 * slabs, stride=SUB)
            for n in range(count)
        ]
        two_planes = 2 * period // LANE
        field = []
        for n in range(0, count, 2):
            one, two = ([lines[t, r, :] for t in halves_of] for r in rows[n : n + 2])
            field += [
                join(lambda t: one[t], lambda t: place(two, 0, period, t), period, t)
                for t in range(two_planes)
            ]
        pair = (part * SUB + k) // 2
        kernel = []
        for n in range(count // 2):
            kernel += [
                cube[pair + n, :, t * LANE : (t + 1) * LANE] for t in range(two_planes)
            ]
        stretches = []
        for t in range(0, len(field), 2):
            some = jnp.concatenate(kernel[t : t + 2], axis=1)
            spectra = left_mul(xf[0], xf[1], split(jnp.concatenate(field[t : t + 2], axis=1)))
            spectra = [spectra[:period] * some, spectra[period:] * some]
            stretches.append(split(jnp.concatenate(spectra, axis=0)))
        field = []
        for high, low in stretches:
            done = mm(xi[...], jnp.concatenate([high, high, low], axis=0))
            field += [done[:, t : t + LANE] for t in range(0, done.shape[1], LANE)]
        for n, r in enumerate(rows):
            own = field[n // 2 * two_planes : (n // 2 + 1) * two_planes]
            for t in halves_of:
                lines[t, r, :] = own[t] if n % 2 == 0 else place(own, period, 0, t)

    def inverse_y(part):
        total = {}
        for kind in range(len(plan.pair_kinds)):
            own = [x for x in range(planes) if plan.pair_kind[x % per] == kind]
            field = [
                jnp.concatenate(
                    [lines[t, line(part, x, c), :] for c in range(2) for t in halves_of], axis=1
                )
                for x in own
            ]
            field = jnp.concatenate(field, axis=0) if len(field) > 1 else field[0]
            field = right_mul(split(field), yi[0, kind], yi[1, kind])
            for n, x in enumerate(own):
                for t in halves_of:
                    spot = (x // per, plan.pair_starts[x % per] // LANE + t)
                    term = field[n * size : (n + 1) * size, t * LANE : (t + 1) * LANE]
                    total[spot] = total[spot] + term if spot in total else term
        for chunk in range(plan.chunks):
            for t in range(plan.lanes // LANE):
                term = total.get((chunk, t))
                if term is None:
                    term = jnp.zeros((size, LANE), F32)
                leaving[chunk, part, :, :, t * LANE : (t + 1) * LANE] = term.reshape(
                    slabs, SUB, LANE
                )

    def y_chunk(chunk):
        with jax.named_scope("w_in0"):
            spread_in(whole(chunk))
        with jax.named_scope("p_y"):
            forward_y([chunk], range(parts))

    def one_part(part):
        with jax.named_scope("w_in0p"):
            when(part == 0, lambda: spread_in(held[0]))
            when(part == last_part, lambda: spread_in(held[1]))
            spread_in(tail(part))
        with jax.named_scope("p_y1"):
            forward_y([hold, last_chunk], [part])
        with jax.named_scope("p_x"):
            live = SUB if plan.freqs % SUB == 0 else min(SUB, plan.freqs - part * SUB)
            some_planes(part, 0, live)
        with jax.named_scope("p_yi"):
            inverse_y(part)

            def final():
                each(plan.chunks, lambda chunk: with_kept(chunk, spread_out), True)

            for p, count in enumerate(early_chunks):
                if count:
                    when(part == p, lambda p=p, count=count: spread_out(early(p, count)))
            when(part == last_part, final)

    each(hold, y_chunk, even)
    each(parts, one_part, plan.freqs % SUB == 0)

    def inverse_z(chunk):
        with jax.named_scope("w_in1"):
            with_kept(chunk, spread_in)
        at, count = block(chunk), plan.sizes(chunk)
        for col in range(0, columns, LANE):
            for r in range(0, plan.lanes, LANE):
                got = []
                for n in range(share):
                    part = col // LANE * share + n
                    if part < parts:
                        one = landing[chunk, part, :, :, r : r + LANE].reshape(slabs * SUB, LANE)
                    else:
                        one = jnp.zeros((slabs * SUB, LANE), F32)
                    got.append(one)
                got = jnp.concatenate(got, axis=0) if share > 1 else got[0]
                turned[r : r + LANE, col : col + LANE] = got.T
        rows = []
        for j in range(fold):
            for x in range(count):
                firsts = [x * period + c * grid + j * quads for c in range(2)]
                rows.append(jnp.concatenate([turned[f : f + quads, :] for f in firsts], axis=1))
        total = right_mul(split(jnp.concatenate(rows, axis=0)), zi[0], zi[1])
        strips = [
            [
                total[j * count * quads : (j + 1) * count * quads, t * LANE : (t + 1) * LANE]
                for t in range(wide // LANE)
            ]
            for j in range(fold)
        ]

        def potential(i):
            def strip(j):
                if j == fold - 1:
                    return lambda t: place(strips[j], i * grid, j * grid, t)
                return lambda t: join(
                    lambda t: place(strips[j], i * grid, j * grid, t), strip(j + 1), (j + 1) * grid, t
                )

            return jnp.concatenate([strip(0)(t) for t in range(tiles)], axis=1)

        far = None
        partner = bank[right, at]
        for i in range(2):
            field = potential(i)
            terms[i, at] = field * partner
            term = field * bank[left[i], at]
            far = term if far is None else far + term
        terms[2, at] = far
        both(sends_back(chunk), lambda copy: copy.start())

    with jax.named_scope("w_in1"):
        for part, count in enumerate(early_chunks):
            if count:
                spread_in(early(part, count))
    each(plan.chunks, inverse_z, even)

    weight = [-1.0 / s for s in scale]

    def finish(chunk):
        heard = ([answer(chunk, 0, 0, mate), answer(chunk, 1, 1, mate)], [answer(chunk, 2, 0, mask)])
        if quad:
            heard[1].append(answer(chunk, 2, 1, mask ^ 1))
        with jax.named_scope("w_back"):
            both(heard, lambda copy: copy.wait_recv())

        def put(i, value):
            for n in range(plan.sizes(chunk)):
                for r in range(tiles):
                    out_ref[cells(chunk * per + n, i, r), :] = (
                        value[n * quads : (n + 1) * quads, r * LANE : (r + 1) * LANE] * weight[i]
                    )

        @pl.when(owner)
        def _():
            for i in range(2):
                put(i, terms[i, block(chunk)] + back[i, block(chunk)])

        @pl.when(helper)
        def _():
            put(0, back[0, block(chunk)])
            put(1, back[1, block(chunk)] if quad else terms[2, block(chunk)])

    with jax.named_scope("p_drain"):
        each(plan.chunks, lambda n: both(sends_ahead(n), lambda copy: copy.wait_send()), even)
        for piece in pieces:
            for step in steps:
                spread(piece, step, False).wait_send()
    each(plan.chunks, finish, even)
    with jax.named_scope("p_drain2"):
        each(plan.chunks, lambda n: both(sends_back(n), lambda copy: copy.wait_send()), even)


def run_core(plan, mask, occupation, orbitals, kernel, tables):
    operands = [orbitals, kernel] + [tables[name] for name in NAMES]
    out = jax.ShapeDtypeStruct(orbitals.shape, F32)
    wire = pltpu.VMEM((plan.chunks, plan.parts, plan.slabs, SUB, plan.lanes), F32)
    dma = pltpu.SemaphoreType.DMA
    return pl.pallas_call(
        lambda *refs: core(plan, mask, *refs),
        out_shape=out,
        in_specs=[pl.BlockSpec(memory_space=pltpu.SMEM)]
        + [pl.BlockSpec(memory_space=pl.ANY)] * len(operands),
        out_specs=pl.BlockSpec(memory_space=pltpu.VMEM),
        scratch_shapes=[pltpu.VMEM(op.shape, op.dtype) for op in operands]
        + [
            pltpu.VMEM((5, plan.rows, plan.group), F32),
            pltpu.VMEM((3, plan.rows, plan.group), F32),
            pltpu.VMEM((2, plan.rows, plan.group), F32),
            pltpu.VMEM((plan.freqs // 2, plan.period, 2 * plan.period), F32),
            pltpu.VMEM((plan.lanes, plan.columns), F32),
            wire,
            wire,
            wire,
            wire,
            pltpu.VMEM((plan.wide // LANE, plan.parts * plan.line_rows, LANE), F32),
            dma((len(operands),)),
            dma((2, plan.chunks)),
            dma((3, plan.chunks)),
        ]
        + [dma((plan.chunks + plan.parts, plan.slabs))] * 4
        + [dma((3, plan.chunks)), dma((2, plan.chunks))],
        compiler_params=pltpu.CompilerParams(
            collective_id=mask, has_side_effects=True, vmem_limit_bytes=62 * 2**20
        ),
    )(occupation, *operands)


def local(orbitals, occupation, kernel_hat, pair_mask):
    orbit_count, planes, plane_cells = orbitals.shape
    assert orbit_count == 2 and plane_cells % LANE == 0
    slabs = lax.axis_size("slab")
    groups = lax.axis_size("grp")
    freqs, columns = kernel_hat.shape
    plan = Plan(planes, plane_cells, slabs, freqs)
    tables = {name: jnp.asarray(t) for name, t in plan.tables().items()}
    tiles = plane_cells // LANE
    flat = orbitals.reshape(2, planes, tiles, LANE).transpose(1, 2, 0, 3).reshape(-1, LANE)
    if freqs % SUB == 0:
        kernel = kernel_hat.reshape(freqs // SUB, SUB, columns // LANE, LANE)
        kernel = kernel.transpose(0, 2, 1, 3).reshape(-1, LANE)
    else:
        kernel = kernel_hat.reshape(freqs, columns // LANE, LANE)
        kernel = kernel.transpose(1, 0, 2).reshape(-1, LANE)

    def branch(mask):
        return lambda *args: run_core(plan, mask, *args, tables)

    branches = [branch(mask) for mask in range(1, groups)]
    out = lax.switch(pair_mask[0] - 1, branches, occupation, flat, kernel)
    return out.reshape(planes, tiles, 2, LANE).transpose(2, 0, 1, 3).reshape(2, planes, plane_cells)


def solution(mesh):
    return jax.shard_map(
        local,
        mesh=mesh,
        in_specs=(P("grp", "slab", None), P("grp"), P("slab", None), P()),
        out_specs=P("grp", "slab", None),
        check_vma=False,
    )
```

```python
import math

import jax
import jax.numpy as jnp
import ml_dtypes
import numpy as np
from jax import lax
from jax.experimental import pallas as pl
from jax.experimental.pallas import tpu as pltpu
from jax.sharding import PartitionSpec as P

LANE = 128
EARLY = (4, 2)
LATER = 3
SUB = 8
F32 = jnp.float32


def halves(table):
    high = table.astype(np.float32).astype(ml_dtypes.bfloat16)
    low = (table - high.astype(np.float64)).astype(ml_dtypes.bfloat16)
    return np.stack([high, low])


def padded(size, unit):
    return -(-size // unit) * unit


class Plan:
    def __init__(self, planes, plane_cells, slabs, freqs):
        self.planes, self.slabs, self.freqs = planes, slabs, freqs
        self.grid = math.isqrt(plane_cells)
        self.period = 2 * self.grid
        self.group = math.lcm(self.grid, LANE)
        self.fold = self.group // self.grid
        self.quads = self.grid // self.fold
        self.tiles = self.group // LANE
        self.rows = planes * self.quads
        self.per = math.lcm(self.period, LANE) // self.period
        self.chunks = -(-planes // self.per)
        self.wide = padded(self.period, LANE)
        self.lanes = self.per * self.period
        self.parts = -(-freqs // SUB)
        self.columns = padded(self.parts * slabs * SUB, LANE)
        self.line_rows = planes * 2 * slabs * SUB
        self.pair_starts = self.windows(self.per, self.period, self.lanes)
        assert self.period % LANE == LANE // 2 and LANE % (slabs * SUB) == 0

    def windows(self, count, step, lanes):
        return [min(j * step // LANE * LANE, lanes - self.wide) for j in range(count)]

    def sizes(self, chunk):
        even = self.planes % self.per == 0
        return self.per if even else min(self.per, self.planes - chunk * self.per)

    def wave(self, left, right):
        angle = 2.0 * math.pi / self.period * (np.outer(left, right) % self.period)
        return np.cos(angle), np.sin(angle)

    def tables(self):
        grid, period, fold, wide = self.grid, self.period, self.fold, self.wide
        columns = self.columns
        freq = np.zeros(columns, int)
        live = np.zeros(columns, bool)
        for n in range(self.parts * self.slabs * SUB):
            part, rest = divmod(n, self.slabs * SUB)
            own = part * SUB + rest % SUB
            freq[n] = rest // SUB * self.freqs + own
            live[n] = own < self.freqs
        cells = np.arange(grid)
        zc, zs = self.wave(cells, np.where(live, freq, 0))
        zc, zs = zc * live, zs * live
        zf = np.zeros((wide, 2 * columns))
        zf[:grid, :columns], zf[:grid, columns:] = zc, -zs
        zf[grid:period, :columns], zf[grid:period, columns:] = zs, zc
        zi = np.zeros((2 * columns, wide))
        zi[:columns, :grid], zi[:columns, grid:period] = zc.T / period, zs.T / period
        zi[columns:, :grid], zi[columns:, grid:period] = -zs.T / period, zc.T / period
        y_order = np.array([fold * q + j for j in range(fold) for q in range(self.quads)])
        ky_order = np.concatenate([np.arange(0, period, 2), np.arange(1, period, 2)])
        yc, ys = self.wave(y_order, ky_order)
        offsets = [j * period - self.pair_starts[j] for j in range(self.per)]
        reach = max(offsets)
        self.pair_slides = [reach - offset for offset in offsets]
        self.pair_kinds = sorted(set(offsets))
        self.pair_kind = [self.pair_kinds.index(offset) for offset in offsets]
        yf = np.zeros((reach + wide, 2 * wide))
        re, im = slice(reach, reach + grid), slice(reach + grid, reach + period)
        yf[re, :period], yf[re, wide : wide + period] = yc, -ys
        yf[im, :period], yf[im, wide : wide + period] = ys, yc
        yi = np.zeros((len(self.pair_kinds), 2 * wide, wide))
        for n, offset in enumerate(self.pair_kinds):
            re, im = slice(offset, offset + grid), slice(offset + grid, offset + period)
            yi[n, :period, re], yi[n, :period, im] = yc.T / period, ys.T / period
            yi[n, wide : wide + period, re] = -ys.T / period
            yi[n, wide : wide + period, im] = yc.T / period
        row = [
            (c, s * self.planes + x)
            for x in range(self.planes)
            for c in range(2)
            for s in range(self.slabs)
        ]
        side = np.array([r[0] for r in row])
        cos, sin = self.wave(np.arange(period), np.array([r[1] for r in row]))
        xf = np.concatenate([np.where(side == 0, cos, sin), np.where(side == 0, -sin, cos)])
        xi = np.concatenate([np.where(side == 0, cos, sin), np.where(side == 0, -sin, cos)])
        return {
            "zf": halves(zf),
            "zi": halves(zi),
            "yf": halves(yf),
            "yi": halves(yi),
            "xf": halves(xf),
            "xi": np.concatenate([halves(xi.T / period)[n] for n in (0, 1, 0)], axis=1),
        }


def mm(left, right):
    return jnp.dot(left, right, preferred_element_type=F32)


def split(value):
    high = value.astype(jnp.bfloat16)
    low = (value - high.astype(F32)).astype(jnp.bfloat16)
    return high, low


def right_mul(value, high, low):
    vh, vl = value
    return mm(vh, high) + mm(vh, low) + mm(vl, high)


def left_mul(high, low, value):
    vh, vl = value
    return mm(high, vh) + mm(low, vh) + mm(high, vl)


def each(count, body, looped):
    if looped and count > 1:
        lax.fori_loop(0, count, lambda n, carry: (body(n), carry)[1], 0)
    else:
        for n in range(count):
            body(n)


def lane_of(value):
    return lax.broadcasted_iota(jnp.int32, value.shape, 1)


def place(tiles, start, dest, index):
    shift = (dest - start) % LANE
    base = index + (start - dest + shift) // LANE
    if shift == 0:
        return tiles[base]
    below, above = (
        pltpu.roll(tiles[n], shift, 1) if 0 <= n < len(tiles) else None for n in (base - 1, base)
    )
    if below is None or above is None:
        return above if below is None else below
    return jnp.where(lane_of(above) < shift, below, above)


def join(first, second, at, index):
    low, high = index * LANE, (index + 1) * LANE
    if at <= low:
        return second(index)
    if at >= high:
        return first(index)
    value = first(index)
    return jnp.where(lane_of(value) < at - low, value, second(index))


NAMES = ("zf", "yf", "xf", "xi", "yi", "zi")


def core(plan, mask, *refs):
    occ_ref, orb_hbm, kern_hbm, *table_hbm = refs[:9]
    out_hbm = refs[9]
    raw, flat, zf, yf, xf, xi, yi, zi = refs[10:18]
    bank, terms, back, cube, turned, going, coming, leaving, landing, lines = refs[18:28]
    load_sem, zs, zr, fs, fr, bs, br, rs, rr, put_sem = refs[28:]
    slabs, parts, planes, period = plan.slabs, plan.parts, plan.planes, plan.period
    grid, quads, fold, wide, tiles = plan.grid, plan.quads, plan.fold, plan.wide, plan.tiles
    columns = plan.columns

    loads = [
        pltpu.make_async_copy(source, dest, load_sem.at[n])
        for n, (source, dest) in enumerate(
            zip([orb_hbm, kern_hbm, *table_hbm], [raw, flat, zf, yf, xf, xi, yi, zi])
        )
    ]
    loads[0].start()

    me = lax.axis_index("slab")
    g = lax.axis_index("grp")
    top = 1 << (mask.bit_length() - 1)
    quad = mask % 2 == 0
    owner = (g % 2) == ((g // top) % 2 if quad else 0)
    helper = jnp.logical_not(owner)
    mate = 1 if quad else mask
    steps = sorted(range(1, slabs), key=lambda step: -step)
    others = sorted({mate, mask, mask ^ 1} if quad else {mask})
    barrier = pltpu.get_barrier_semaphore()
    mesh_id = pl.DeviceIdType.MESH
    for other in others:
        pl.semaphore_signal(barrier, 1, device_id={"grp": g ^ other}, device_id_type=mesh_id)
    for step in steps:
        pl.semaphore_signal(barrier, 1, device_id={"slab": me ^ step}, device_id_type=mesh_id)

    def hop(source, dest, send_sem, recv_sem, other):
        return pltpu.make_async_remote_copy(
            src_ref=source,
            dst_ref=dest,
            send_sem=send_sem,
            recv_sem=recv_sem,
            device_id={"grp": g ^ other},
            device_id_type=mesh_id,
        )

    per = plan.per
    even = planes % per == 0
    last_chunk, last_part = plan.chunks - 1, parts - 1

    def aligned(start, size):
        return pl.ds(start if isinstance(start, int) else pl.multiple_of(start, SUB), size)

    def block(chunk):
        return aligned(chunk * (per * quads), plan.sizes(chunk) * quads)

    def when(condition, act):
        if isinstance(condition, bool):
            if condition:
                act()
        else:
            pl.when(condition)(act)

    def ahead(chunk, source, slot, other):
        at = block(chunk)
        return hop(bank.at[source, at], bank.at[slot, at], zs.at[0], zr.at[chunk], other)

    def answer(chunk, source, slot, other):
        at = block(chunk)
        return hop(terms.at[source, at], back.at[slot, at], rs.at[0], rr.at[chunk], other)

    def await_bytes(ref, sem):
        pltpu.make_async_copy(ref, ref, sem).wait()

    def sends_ahead(chunk):
        mine = [ahead(chunk, 0, 2, mate), ahead(chunk, 1, 3, mate)]
        theirs = [ahead(chunk, 0, 4, mask)] + ([ahead(chunk, 1, 4, mask ^ 1)] if quad else [])
        return mine, theirs

    crossing = False

    def sends_ahead_now(chunk):
        mine, theirs = sends_ahead(chunk)
        return mine, ([] if crossing else theirs)

    def sends_ahead_later(chunk):
        if not crossing:
            return

        @pl.when(helper)
        def _():
            when(chunk >= LATER, lambda: ahead(chunk - LATER, 0, 4, mask).start())

            def others_left():
                for n in range(max(0, plan.chunks - LATER), plan.chunks):
                    ahead(n, 0, 4, mask).start()

            when(chunk == last_chunk, others_left)

    def sends_back(chunk):
        mine = [answer(chunk, 2, 0, mask)]
        theirs = [answer(chunk, 0, 0, mate), answer(chunk, 1, 1, mate)]
        return mine, theirs + ([answer(chunk, 2, 1, mask ^ 1)] if quad else [])

    def both(pair, act):
        for role, copies in zip((owner, helper), pair):

            @pl.when(role)
            def _(copies=copies):
                for copy in copies:
                    act(copy)

    every = slice(None)
    ways = ((going, coming, fs, fr), (leaving, landing, bs, br))

    def whole(chunk):
        return 0, chunk, every, chunk

    def tail(part):
        return 0, last_chunk, part, last_chunk + part

    early_chunks = [last_chunk * EARLY[min(p, 1)] // 6 for p in range(last_part)]
    kept = [sum(chunk < count for count in early_chunks) for chunk in range(plan.chunks)]

    def early(part, count):
        return 1, slice(0, count), part, part

    def late(chunk, done):
        return 1, chunk, slice(done, parts), last_part + chunk

    hold = last_chunk - 1
    held = (0, hold, 0, hold), (0, hold, slice(1, parts), last_chunk + parts)
    def with_kept(chunk, act):
        for done in sorted(set(kept)):
            own = [n for n in range(plan.chunks) if kept[n] == done]
            if isinstance(chunk, int):
                if chunk in own:
                    act(late(chunk, done))
            else:
                inside = jnp.logical_and(chunk >= own[0], chunk <= own[-1])
                pl.when(inside)(lambda done=done: act(late(chunk, done)))

    def spread(piece, step):
        way, chunk, part, sem = piece
        source, dest, ss, sr = ways[way]
        peer = me ^ step
        return pltpu.make_async_remote_copy(
            src_ref=source.at[chunk, part, peer],
            dst_ref=dest.at[chunk, part, me],
            send_sem=ss.at[0],
            recv_sem=sr.at[sem],
            device_id={"slab": peer},
            device_id_type=mesh_id,
        )

    def spread_out(piece):
        for step in steps:
            spread(piece, step).start()
        way, chunk, part, _ = piece
        source, dest = ways[way][:2]
        dest[chunk, part, pl.ds(me, 1)] = source[chunk, part, pl.ds(me, 1)]

    def spread_in(piece):
        way, chunk, part, sem = piece
        _, dest, _, sr = ways[way]
        await_bytes(dest.at[chunk, part, 0 : slabs - 1], sr.at[sem])

    scale = [jnp.sqrt(0.25 * jnp.full((1, LANE), occ_ref[i], jnp.int32).astype(F32)) for i in range(2)]

    def cells(x, i, r):
        return pl.ds((x * quads * tiles + r) * 2 + i, quads, stride=2 * tiles)

    with jax.named_scope("w_raw"):
        loads[0].wait()

    def own_chunk(chunk):
        for n in range(plan.sizes(chunk)):
            x = chunk * per + n
            for i in range(2):
                for r in range(tiles):
                    bank[i, aligned(x * quads, quads), r * LANE : (r + 1) * LANE] = (
                        raw[cells(x, i, r), :] * scale[i]
                    )

        def meet():
            with jax.named_scope("w_barrier"):
                pl.semaphore_wait(barrier, len(others) + len(steps))

        when(chunk == 0, meet)
        both(sends_ahead_now(chunk), lambda copy: copy.start())

    own_chunk(0)
    for load in loads[1:]:
        load.start()
    for chunk in range(1, plan.chunks):
        own_chunk(chunk)

    with jax.named_scope("w_kern"):
        loads[1].wait()
    pairs = period // 2
    pitch = 2 * period // LANE
    if plan.freqs % SUB == 0:
        unit = SUB
        plane_start = lambda k: k // SUB * (period * period // LANE * SUB) + k % SUB
    else:
        unit = plan.freqs
        plane_start = lambda k: k

    def cube_side(k, side):
        first = plane_start(k)
        got = [flat[pl.ds(first + m * unit, pairs, stride=pitch * unit), :] for m in range(pitch)]
        n = pitch // 2
        swapped = [pltpu.roll(v, LANE // 2, 1) for v in got[n:]]
        spare = jnp.zeros((wide - period, LANE), F32)
        result = []
        for t in range(n + 1):
            odd = swapped[t]
            if t < n:
                odd = jnp.where(lane_of(odd) < LANE // 2, odd, swapped[t + 1])
            rows = [got[t], odd, spare] if side == 0 else [spare, got[t], odd]
            result.append(jnp.concatenate(rows, axis=0).T[: min(LANE, period - t * LANE)])
        return result

    def cube_pair(pair, carry):
        low, high = cube_side(2 * pair, 0), cube_side(2 * pair + 1, 1)
        meet = period // LANE * LANE
        for t, (one, two) in enumerate(zip(low, high)):
            rows = slice(t * LANE, t * LANE + one.shape[0])
            cube[pair, rows, :meet] = one[:, :meet]
            cube[pair, rows, meet:wide] = one[:, meet:] + two[:, :LANE]
            cube[pair, rows, wide:] = two[:, LANE:]
        return carry

    with jax.named_scope("p_cube"):
        lax.fori_loop(0, plan.freqs // 2, cube_pair, 0)

    left = [jnp.where(owner, i, 2 + i) for i in range(2)]
    right = jnp.where(owner, 4, 4 if quad else 1)
    for load in loads[2:]:
        load.wait()

    share = LANE // (slabs * SUB)

    def forward_z(chunk):
        with jax.named_scope("w_ahead"):
            at = block(chunk)
            pl.when(owner)(lambda: await_bytes(bank.at[4, at], zr.at[chunk]))
            heard = bank.at[2:5, at] if quad else bank.at[2:4, at]
            pl.when(helper)(lambda: await_bytes(heard, zr.at[chunk]))
        sends_ahead_later(chunk)
        at, count = block(chunk), plan.sizes(chunk)
        partner = bank[right, at]
        densities = [bank[left[i], at] * partner for i in range(2)]
        if count < per:
            turned[count * period :, :] = jnp.zeros(((per - count) * period, columns), F32)
        fields = []
        for j in range(fold):
            one, two = ([d[:, t * LANE : (t + 1) * LANE] for t in range(tiles)] for d in densities)
            fields.append(
                jnp.concatenate(
                    [
                        join(
                            lambda n: place(one, j * grid, 0, n),
                            lambda n: place(two, j * grid, grid, n),
                            grid,
                            n,
                        )
                        for n in range(wide // LANE)
                    ],
                    axis=1,
                )
            )
        total = right_mul(split(jnp.concatenate(fields, axis=0)), zf[0], zf[1])
        for j in range(fold):
            for x in range(count):
                for c in range(2):
                    first = x * period + c * grid + j * quads
                    row = (j * count + x) * quads
                    turned[first : first + quads, :] = total[
                        row : row + quads, c * columns : (c + 1) * columns
                    ]
        for col in range(0, columns, LANE):
            for r in range(0, plan.lanes, LANE):
                flip = turned[r : r + LANE, col : col + LANE].T.reshape(share, slabs, SUB, LANE)
                for n in range(min(share, parts - col // LANE * share)):
                    going[chunk, col // LANE * share + n, :, :, r : r + LANE] = flip[n]

        def by_part():
            spread_out(tail(0))
            spread_out(held[1])
            each(last_part, lambda part: spread_out(tail(part + 1)), True)

        when(chunk < hold, lambda: spread_out(whole(chunk)))
        when(chunk == hold, lambda: spread_out(held[0]))
        when(chunk == last_chunk, by_part)

    each(plan.chunks, forward_z, even)

    size = slabs * SUB
    halves_of = range(wide // LANE)

    def line(part, x, c):
        return aligned(part * plan.line_rows + (x * 2 + c) * size, size)

    def forward_y(some_chunks, some):
        for kind, offset in enumerate(plan.pair_kinds):
            own = [
                (chunk, j, part)
                for chunk in some_chunks
                for j in range(plan.sizes(chunk))
                if plan.pair_kind[j] == kind
                for part in some
            ]
            piece = []
            for chunk, j, part in own:
                lane = slice(plan.pair_starts[j], plan.pair_starts[j] + wide)
                piece.append(coming[chunk, part, :, :, lane].reshape(size, wide))
            slide = plan.pair_kinds[-1] - offset
            rows = slice(slide, slide + wide)
            piece = jnp.concatenate(piece, axis=0) if len(piece) > 1 else piece[0]
            field = right_mul(split(piece), yf[0, rows], yf[1, rows])
            for n, (chunk, j, part) in enumerate(own):
                for c in range(2):
                    for t in halves_of:
                        spot = c * wide + t * LANE
                        lines[t, line(part, chunk * per + j, c), :] = field[
                            n * size : (n + 1) * size, spot : spot + LANE
                        ]

    def some_planes(part, k, count):
        rows = [
            pl.ds(part * plan.line_rows + k + n, planes * 2 * slabs, stride=SUB)
            for n in range(count)
        ]
        two_planes = 2 * period // LANE
        field = []
        for n in range(0, count, 2):
            one, two = ([lines[t, r, :] for t in halves_of] for r in rows[n : n + 2])
            field += [
                join(lambda t: one[t], lambda t: place(two, 0, period, t), period, t)
                for t in range(two_planes)
            ]
        pair = (part * SUB + k) // 2
        kernel = []
        for n in range(count // 2):
            kernel += [
                cube[pair + n, :, t * LANE : (t + 1) * LANE] for t in range(two_planes)
            ]
        stretches = []
        for t in range(0, len(field), 2):
            some = jnp.concatenate(kernel[t : t + 2], axis=1)
            spectra = left_mul(xf[0], xf[1], split(jnp.concatenate(field[t : t + 2], axis=1)))
            spectra = [spectra[:period] * some, spectra[period:] * some]
            stretches.append(split(jnp.concatenate(spectra, axis=0)))
        field = []
        for high, low in stretches:
            done = mm(xi[...], jnp.concatenate([high, high, low], axis=0))
            field += [done[:, t : t + LANE] for t in range(0, done.shape[1], LANE)]
        for n, r in enumerate(rows):
            own = field[n // 2 * two_planes : (n // 2 + 1) * two_planes]
            for t in halves_of:
                lines[t, r, :] = own[t] if n % 2 == 0 else place(own, period, 0, t)

    def inverse_y(part):
        total = {}
        for kind in range(len(plan.pair_kinds)):
            own = [x for x in range(planes) if plan.pair_kind[x % per] == kind]
            field = [
                jnp.concatenate(
                    [lines[t, line(part, x, c), :] for c in range(2) for t in halves_of], axis=1
                )
                for x in own
            ]
            field = jnp.concatenate(field, axis=0) if len(field) > 1 else field[0]
            field = right_mul(split(field), yi[0, kind], yi[1, kind])
            for n, x in enumerate(own):
                for t in halves_of:
                    spot = (x // per, plan.pair_starts[x % per] // LANE + t)
                    term = field[n * size : (n + 1) * size, t * LANE : (t + 1) * LANE]
                    total[spot] = total[spot] + term if spot in total else term
        for chunk in range(plan.chunks):
            for t in range(plan.lanes // LANE):
                term = total.get((chunk, t))
                if term is None:
                    term = jnp.zeros((size, LANE), F32)
                leaving[chunk, part, :, :, t * LANE : (t + 1) * LANE] = term.reshape(
                    slabs, SUB, LANE
                )

    def y_chunk(chunk):
        with jax.named_scope("w_in0"):
            spread_in(whole(chunk))
        with jax.named_scope("p_y"):
            forward_y([chunk], range(parts))

    def one_part(part):
        with jax.named_scope("w_in0p"):
            when(part == 0, lambda: spread_in(held[0]))
            when(part == 1, lambda: spread_in(held[1]))
            spread_in(tail(part))
        with jax.named_scope("p_y1"):
            forward_y([hold, last_chunk], [part])
        with jax.named_scope("p_x"):
            live = SUB if plan.freqs % SUB == 0 else min(SUB, plan.freqs - part * SUB)
            some_planes(part, 0, live)
        with jax.named_scope("p_yi"):
            inverse_y(part)

            def final():
                each(plan.chunks, lambda chunk: with_kept(chunk, spread_out), True)

            for p, count in enumerate(early_chunks):
                if count:
                    when(part == p, lambda p=p, count=count: spread_out(early(p, count)))
            when(part == last_part, final)

    each(hold, y_chunk, even)
    each(parts, one_part, plan.freqs % SUB == 0)

    def inverse_z(chunk):
        with jax.named_scope("w_in1"):
            with_kept(chunk, spread_in)
        at, count = block(chunk), plan.sizes(chunk)
        for col in range(0, columns, LANE):
            for r in range(0, plan.lanes, LANE):
                got = []
                for n in range(share):
                    part = col // LANE * share + n
                    if part < parts:
                        one = landing[chunk, part, :, :, r : r + LANE].reshape(slabs * SUB, LANE)
                    else:
                        one = jnp.zeros((slabs * SUB, LANE), F32)
                    got.append(one)
                got = jnp.concatenate(got, axis=0) if share > 1 else got[0]
                turned[r : r + LANE, col : col + LANE] = got.T
        rows = []
        for j in range(fold):
            for x in range(count):
                firsts = [x * period + c * grid + j * quads for c in range(2)]
                rows.append(jnp.concatenate([turned[f : f + quads, :] for f in firsts], axis=1))
        total = right_mul(split(jnp.concatenate(rows, axis=0)), zi[0], zi[1])
        strips = [
            [
                total[j * count * quads : (j + 1) * count * quads, t * LANE : (t + 1) * LANE]
                for t in range(wide // LANE)
            ]
            for j in range(fold)
        ]

        def potential(i):
            def strip(j):
                if j == fold - 1:
                    return lambda t: place(strips[j], i * grid, j * grid, t)
                return lambda t: join(
                    lambda t: place(strips[j], i * grid, j * grid, t), strip(j + 1), (j + 1) * grid, t
                )

            return jnp.concatenate([strip(0)(t) for t in range(tiles)], axis=1)

        far = None
        partner = bank[right, at]
        for i in range(2):
            field = potential(i)
            terms[i, at] = field * partner
            term = field * bank[left[i], at]
            far = term if far is None else far + term
        terms[2, at] = far
        both(sends_back(chunk), lambda copy: copy.start())

    with jax.named_scope("w_in1"):
        for part, count in enumerate(early_chunks):
            if count:
                spread_in(early(part, count))
    each(plan.chunks, inverse_z, even)

    weight = [-1.0 / s for s in scale]

    def result(chunk):
        rows = quads * tiles * 2
        at = aligned(chunk * (per * rows), plan.sizes(chunk) * rows)
        return pltpu.make_async_copy(raw.at[at], out_hbm.at[at], put_sem.at[0])

    def finish(chunk):
        with jax.named_scope("w_back"):
            at = block(chunk)
            pl.when(owner)(lambda: await_bytes(back.at[:, at], rr.at[chunk]))
            heard = back.at[:, at] if quad else back.at[0, at]
            pl.when(helper)(lambda: await_bytes(heard, rr.at[chunk]))

        def put(i, value):
            for n in range(plan.sizes(chunk)):
                for r in range(tiles):
                    raw[cells(chunk * per + n, i, r), :] = (
                        value[n * quads : (n + 1) * quads, r * LANE : (r + 1) * LANE] * weight[i]
                    )

        @pl.when(owner)
        def _():
            for i in range(2):
                put(i, terms[i, block(chunk)] + back[i, block(chunk)])

        @pl.when(helper)
        def _():
            put(0, back[0, block(chunk)])
            put(1, back[1, block(chunk)] if quad else terms[2, block(chunk)])

        result(chunk).start()

    with jax.named_scope("p_drain"):
        pl.when(owner)(lambda: await_bytes(bank.at[0:2], zs.at[0]))
        pl.when(helper)(lambda: await_bytes(bank.at[0:2] if quad else bank.at[0], zs.at[0]))
        for source, sem in ((going, fs), (leaving, bs)):
            await_bytes(source.at[:, :, 0 : slabs - 1], sem.at[0])
    each(plan.chunks, finish, even)
    with jax.named_scope("p_drain2"):
        pl.when(owner)(lambda: await_bytes(terms.at[2], rs.at[0]))
        pl.when(helper)(lambda: await_bytes(terms.at[0:3] if quad else terms.at[0:2], rs.at[0]))
        await_bytes(raw, put_sem.at[0])


def run_core(plan, mask, occupation, orbitals, kernel, tables):
    operands = [orbitals, kernel] + [tables[name] for name in NAMES]
    out = jax.ShapeDtypeStruct(orbitals.shape, F32)
    wire = pltpu.VMEM((plan.chunks, plan.parts, plan.slabs, SUB, plan.lanes), F32)
    dma = pltpu.SemaphoreType.DMA
    return pl.pallas_call(
        lambda *refs: core(plan, mask, *refs),
        out_shape=out,
        in_specs=[pl.BlockSpec(memory_space=pltpu.SMEM)]
        + [pl.BlockSpec(memory_space=pl.ANY)] * len(operands),
        out_specs=pl.BlockSpec(memory_space=pl.ANY),
        scratch_shapes=[pltpu.VMEM(op.shape, op.dtype) for op in operands]
        + [
            pltpu.VMEM((5, plan.rows, plan.group), F32),
            pltpu.VMEM((3, plan.rows, plan.group), F32),
            pltpu.VMEM((2, plan.rows, plan.group), F32),
            pltpu.VMEM((plan.freqs // 2, plan.period, 2 * plan.period), F32),
            pltpu.VMEM((plan.lanes, plan.columns), F32),
            wire,
            wire,
            wire,
            wire,
            pltpu.VMEM((plan.wide // LANE, plan.parts * plan.line_rows, LANE), F32),
            dma((len(operands),)),
            dma((1,)),
            dma((plan.chunks,)),
            dma((1,)),
            dma((plan.chunks + plan.parts,)),
            dma((1,)),
            dma((plan.chunks + plan.parts,)),
            dma((1,)),
            dma((plan.chunks,)),
            dma((1,)),
        ],
        compiler_params=pltpu.CompilerParams(
            collective_id=mask, has_side_effects=True, vmem_limit_bytes=62 * 2**20
        ),
    )(occupation, *operands)


def local(orbitals, occupation, kernel_hat, pair_mask):
    orbit_count, planes, plane_cells = orbitals.shape
    assert orbit_count == 2 and plane_cells % LANE == 0
    slabs = lax.axis_size("slab")
    groups = lax.axis_size("grp")
    freqs, columns = kernel_hat.shape
    plan = Plan(planes, plane_cells, slabs, freqs)
    tables = {name: jnp.asarray(t) for name, t in plan.tables().items()}
    tiles = plane_cells // LANE
    flat = orbitals.reshape(2, planes, tiles, LANE).transpose(1, 2, 0, 3).reshape(-1, LANE)
    if freqs % SUB == 0:
        kernel = kernel_hat.reshape(freqs // SUB, SUB, columns // LANE, LANE)
        kernel = kernel.transpose(0, 2, 1, 3).reshape(-1, LANE)
    else:
        kernel = kernel_hat.reshape(freqs, columns // LANE, LANE)
        kernel = kernel.transpose(1, 0, 2).reshape(-1, LANE)

    def branch(mask):
        return lambda *args: run_core(plan, mask, *args, tables)

    branches = [branch(mask) for mask in range(1, groups)]
    out = lax.switch(pair_mask[0] - 1, branches, occupation, flat, kernel)
    return out.reshape(planes, tiles, 2, LANE).transpose(2, 0, 1, 3).reshape(2, planes, plane_cells)


def solution(mesh):
    return jax.shard_map(
        local,
        mesh=mesh,
        in_specs=(P("grp", "slab", None), P("grp"), P("slab", None), P()),
        out_specs=P("grp", "slab", None),
        check_vma=False,
    )
```

```python
import math

import jax
import jax.numpy as jnp
import ml_dtypes
import numpy as np
from jax import lax
from jax.experimental import pallas as pl
from jax.experimental.pallas import tpu as pltpu
from jax.sharding import PartitionSpec as P

LANE = 128
EARLY = (3, 2)
LATER = 3
SUB = 8
F32 = jnp.float32


def halves(table):
    high = table.astype(np.float32).astype(ml_dtypes.bfloat16)
    low = (table - high.astype(np.float64)).astype(ml_dtypes.bfloat16)
    return np.stack([high, low])


def padded(size, unit):
    return -(-size // unit) * unit


class Plan:
    def __init__(self, planes, plane_cells, slabs, freqs):
        self.planes, self.slabs, self.freqs = planes, slabs, freqs
        self.grid = math.isqrt(plane_cells)
        self.period = 2 * self.grid
        self.group = math.lcm(self.grid, LANE)
        self.fold = self.group // self.grid
        self.quads = self.grid // self.fold
        self.tiles = self.group // LANE
        self.rows = planes * self.quads
        self.per = math.lcm(self.period, LANE) // self.period
        self.chunks = -(-planes // self.per)
        self.wide = padded(self.period, LANE)
        self.lanes = self.per * self.period
        self.parts = -(-freqs // SUB)
        self.columns = padded(self.parts * slabs * SUB, LANE)
        self.line_rows = planes * 2 * slabs * SUB
        self.pair_starts = self.windows(self.per, self.period, self.lanes)
        assert self.period % LANE == LANE // 2 and LANE % (slabs * SUB) == 0

    def windows(self, count, step, lanes):
        return [min(j * step // LANE * LANE, lanes - self.wide) for j in range(count)]

    def sizes(self, chunk):
        even = self.planes % self.per == 0
        return self.per if even else min(self.per, self.planes - chunk * self.per)

    def wave(self, left, right):
        angle = 2.0 * math.pi / self.period * (np.outer(left, right) % self.period)
        return np.cos(angle), np.sin(angle)

    def tables(self):
        grid, period, fold, wide = self.grid, self.period, self.fold, self.wide
        columns = self.columns
        freq = np.zeros(columns, int)
        live = np.zeros(columns, bool)
        for n in range(self.parts * self.slabs * SUB):
            part, rest = divmod(n, self.slabs * SUB)
            own = part * SUB + rest % SUB
            freq[n] = rest // SUB * self.freqs + own
            live[n] = own < self.freqs
        cells = np.arange(grid)
        zc, zs = self.wave(cells, np.where(live, freq, 0))
        zc, zs = zc * live, zs * live
        zf = np.zeros((wide, 2 * columns))
        zf[:grid, :columns], zf[:grid, columns:] = zc, -zs
        zf[grid:period, :columns], zf[grid:period, columns:] = zs, zc
        zi = np.zeros((2 * columns, wide))
        zi[:columns, :grid], zi[:columns, grid:period] = zc.T / period, zs.T / period
        zi[columns:, :grid], zi[columns:, grid:period] = -zs.T / period, zc.T / period
        y_order = np.array([fold * q + j for j in range(fold) for q in range(self.quads)])
        ky_order = np.concatenate([np.arange(0, period, 2), np.arange(1, period, 2)])
        yc, ys = self.wave(y_order, ky_order)
        offsets = [j * period - self.pair_starts[j] for j in range(self.per)]
        reach = max(offsets)
        self.pair_slides = [reach - offset for offset in offsets]
        self.pair_kinds = sorted(set(offsets))
        self.pair_kind = [self.pair_kinds.index(offset) for offset in offsets]
        yf = np.zeros((reach + wide, 2 * wide))
        re, im = slice(reach, reach + grid), slice(reach + grid, reach + period)
        yf[re, :period], yf[re, wide : wide + period] = yc, -ys
        yf[im, :period], yf[im, wide : wide + period] = ys, yc
        yi = np.zeros((len(self.pair_kinds), 2 * wide, wide))
        for n, offset in enumerate(self.pair_kinds):
            re, im = slice(offset, offset + grid), slice(offset + grid, offset + period)
            yi[n, :period, re], yi[n, :period, im] = yc.T / period, ys.T / period
            yi[n, wide : wide + period, re] = -ys.T / period
            yi[n, wide : wide + period, im] = yc.T / period
        row = [
            (c, s * self.planes + x)
            for x in range(self.planes)
            for c in range(2)
            for s in range(self.slabs)
        ]
        side = np.array([r[0] for r in row])
        cos, sin = self.wave(np.arange(period), np.array([r[1] for r in row]))
        xf = np.concatenate([np.where(side == 0, cos, sin), np.where(side == 0, -sin, cos)])
        xi = np.concatenate([np.where(side == 0, cos, sin), np.where(side == 0, -sin, cos)])
        return {
            "zf": halves(zf),
            "zi": halves(zi),
            "yf": halves(yf),
            "yi": halves(yi),
            "xf": halves(xf),
            "xi": np.concatenate([halves(xi.T / period)[n] for n in (0, 1, 0)], axis=1),
        }


def mm(left, right):
    return jnp.dot(left, right, preferred_element_type=F32)


def split(value):
    high = value.astype(jnp.bfloat16)
    low = (value - high.astype(F32)).astype(jnp.bfloat16)
    return high, low


def right_mul(value, high, low):
    vh, vl = value
    return mm(vh, high) + mm(vh, low) + mm(vl, high)


def left_mul(high, low, value):
    vh, vl = value
    return mm(high, vh) + mm(low, vh) + mm(high, vl)


def each(count, body, looped):
    if looped and count > 1:
        lax.fori_loop(0, count, lambda n, carry: (body(n), carry)[1], 0)
    else:
        for n in range(count):
            body(n)


def lane_of(value):
    return lax.broadcasted_iota(jnp.int32, value.shape, 1)


def place(tiles, start, dest, index):
    shift = (dest - start) % LANE
    base = index + (start - dest + shift) // LANE
    if shift == 0:
        return tiles[base]
    below, above = (
        pltpu.roll(tiles[n], shift, 1) if 0 <= n < len(tiles) else None for n in (base - 1, base)
    )
    if below is None or above is None:
        return above if below is None else below
    return jnp.where(lane_of(above) < shift, below, above)


def join(first, second, at, index):
    low, high = index * LANE, (index + 1) * LANE
    if at <= low:
        return second(index)
    if at >= high:
        return first(index)
    value = first(index)
    return jnp.where(lane_of(value) < at - low, value, second(index))


NAMES = ("zf", "yf", "xf", "xi", "yi", "zi")


def core(plan, mask, *refs):
    occ_ref, orb_hbm, kern_hbm, *table_hbm = refs[:9]
    out_hbm = refs[9]
    raw, flat, zf, yf, xf, xi, yi, zi = refs[10:18]
    bank, terms, back, cube, turned, going, coming, leaving, landing, lines = refs[18:28]
    load_sem, zs, zr, fs, fr, bs, br, rs, rr, put_sem = refs[28:]
    slabs, parts, planes, period = plan.slabs, plan.parts, plan.planes, plan.period
    grid, quads, fold, wide, tiles = plan.grid, plan.quads, plan.fold, plan.wide, plan.tiles
    columns = plan.columns

    loads = [
        pltpu.make_async_copy(source, dest, load_sem.at[n])
        for n, (source, dest) in enumerate(
            zip([orb_hbm, kern_hbm, *table_hbm], [raw, flat, zf, yf, xf, xi, yi, zi])
        )
    ]
    loads[0].start()

    me = lax.axis_index("slab")
    g = lax.axis_index("grp")
    top = 1 << (mask.bit_length() - 1)
    quad = mask % 2 == 0
    owner = (g % 2) == ((g // top) % 2 if quad else 0)
    helper = jnp.logical_not(owner)
    mate = 1 if quad else mask
    steps = sorted(range(1, slabs), key=lambda step: -step)
    others = sorted({mate, mask, mask ^ 1} if quad else {mask})
    barrier = pltpu.get_barrier_semaphore()
    mesh_id = pl.DeviceIdType.MESH
    for other in others:
        pl.semaphore_signal(barrier, 1, device_id={"grp": g ^ other}, device_id_type=mesh_id)
    for step in steps:
        pl.semaphore_signal(barrier, 1, device_id={"slab": me ^ step}, device_id_type=mesh_id)

    def hop(source, dest, send_sem, recv_sem, other):
        return pltpu.make_async_remote_copy(
            src_ref=source,
            dst_ref=dest,
            send_sem=send_sem,
            recv_sem=recv_sem,
            device_id={"grp": g ^ other},
            device_id_type=mesh_id,
        )

    per = plan.per
    even = planes % per == 0
    last_chunk, last_part = plan.chunks - 1, parts - 1

    def aligned(start, size):
        return pl.ds(start if isinstance(start, int) else pl.multiple_of(start, SUB), size)

    def block(chunk):
        return aligned(chunk * (per * quads), plan.sizes(chunk) * quads)

    def when(condition, act):
        if isinstance(condition, bool):
            if condition:
                act()
        else:
            pl.when(condition)(act)

    def ahead(chunk, source, slot, other):
        at = block(chunk)
        return hop(bank.at[source, at], bank.at[slot, at], zs.at[0], zr.at[chunk], other)

    def answer(chunk, source, slot, other):
        at = block(chunk)
        return hop(terms.at[source, at], back.at[slot, at], rs.at[0], rr.at[chunk], other)

    def await_bytes(ref, sem):
        pltpu.make_async_copy(ref, ref, sem).wait()

    def sends_ahead(chunk):
        mine = [ahead(chunk, 0, 2, mate), ahead(chunk, 1, 3, mate)]
        theirs = [ahead(chunk, 0, 4, mask)] + ([ahead(chunk, 1, 4, mask ^ 1)] if quad else [])
        return mine, theirs

    crossing = False

    def sends_ahead_now(chunk):
        mine, theirs = sends_ahead(chunk)
        return mine, ([] if crossing else theirs)

    def sends_ahead_later(chunk):
        if not crossing:
            return

        @pl.when(helper)
        def _():
            when(chunk >= LATER, lambda: ahead(chunk - LATER, 0, 4, mask).start())

            def others_left():
                for n in range(max(0, plan.chunks - LATER), plan.chunks):
                    ahead(n, 0, 4, mask).start()

            when(chunk == last_chunk, others_left)

    def sends_back(chunk):
        mine = [answer(chunk, 2, 0, mask)]
        theirs = [answer(chunk, 0, 0, mate), answer(chunk, 1, 1, mate)]
        return mine, theirs + ([answer(chunk, 2, 1, mask ^ 1)] if quad else [])

    def both(pair, act):
        for role, copies in zip((owner, helper), pair):

            @pl.when(role)
            def _(copies=copies):
                for copy in copies:
                    act(copy)

    every = slice(None)
    ways = ((going, coming, fs, fr), (leaving, landing, bs, br))

    def whole(chunk):
        return 0, chunk, every, chunk

    def tail(part):
        return 0, last_chunk, part, last_chunk + part

    early_chunks = [max(1, plan.chunks * EARLY[min(p, 1)] // 6) for p in range(last_part)]
    kept = [sum(chunk < count for count in early_chunks) for chunk in range(plan.chunks)]

    def early(part, count):
        return 1, slice(0, count), part, part

    def late(chunk, done):
        return 1, chunk, slice(done, parts), last_part + chunk

    hold = last_chunk - 1
    held = (0, hold, 0, hold), (0, hold, slice(1, parts), last_chunk + parts)
    def with_kept(chunk, act):
        for done in sorted(set(kept)):
            own = [n for n in range(plan.chunks) if kept[n] == done]
            if isinstance(chunk, int):
                if chunk in own:
                    act(late(chunk, done))
            else:
                inside = jnp.logical_and(chunk >= own[0], chunk <= own[-1])
                pl.when(inside)(lambda done=done: act(late(chunk, done)))

    def spread(piece, step):
        way, chunk, part, sem = piece
        source, dest, ss, sr = ways[way]
        peer = me ^ step
        return pltpu.make_async_remote_copy(
            src_ref=source.at[chunk, part, peer],
            dst_ref=dest.at[chunk, part, me],
            send_sem=ss.at[0],
            recv_sem=sr.at[sem],
            device_id={"slab": peer},
            device_id_type=mesh_id,
        )

    def spread_out(piece):
        for step in steps:
            spread(piece, step).start()
        way, chunk, part, _ = piece
        source, dest = ways[way][:2]
        dest[chunk, part, pl.ds(me, 1)] = source[chunk, part, pl.ds(me, 1)]

    def spread_in(piece):
        way, chunk, part, sem = piece
        _, dest, _, sr = ways[way]
        await_bytes(dest.at[chunk, part, 0 : slabs - 1], sr.at[sem])

    scale = [jnp.sqrt(0.25 * jnp.full((1, LANE), occ_ref[i], jnp.int32).astype(F32)) for i in range(2)]

    def cells(x, i, r):
        return pl.ds((x * quads * tiles + r) * 2 + i, quads, stride=2 * tiles)

    with jax.named_scope("w_raw"):
        loads[0].wait()

    def own_chunk(chunk):
        for n in range(plan.sizes(chunk)):
            x = chunk * per + n
            for i in range(2):
                for r in range(tiles):
                    bank[i, aligned(x * quads, quads), r * LANE : (r + 1) * LANE] = (
                        raw[cells(x, i, r), :] * scale[i]
                    )

        def meet():
            with jax.named_scope("w_barrier"):
                pl.semaphore_wait(barrier, len(others) + len(steps))

        when(chunk == 0, meet)
        both(sends_ahead_now(chunk), lambda copy: copy.start())

    own_chunk(0)
    for load in loads[1:]:
        load.start()
    for chunk in range(1, plan.chunks):
        own_chunk(chunk)

    with jax.named_scope("w_kern"):
        loads[1].wait()
    pairs = period // 2
    pitch = 2 * period // LANE
    if plan.freqs % SUB == 0:
        unit = SUB
        plane_start = lambda k: k // SUB * (period * period // LANE * SUB) + k % SUB
    else:
        unit = plan.freqs
        plane_start = lambda k: k

    def cube_side(k, side):
        first = plane_start(k)
        got = [flat[pl.ds(first + m * unit, pairs, stride=pitch * unit), :] for m in range(pitch)]
        n = pitch // 2
        swapped = [pltpu.roll(v, LANE // 2, 1) for v in got[n:]]
        spare = jnp.zeros((wide - period, LANE), F32)
        result = []
        for t in range(n + 1):
            odd = swapped[t]
            if t < n:
                odd = jnp.where(lane_of(odd) < LANE // 2, odd, swapped[t + 1])
            rows = [got[t], odd, spare] if side == 0 else [spare, got[t], odd]
            result.append(jnp.concatenate(rows, axis=0).T[: min(LANE, period - t * LANE)])
        return result

    def cube_pair(pair, carry):
        low, high = cube_side(2 * pair, 0), cube_side(2 * pair + 1, 1)
        meet = period // LANE * LANE
        for t, (one, two) in enumerate(zip(low, high)):
            rows = slice(t * LANE, t * LANE + one.shape[0])
            cube[pair, rows, :meet] = one[:, :meet]
            cube[pair, rows, meet:wide] = one[:, meet:] + two[:, :LANE]
            cube[pair, rows, wide:] = two[:, LANE:]
        return carry

    with jax.named_scope("p_cube"):
        lax.fori_loop(0, plan.freqs // 2, cube_pair, 0)

    left = [jnp.where(owner, i, 2 + i) for i in range(2)]
    right = jnp.where(owner, 4, 4 if quad else 1)
    for load in loads[2:]:
        load.wait()

    share = LANE // (slabs * SUB)

    def forward_z(chunk):
        with jax.named_scope("w_ahead"):
            at = block(chunk)
            pl.when(owner)(lambda: await_bytes(bank.at[4, at], zr.at[chunk]))
            heard = bank.at[2:5, at] if quad else bank.at[2:4, at]
            pl.when(helper)(lambda: await_bytes(heard, zr.at[chunk]))
        sends_ahead_later(chunk)
        at, count = block(chunk), plan.sizes(chunk)
        partner = bank[right, at]
        densities = [bank[left[i], at] * partner for i in range(2)]
        if count < per:
            turned[count * period :, :] = jnp.zeros(((per - count) * period, columns), F32)
        fields = []
        for j in range(fold):
            one, two = ([d[:, t * LANE : (t + 1) * LANE] for t in range(tiles)] for d in densities)
            fields.append(
                jnp.concatenate(
                    [
                        join(
                            lambda n: place(one, j * grid, 0, n),
                            lambda n: place(two, j * grid, grid, n),
                            grid,
                            n,
                        )
                        for n in range(wide // LANE)
                    ],
                    axis=1,
                )
            )
        total = right_mul(split(jnp.concatenate(fields, axis=0)), zf[0], zf[1])
        for j in range(fold):
            for x in range(count):
                for c in range(2):
                    first = x * period + c * grid + j * quads
                    row = (j * count + x) * quads
                    turned[first : first + quads, :] = total[
                        row : row + quads, c * columns : (c + 1) * columns
                    ]
        for col in range(0, columns, LANE):
            for r in range(0, plan.lanes, LANE):
                flip = turned[r : r + LANE, col : col + LANE].T.reshape(share, slabs, SUB, LANE)
                for n in range(min(share, parts - col // LANE * share)):
                    going[chunk, col // LANE * share + n, :, :, r : r + LANE] = flip[n]

        def by_part():
            spread_out(tail(0))
            spread_out(held[1])
            each(last_part, lambda part: spread_out(tail(part + 1)), True)

        when(chunk < hold, lambda: spread_out(whole(chunk)))
        when(chunk == hold, lambda: spread_out(held[0]))
        when(chunk == last_chunk, by_part)

    each(plan.chunks, forward_z, even)

    size = slabs * SUB
    halves_of = range(wide // LANE)

    def line(part, x, c):
        return aligned(part * plan.line_rows + (x * 2 + c) * size, size)

    def forward_y(some_chunks, some):
        for kind, offset in enumerate(plan.pair_kinds):
            own = [
                (chunk, j, part)
                for chunk in some_chunks
                for j in range(plan.sizes(chunk))
                if plan.pair_kind[j] == kind
                for part in some
            ]
            piece = []
            for chunk, j, part in own:
                lane = slice(plan.pair_starts[j], plan.pair_starts[j] + wide)
                piece.append(coming[chunk, part, :, :, lane].reshape(size, wide))
            slide = plan.pair_kinds[-1] - offset
            rows = slice(slide, slide + wide)
            piece = jnp.concatenate(piece, axis=0) if len(piece) > 1 else piece[0]
            field = right_mul(split(piece), yf[0, rows], yf[1, rows])
            for n, (chunk, j, part) in enumerate(own):
                for c in range(2):
                    for t in halves_of:
                        spot = c * wide + t * LANE
                        lines[t, line(part, chunk * per + j, c), :] = field[
                            n * size : (n + 1) * size, spot : spot + LANE
                        ]

    def some_planes(part, k, count):
        rows = [
            pl.ds(part * plan.line_rows + k + n, planes * 2 * slabs, stride=SUB)
            for n in range(count)
        ]
        two_planes = 2 * period // LANE
        field = []
        for n in range(0, count, 2):
            one, two = ([lines[t, r, :] for t in halves_of] for r in rows[n : n + 2])
            field += [
                join(lambda t: one[t], lambda t: place(two, 0, period, t), period, t)
                for t in range(two_planes)
            ]
        pair = (part * SUB + k) // 2
        kernel = []
        for n in range(count // 2):
            kernel += [
                cube[pair + n, :, t * LANE : (t + 1) * LANE] for t in range(two_planes)
            ]
        stretches = []
        for t in range(0, len(field), 2):
            some = jnp.concatenate(kernel[t : t + 2], axis=1)
            spectra = left_mul(xf[0], xf[1], split(jnp.concatenate(field[t : t + 2], axis=1)))
            spectra = [spectra[:period] * some, spectra[period:] * some]
            stretches.append(split(jnp.concatenate(spectra, axis=0)))
        field = []
        for high, low in stretches:
            done = mm(xi[...], jnp.concatenate([high, high, low], axis=0))
            field += [done[:, t : t + LANE] for t in range(0, done.shape[1], LANE)]
        for n, r in enumerate(rows):
            own = field[n // 2 * two_planes : (n // 2 + 1) * two_planes]
            for t in halves_of:
                lines[t, r, :] = own[t] if n % 2 == 0 else place(own, period, 0, t)

    def inverse_y(items):
        total = {}
        for kind in range(len(plan.pair_kinds)):
            own = [
                (part, chunk, j)
                for part, chunk in items
                for j in range(plan.sizes(chunk))
                if plan.pair_kind[j] == kind
            ]
            if not own:
                continue
            field = [
                jnp.concatenate(
                    [
                        lines[t, line(part, chunk * per + j, c), :]
                        for c in range(2)
                        for t in halves_of
                    ],
                    axis=1,
                )
                for part, chunk, j in own
            ]
            field = jnp.concatenate(field, axis=0) if len(field) > 1 else field[0]
            field = right_mul(split(field), yi[0, kind], yi[1, kind])
            for n, (part, chunk, j) in enumerate(own):
                for t in halves_of:
                    spot = (part, chunk, plan.pair_starts[j] // LANE + t)
                    term = field[n * size : (n + 1) * size, t * LANE : (t + 1) * LANE]
                    total[spot] = total[spot] + term if spot in total else term
        for part, chunk in items:
            for t in range(plan.lanes // LANE):
                term = total.get((part, chunk, t))
                if term is None:
                    term = jnp.zeros((size, LANE), F32)
                leaving[chunk, part, :, :, t * LANE : (t + 1) * LANE] = term.reshape(
                    slabs, SUB, LANE
                )

    def y_chunk(chunk):
        with jax.named_scope("w_in0"):
            spread_in(whole(chunk))
        with jax.named_scope("p_y"):
            forward_y([chunk], range(parts))

    def one_part(part):
        with jax.named_scope("w_in0p"):
            when(part == 0, lambda: spread_in(held[0]))
            when(part == 1, lambda: spread_in(held[1]))
            spread_in(tail(part))
        with jax.named_scope("p_y1"):
            forward_y([hold, last_chunk], [part])
        with jax.named_scope("p_x"):
            live = SUB if plan.freqs % SUB == 0 else min(SUB, plan.freqs - part * SUB)
            some_planes(part, 0, live)
        with jax.named_scope("p_yi"):
            for p, count in enumerate(early_chunks):

                def leave(p=p, count=count):
                    inverse_y([(p, chunk) for chunk in range(count)])
                    spread_out(early(p, count))

                when(part == p, leave)

    each(hold, y_chunk, even)
    each(parts, one_part, plan.freqs % SUB == 0)
    with jax.named_scope("p_yl"):
        for first, end in ((0, 1), (1, 3), (3, plan.chunks)):
            some = range(first, min(end, plan.chunks))
            if some:
                inverse_y([(p, chunk) for chunk in some for p in range(kept[chunk], parts)])
                each(len(some), lambda n: with_kept(first + n, spread_out), False)

    def inverse_z(chunk):
        with jax.named_scope("w_in1"):
            with_kept(chunk, spread_in)
        at, count = block(chunk), plan.sizes(chunk)
        for col in range(0, columns, LANE):
            for r in range(0, plan.lanes, LANE):
                got = []
                for n in range(share):
                    part = col // LANE * share + n
                    if part < parts:
                        one = landing[chunk, part, :, :, r : r + LANE].reshape(slabs * SUB, LANE)
                    else:
                        one = jnp.zeros((slabs * SUB, LANE), F32)
                    got.append(one)
                got = jnp.concatenate(got, axis=0) if share > 1 else got[0]
                turned[r : r + LANE, col : col + LANE] = got.T
        rows = []
        for j in range(fold):
            for x in range(count):
                firsts = [x * period + c * grid + j * quads for c in range(2)]
                rows.append(jnp.concatenate([turned[f : f + quads, :] for f in firsts], axis=1))
        total = right_mul(split(jnp.concatenate(rows, axis=0)), zi[0], zi[1])
        strips = [
            [
                total[j * count * quads : (j + 1) * count * quads, t * LANE : (t + 1) * LANE]
                for t in range(wide // LANE)
            ]
            for j in range(fold)
        ]

        def potential(i):
            def strip(j):
                if j == fold - 1:
                    return lambda t: place(strips[j], i * grid, j * grid, t)
                return lambda t: join(
                    lambda t: place(strips[j], i * grid, j * grid, t), strip(j + 1), (j + 1) * grid, t
                )

            return jnp.concatenate([strip(0)(t) for t in range(tiles)], axis=1)

        far = None
        partner = bank[right, at]
        for i in range(2):
            field = potential(i)
            terms[i, at] = field * partner
            term = field * bank[left[i], at]
            far = term if far is None else far + term
        terms[2, at] = far
        both(sends_back(chunk), lambda copy: copy.start())

    with jax.named_scope("w_in1"):
        for part, count in enumerate(early_chunks):
            spread_in(early(part, count))
    each(plan.chunks, inverse_z, even)

    weight = [-1.0 / s for s in scale]

    def result(chunk):
        rows = quads * tiles * 2
        at = aligned(chunk * (per * rows), plan.sizes(chunk) * rows)
        return pltpu.make_async_copy(raw.at[at], out_hbm.at[at], put_sem.at[0])

    def finish(chunk):
        with jax.named_scope("w_back"):
            at = block(chunk)
            pl.when(owner)(lambda: await_bytes(back.at[:, at], rr.at[chunk]))
            heard = back.at[:, at] if quad else back.at[0, at]
            pl.when(helper)(lambda: await_bytes(heard, rr.at[chunk]))

        def put(i, value):
            for n in range(plan.sizes(chunk)):
                for r in range(tiles):
                    raw[cells(chunk * per + n, i, r), :] = (
                        value[n * quads : (n + 1) * quads, r * LANE : (r + 1) * LANE] * weight[i]
                    )

        @pl.when(owner)
        def _():
            for i in range(2):
                put(i, terms[i, block(chunk)] + back[i, block(chunk)])

        @pl.when(helper)
        def _():
            put(0, back[0, block(chunk)])
            put(1, back[1, block(chunk)] if quad else terms[2, block(chunk)])

        result(chunk).start()

    with jax.named_scope("p_drain"):
        pl.when(owner)(lambda: await_bytes(bank.at[0:2], zs.at[0]))
        pl.when(helper)(lambda: await_bytes(bank.at[0:2] if quad else bank.at[0], zs.at[0]))
        for source, sem in ((going, fs), (leaving, bs)):
            await_bytes(source.at[:, :, 0 : slabs - 1], sem.at[0])
    each(plan.chunks, finish, even)
    with jax.named_scope("p_drain2"):
        pl.when(owner)(lambda: await_bytes(terms.at[2], rs.at[0]))
        pl.when(helper)(lambda: await_bytes(terms.at[0:3] if quad else terms.at[0:2], rs.at[0]))
        await_bytes(raw, put_sem.at[0])


def run_core(plan, mask, occupation, orbitals, kernel, tables):
    operands = [orbitals, kernel] + [tables[name] for name in NAMES]
    out = jax.ShapeDtypeStruct(orbitals.shape, F32)
    wire = pltpu.VMEM((plan.chunks, plan.parts, plan.slabs, SUB, plan.lanes), F32)
    dma = pltpu.SemaphoreType.DMA
    return pl.pallas_call(
        lambda *refs: core(plan, mask, *refs),
        out_shape=out,
        in_specs=[pl.BlockSpec(memory_space=pltpu.SMEM)]
        + [pl.BlockSpec(memory_space=pl.ANY)] * len(operands),
        out_specs=pl.BlockSpec(memory_space=pl.ANY),
        scratch_shapes=[pltpu.VMEM(op.shape, op.dtype) for op in operands]
        + [
            pltpu.VMEM((5, plan.rows, plan.group), F32),
            pltpu.VMEM((3, plan.rows, plan.group), F32),
            pltpu.VMEM((2, plan.rows, plan.group), F32),
            pltpu.VMEM((plan.freqs // 2, plan.period, 2 * plan.period), F32),
            pltpu.VMEM((plan.lanes, plan.columns), F32),
            wire,
            wire,
            wire,
            wire,
            pltpu.VMEM((plan.wide // LANE, plan.parts * plan.line_rows, LANE), F32),
            dma((len(operands),)),
            dma((1,)),
            dma((plan.chunks,)),
            dma((1,)),
            dma((plan.chunks + plan.parts,)),
            dma((1,)),
            dma((plan.chunks + plan.parts,)),
            dma((1,)),
            dma((plan.chunks,)),
            dma((1,)),
        ],
        compiler_params=pltpu.CompilerParams(
            collective_id=mask, has_side_effects=True, vmem_limit_bytes=62 * 2**20
        ),
    )(occupation, *operands)


def local(orbitals, occupation, kernel_hat, pair_mask):
    orbit_count, planes, plane_cells = orbitals.shape
    assert orbit_count == 2 and plane_cells % LANE == 0
    slabs = lax.axis_size("slab")
    groups = lax.axis_size("grp")
    freqs, columns = kernel_hat.shape
    plan = Plan(planes, plane_cells, slabs, freqs)
    tables = {name: jnp.asarray(t) for name, t in plan.tables().items()}
    tiles = plane_cells // LANE
    flat = orbitals.reshape(2, planes, tiles, LANE).transpose(1, 2, 0, 3).reshape(-1, LANE)
    if freqs % SUB == 0:
        kernel = kernel_hat.reshape(freqs // SUB, SUB, columns // LANE, LANE)
        kernel = kernel.transpose(0, 2, 1, 3).reshape(-1, LANE)
    else:
        kernel = kernel_hat.reshape(freqs, columns // LANE, LANE)
        kernel = kernel.transpose(1, 0, 2).reshape(-1, LANE)

    def branch(mask):
        return lambda *args: run_core(plan, mask, *args, tables)

    branches = [branch(mask) for mask in range(1, groups)]
    out = lax.switch(pair_mask[0] - 1, branches, occupation, flat, kernel)
    return out.reshape(planes, tiles, 2, LANE).transpose(2, 0, 1, 3).reshape(2, planes, plane_cells)


def solution(mesh):
    return jax.shard_map(
        local,
        mesh=mesh,
        in_specs=(P("grp", "slab", None), P("grp"), P("slab", None), P()),
        out_specs=P("grp", "slab", None),
        check_vma=False,
    )
```

```python
import math

import jax
import jax.numpy as jnp
import ml_dtypes
import numpy as np
from jax import lax
from jax.experimental import pallas as pl
from jax.experimental.pallas import tpu as pltpu
from jax.sharding import PartitionSpec as P

LANE = 128
EARLY = (3, 2)
LATER = 3
SUB = 8
F32 = jnp.float32


def halves(table):
    high = table.astype(np.float32).astype(ml_dtypes.bfloat16)
    low = (table - high.astype(np.float64)).astype(ml_dtypes.bfloat16)
    return np.stack([high, low])


def padded(size, unit):
    return -(-size // unit) * unit


class Plan:
    def __init__(self, planes, plane_cells, slabs, freqs):
        self.planes, self.slabs, self.freqs = planes, slabs, freqs
        self.grid = math.isqrt(plane_cells)
        self.period = 2 * self.grid
        self.group = math.lcm(self.grid, LANE)
        self.fold = self.group // self.grid
        self.quads = self.grid // self.fold
        self.tiles = self.group // LANE
        self.rows = planes * self.quads
        self.per = math.lcm(self.period, LANE) // self.period
        self.chunks = -(-planes // self.per)
        self.wide = padded(self.period, LANE)
        self.lanes = self.per * self.period
        self.parts = -(-freqs // SUB)
        self.columns = padded(self.parts * slabs * SUB, LANE)
        self.line_rows = planes * 2 * slabs * SUB
        self.pair_starts = self.windows(self.per, self.period, self.lanes)
        assert self.period % LANE == LANE // 2 and LANE % (slabs * SUB) == 0

    def windows(self, count, step, lanes):
        return [min(j * step // LANE * LANE, lanes - self.wide) for j in range(count)]

    def sizes(self, chunk):
        even = self.planes % self.per == 0
        return self.per if even else min(self.per, self.planes - chunk * self.per)

    def wave(self, left, right):
        angle = 2.0 * math.pi / self.period * (np.outer(left, right) % self.period)
        return np.cos(angle), np.sin(angle)

    def tables(self):
        grid, period, fold, wide = self.grid, self.period, self.fold, self.wide
        columns = self.columns
        freq = np.zeros(columns, int)
        live = np.zeros(columns, bool)
        for n in range(self.parts * self.slabs * SUB):
            part, rest = divmod(n, self.slabs * SUB)
            own = part * SUB + rest % SUB
            freq[n] = rest // SUB * self.freqs + own
            live[n] = own < self.freqs
        cells = np.arange(grid)
        zc, zs = self.wave(cells, np.where(live, freq, 0))
        zc, zs = zc * live, zs * live
        zf = np.zeros((wide, 2 * columns))
        zf[:grid, :columns], zf[:grid, columns:] = zc, -zs
        zf[grid:period, :columns], zf[grid:period, columns:] = zs, zc
        zi = np.zeros((2 * columns, wide))
        zi[:columns, :grid], zi[:columns, grid:period] = zc.T / period, zs.T / period
        zi[columns:, :grid], zi[columns:, grid:period] = -zs.T / period, zc.T / period
        y_order = np.array([fold * q + j for j in range(fold) for q in range(self.quads)])
        ky_order = np.concatenate([np.arange(0, period, 2), np.arange(1, period, 2)])
        yc, ys = self.wave(y_order, ky_order)
        offsets = [j * period - self.pair_starts[j] for j in range(self.per)]
        reach = max(offsets)
        self.pair_slides = [reach - offset for offset in offsets]
        self.pair_kinds = sorted(set(offsets))
        self.pair_kind = [self.pair_kinds.index(offset) for offset in offsets]
        yf = np.zeros((reach + wide, 2 * wide))
        re, im = slice(reach, reach + grid), slice(reach + grid, reach + period)
        yf[re, :period], yf[re, wide : wide + period] = yc, -ys
        yf[im, :period], yf[im, wide : wide + period] = ys, yc
        yi = np.zeros((len(self.pair_kinds), 2 * wide, wide))
        for n, offset in enumerate(self.pair_kinds):
            re, im = slice(offset, offset + grid), slice(offset + grid, offset + period)
            yi[n, :period, re], yi[n, :period, im] = yc.T / period, ys.T / period
            yi[n, wide : wide + period, re] = -ys.T / period
            yi[n, wide : wide + period, im] = yc.T / period
        row = [
            (c, s * self.planes + x)
            for x in range(self.planes)
            for c in range(2)
            for s in range(self.slabs)
        ]
        side = np.array([r[0] for r in row])
        cos, sin = self.wave(np.arange(period), np.array([r[1] for r in row]))
        xf = np.concatenate([np.where(side == 0, cos, sin), np.where(side == 0, -sin, cos)])
        xi = np.concatenate([np.where(side == 0, cos, sin), np.where(side == 0, -sin, cos)])
        return {
            "zf": halves(zf),
            "zi": halves(zi),
            "yf": halves(yf),
            "yi": halves(yi),
            "xf": halves(xf),
            "xi": np.concatenate([halves(xi.T / period)[n] for n in (0, 1, 0)], axis=1),
        }


def mm(left, right):
    return jnp.dot(left, right, preferred_element_type=F32)


def split(value):
    high = value.astype(jnp.bfloat16)
    low = (value - high.astype(F32)).astype(jnp.bfloat16)
    return high, low


def right_mul(value, high, low):
    vh, vl = value
    return mm(vh, high) + mm(vh, low) + mm(vl, high)


def left_mul(high, low, value):
    vh, vl = value
    return mm(high, vh) + mm(low, vh) + mm(high, vl)


def each(count, body, looped):
    if looped and count > 1:
        lax.fori_loop(0, count, lambda n, carry: (body(n), carry)[1], 0)
    else:
        for n in range(count):
            body(n)


def lane_of(value):
    return lax.broadcasted_iota(jnp.int32, value.shape, 1)


def place(tiles, start, dest, index):
    shift = (dest - start) % LANE
    base = index + (start - dest + shift) // LANE
    if shift == 0:
        return tiles[base]
    below, above = (
        pltpu.roll(tiles[n], shift, 1) if 0 <= n < len(tiles) else None for n in (base - 1, base)
    )
    if below is None or above is None:
        return above if below is None else below
    return jnp.where(lane_of(above) < shift, below, above)


def join(first, second, at, index):
    low, high = index * LANE, (index + 1) * LANE
    if at <= low:
        return second(index)
    if at >= high:
        return first(index)
    value = first(index)
    return jnp.where(lane_of(value) < at - low, value, second(index))


NAMES = ("zf", "yf", "xf", "xi", "yi", "zi")


def core(plan, mask, *refs):
    occ_ref, orb_hbm, kern_hbm, *table_hbm = refs[:9]
    out_hbm = refs[9]
    raw, flat, zf, yf, xf, xi, yi, zi = refs[10:18]
    bank, terms, back, cube, turned, going, coming, leaving, landing, lines = refs[18:28]
    load_sem, zs, zr, fs, fr, bs, br, rs, rr, put_sem = refs[28:]
    slabs, parts, planes, period = plan.slabs, plan.parts, plan.planes, plan.period
    grid, quads, fold, wide, tiles = plan.grid, plan.quads, plan.fold, plan.wide, plan.tiles
    columns = plan.columns

    loads = [
        pltpu.make_async_copy(source, dest, load_sem.at[n])
        for n, (source, dest) in enumerate(
            zip([orb_hbm, kern_hbm, *table_hbm], [raw, flat, zf, yf, xf, xi, yi, zi])
        )
    ]
    loads[0].start()

    me = lax.axis_index("slab")
    g = lax.axis_index("grp")
    top = 1 << (mask.bit_length() - 1)
    quad = mask % 2 == 0
    owner = (g % 2) == ((g // top) % 2 if quad else 0)
    helper = jnp.logical_not(owner)
    mate = 1 if quad else mask
    steps = sorted(range(1, slabs), key=lambda step: -step)
    others = sorted({mate, mask, mask ^ 1} if quad else {mask})
    barrier = pltpu.get_barrier_semaphore()
    mesh_id = pl.DeviceIdType.MESH
    for other in others:
        pl.semaphore_signal(barrier, 1, device_id={"grp": g ^ other}, device_id_type=mesh_id)
    for step in steps:
        pl.semaphore_signal(barrier, 1, device_id={"slab": me ^ step}, device_id_type=mesh_id)

    def hop(source, dest, send_sem, recv_sem, other):
        return pltpu.make_async_remote_copy(
            src_ref=source,
            dst_ref=dest,
            send_sem=send_sem,
            recv_sem=recv_sem,
            device_id={"grp": g ^ other},
            device_id_type=mesh_id,
        )

    per = plan.per
    even = planes % per == 0
    last_chunk, last_part = plan.chunks - 1, parts - 1

    def aligned(start, size):
        return pl.ds(start if isinstance(start, int) else pl.multiple_of(start, SUB), size)

    def block(chunk):
        return aligned(chunk * (per * quads), plan.sizes(chunk) * quads)

    def when(condition, act):
        if isinstance(condition, bool):
            if condition:
                act()
        else:
            pl.when(condition)(act)

    def ahead(chunk, source, slot, other):
        at = block(chunk)
        return hop(bank.at[source, at], bank.at[slot, at], zs.at[0], zr.at[chunk], other)

    def answer(chunk, source, slot, other):
        at = block(chunk)
        return hop(terms.at[source, at], back.at[slot, at], rs.at[0], rr.at[chunk], other)

    def await_bytes(ref, sem):
        pltpu.make_async_copy(ref, ref, sem).wait()

    def sends_ahead(chunk):
        mine = [ahead(chunk, 0, 2, mate), ahead(chunk, 1, 3, mate)]
        theirs = [ahead(chunk, 0, 4, mask)] + ([ahead(chunk, 1, 4, mask ^ 1)] if quad else [])
        return mine, theirs

    crossing = False

    def sends_ahead_now(chunk):
        mine, theirs = sends_ahead(chunk)
        return mine, ([] if crossing else theirs)

    def sends_ahead_later(chunk):
        if not crossing:
            return

        @pl.when(helper)
        def _():
            when(chunk >= LATER, lambda: ahead(chunk - LATER, 0, 4, mask).start())

            def others_left():
                for n in range(max(0, plan.chunks - LATER), plan.chunks):
                    ahead(n, 0, 4, mask).start()

            when(chunk == last_chunk, others_left)

    def sends_back(chunk):
        mine = [answer(chunk, 2, 0, mask)]
        theirs = [answer(chunk, 0, 0, mate), answer(chunk, 1, 1, mate)]
        return mine, theirs + ([answer(chunk, 2, 1, mask ^ 1)] if quad else [])

    def both(pair, act):
        for role, copies in zip((owner, helper), pair):

            @pl.when(role)
            def _(copies=copies):
                for copy in copies:
                    act(copy)

    every = slice(None)
    ways = ((going, coming, fs, fr), (leaving, landing, bs, br))

    def whole(chunk):
        return 0, chunk, every, chunk

    def tail(part):
        return 0, last_chunk, part, last_chunk + part

    early_chunks = [max(1, plan.chunks * EARLY[min(p, 1)] // 6) for p in range(last_part)]
    kept = [sum(chunk < count for count in early_chunks) for chunk in range(plan.chunks)]

    def early(part, count):
        return 1, slice(0, count), part, part

    def late(chunk, done):
        return 1, chunk, slice(done, parts), last_part + chunk

    hold = last_chunk - 1
    held = (0, hold, 0, hold), (0, hold, slice(1, parts), last_chunk + parts)
    def with_kept(chunk, act):
        for done in sorted(set(kept)):
            own = [n for n in range(plan.chunks) if kept[n] == done]
            if isinstance(chunk, int):
                if chunk in own:
                    act(late(chunk, done))
            else:
                inside = jnp.logical_and(chunk >= own[0], chunk <= own[-1])
                pl.when(inside)(lambda done=done: act(late(chunk, done)))

    def spread(piece, step):
        way, chunk, part, sem = piece
        source, dest, ss, sr = ways[way]
        peer = me ^ step
        return pltpu.make_async_remote_copy(
            src_ref=source.at[chunk, part, peer],
            dst_ref=dest.at[chunk, part, me],
            send_sem=ss.at[0],
            recv_sem=sr.at[sem],
            device_id={"slab": peer},
            device_id_type=mesh_id,
        )

    def spread_out(piece):
        for step in steps:
            spread(piece, step).start()
        way, chunk, part, _ = piece
        source, dest = ways[way][:2]
        dest[chunk, part, pl.ds(me, 1)] = source[chunk, part, pl.ds(me, 1)]

    def spread_in(piece):
        way, chunk, part, sem = piece
        _, dest, _, sr = ways[way]
        await_bytes(dest.at[chunk, part, 0 : slabs - 1], sr.at[sem])

    scale = [jnp.sqrt(0.25 * jnp.full((1, LANE), occ_ref[i], jnp.int32).astype(F32)) for i in range(2)]

    def cells(x, i, r):
        return pl.ds((x * quads * tiles + r) * 2 + i, quads, stride=2 * tiles)

    with jax.named_scope("w_raw"):
        loads[0].wait()

    def own_chunk(chunk):
        for n in range(plan.sizes(chunk)):
            x = chunk * per + n
            for i in range(2):
                for r in range(tiles):
                    bank[i, aligned(x * quads, quads), r * LANE : (r + 1) * LANE] = (
                        raw[cells(x, i, r), :] * scale[i]
                    )

        def meet():
            with jax.named_scope("w_barrier"):
                pl.semaphore_wait(barrier, len(others) + len(steps))

        when(chunk == 0, meet)
        both(sends_ahead_now(chunk), lambda copy: copy.start())

    own_chunk(0)
    for load in loads[1:]:
        load.start()
    for chunk in range(1, plan.chunks):
        own_chunk(chunk)

    with jax.named_scope("w_kern"):
        loads[1].wait()
    pairs = period // 2
    pitch = 2 * period // LANE
    if plan.freqs % SUB == 0:
        unit = SUB
        plane_start = lambda k: k // SUB * (period * period // LANE * SUB) + k % SUB
    else:
        unit = plan.freqs
        plane_start = lambda k: k

    def cube_side(k, side):
        first = plane_start(k)
        got = [flat[pl.ds(first + m * unit, pairs, stride=pitch * unit), :] for m in range(pitch)]
        n = pitch // 2
        swapped = [pltpu.roll(v, LANE // 2, 1) for v in got[n:]]
        spare = jnp.zeros((wide - period, LANE), F32)
        result = []
        for t in range(n + 1):
            odd = swapped[t]
            if t < n:
                odd = jnp.where(lane_of(odd) < LANE // 2, odd, swapped[t + 1])
            rows = [got[t], odd, spare] if side == 0 else [spare, got[t], odd]
            result.append(jnp.concatenate(rows, axis=0).T[: min(LANE, period - t * LANE)])
        return result

    def cube_pair(pair, carry):
        low, high = cube_side(2 * pair, 0), cube_side(2 * pair + 1, 1)
        meet = period // LANE * LANE
        for t, (one, two) in enumerate(zip(low, high)):
            rows = slice(t * LANE, t * LANE + one.shape[0])
            cube[pair, rows, :meet] = one[:, :meet]
            cube[pair, rows, meet:wide] = one[:, meet:] + two[:, :LANE]
            cube[pair, rows, wide:] = two[:, LANE:]
        return carry

    with jax.named_scope("p_cube"):
        lax.fori_loop(0, plan.freqs // 2, cube_pair, 0)

    left = [jnp.where(owner, i, 2 + i) for i in range(2)]
    right = jnp.where(owner, 4, 4 if quad else 1)
    for load in loads[2:]:
        load.wait()

    share = LANE // (slabs * SUB)

    def forward_z(chunk):
        with jax.named_scope("w_ahead"):
            at = block(chunk)
            pl.when(owner)(lambda: await_bytes(bank.at[4, at], zr.at[chunk]))
            heard = bank.at[2:5, at] if quad else bank.at[2:4, at]
            pl.when(helper)(lambda: await_bytes(heard, zr.at[chunk]))
        sends_ahead_later(chunk)
        at, count = block(chunk), plan.sizes(chunk)
        partner = bank[right, at]
        densities = [bank[left[i], at] * partner for i in range(2)]
        if count < per:
            turned[count * period :, :] = jnp.zeros(((per - count) * period, columns), F32)
        fields = []
        for j in range(fold):
            one, two = ([d[:, t * LANE : (t + 1) * LANE] for t in range(tiles)] for d in densities)
            fields.append(
                jnp.concatenate(
                    [
                        join(
                            lambda n: place(one, j * grid, 0, n),
                            lambda n: place(two, j * grid, grid, n),
                            grid,
                            n,
                        )
                        for n in range(wide // LANE)
                    ],
                    axis=1,
                )
            )
        total = right_mul(split(jnp.concatenate(fields, axis=0)), zf[0], zf[1])
        for j in range(fold):
            for x in range(count):
                for c in range(2):
                    first = x * period + c * grid + j * quads
                    row = (j * count + x) * quads
                    turned[first : first + quads, :] = total[
                        row : row + quads, c * columns : (c + 1) * columns
                    ]
        for col in range(0, columns, LANE):
            for r in range(0, plan.lanes, LANE):
                flip = turned[r : r + LANE, col : col + LANE].T.reshape(share, slabs, SUB, LANE)
                for n in range(min(share, parts - col // LANE * share)):
                    going[chunk, col // LANE * share + n, :, :, r : r + LANE] = flip[n]

        def by_part():
            spread_out(tail(0))
            spread_out(held[1])
            each(last_part, lambda part: spread_out(tail(part + 1)), True)

        when(chunk < hold, lambda: spread_out(whole(chunk)))
        when(chunk == hold, lambda: spread_out(held[0]))
        when(chunk == last_chunk, by_part)

    each(plan.chunks, forward_z, even)

    size = slabs * SUB
    halves_of = range(wide // LANE)

    def line(part, x, c):
        return aligned(part * plan.line_rows + (x * 2 + c) * size, size)

    def forward_y(some_chunks, some):
        for kind, offset in enumerate(plan.pair_kinds):
            own = [
                (chunk, j, part)
                for chunk in some_chunks
                for j in range(plan.sizes(chunk))
                if plan.pair_kind[j] == kind
                for part in some
            ]
            piece = []
            for chunk, j, part in own:
                lane = slice(plan.pair_starts[j], plan.pair_starts[j] + wide)
                piece.append(coming[chunk, part, :, :, lane].reshape(size, wide))
            slide = plan.pair_kinds[-1] - offset
            rows = slice(slide, slide + wide)
            piece = jnp.concatenate(piece, axis=0) if len(piece) > 1 else piece[0]
            field = right_mul(split(piece), yf[0, rows], yf[1, rows])
            for n, (chunk, j, part) in enumerate(own):
                for c in range(2):
                    for t in halves_of:
                        spot = c * wide + t * LANE
                        lines[t, line(part, chunk * per + j, c), :] = field[
                            n * size : (n + 1) * size, spot : spot + LANE
                        ]

    def some_planes(part, k, count):
        rows = [
            pl.ds(part * plan.line_rows + k + n, planes * 2 * slabs, stride=SUB)
            for n in range(count)
        ]
        two_planes = 2 * period // LANE
        field = []
        for n in range(0, count, 2):
            one, two = ([lines[t, r, :] for t in halves_of] for r in rows[n : n + 2])
            field += [
                join(lambda t: one[t], lambda t: place(two, 0, period, t), period, t)
                for t in range(two_planes)
            ]
        pair = (part * SUB + k) // 2
        kernel = []
        for n in range(count // 2):
            kernel += [
                cube[pair + n, :, t * LANE : (t + 1) * LANE] for t in range(two_planes)
            ]
        stretches = []
        for t in range(0, len(field), 2):
            some = jnp.concatenate(kernel[t : t + 2], axis=1)
            spectra = left_mul(xf[0], xf[1], split(jnp.concatenate(field[t : t + 2], axis=1)))
            spectra = [spectra[:period] * some, spectra[period:] * some]
            stretches.append(split(jnp.concatenate(spectra, axis=0)))
        field = []
        for high, low in stretches:
            done = mm(xi[...], jnp.concatenate([high, high, low], axis=0))
            field += [done[:, t : t + LANE] for t in range(0, done.shape[1], LANE)]
        for n, r in enumerate(rows):
            own = field[n // 2 * two_planes : (n // 2 + 1) * two_planes]
            for t in halves_of:
                lines[t, r, :] = own[t] if n % 2 == 0 else place(own, period, 0, t)

    def inverse_y(items):
        total = {}
        for kind in range(len(plan.pair_kinds)):
            own = [
                (part, chunk, j)
                for part, chunk in items
                for j in range(plan.sizes(chunk))
                if plan.pair_kind[j] == kind
            ]
            if not own:
                continue
            field = [
                jnp.concatenate(
                    [
                        lines[t, line(part, chunk * per + j, c), :]
                        for c in range(2)
                        for t in halves_of
                    ],
                    axis=1,
                )
                for part, chunk, j in own
            ]
            field = jnp.concatenate(field, axis=0) if len(field) > 1 else field[0]
            field = right_mul(split(field), yi[0, kind], yi[1, kind])
            for n, (part, chunk, j) in enumerate(own):
                for t in halves_of:
                    spot = (part, chunk, plan.pair_starts[j] // LANE + t)
                    term = field[n * size : (n + 1) * size, t * LANE : (t + 1) * LANE]
                    total[spot] = total[spot] + term if spot in total else term
        for part, chunk in items:
            for t in range(plan.lanes // LANE):
                term = total.get((part, chunk, t))
                if term is None:
                    term = jnp.zeros((size, LANE), F32)
                leaving[chunk, part, :, :, t * LANE : (t + 1) * LANE] = term.reshape(
                    slabs, SUB, LANE
                )

    def y_chunk(chunk):
        with jax.named_scope("w_in0"):
            spread_in(whole(chunk))
        with jax.named_scope("p_y"):
            forward_y([chunk], range(parts))

    def one_part(part):
        with jax.named_scope("w_in0p"):
            when(part == 0, lambda: spread_in(held[0]))
            when(part == 1, lambda: spread_in(held[1]))
            spread_in(tail(part))
        with jax.named_scope("p_y1"):
            forward_y([hold, last_chunk], [part])
        with jax.named_scope("p_x"):
            live = SUB if plan.freqs % SUB == 0 else min(SUB, plan.freqs - part * SUB)
            some_planes(part, 0, live)
        with jax.named_scope("p_yi"):
            for p, count in enumerate(early_chunks):

                def leave(p=p, count=count):
                    inverse_y([(p, chunk) for chunk in range(count)])
                    spread_out(early(p, count))

                when(part == p, leave)

    each(hold, y_chunk, even)
    each(parts, one_part, plan.freqs % SUB == 0)
    with jax.named_scope("p_yl"):
        for first, end in ((0, 1), (1, 3), (3, plan.chunks)):
            some = range(first, min(end, plan.chunks))
            if some:
                inverse_y([(p, chunk) for chunk in some for p in range(kept[chunk], parts)])
                each(len(some), lambda n: with_kept(first + n, spread_out), False)

    def inverse_z(chunk):
        with jax.named_scope("w_in1"):
            with_kept(chunk, spread_in)
        at, count = block(chunk), plan.sizes(chunk)
        for col in range(0, columns, LANE):
            for r in range(0, plan.lanes, LANE):
                got = []
                for n in range(share):
                    part = col // LANE * share + n
                    if part < parts:
                        one = landing[chunk, part, :, :, r : r + LANE].reshape(slabs * SUB, LANE)
                    else:
                        one = jnp.zeros((slabs * SUB, LANE), F32)
                    got.append(one)
                got = jnp.concatenate(got, axis=0) if share > 1 else got[0]
                turned[r : r + LANE, col : col + LANE] = got.T
        rows = []
        for j in range(fold):
            for x in range(count):
                firsts = [x * period + c * grid + j * quads for c in range(2)]
                rows.append(jnp.concatenate([turned[f : f + quads, :] for f in firsts], axis=1))
        total = right_mul(split(jnp.concatenate(rows, axis=0)), zi[0], zi[1])
        strips = [
            [
                total[j * count * quads : (j + 1) * count * quads, t * LANE : (t + 1) * LANE]
                for t in range(wide // LANE)
            ]
            for j in range(fold)
        ]

        def potential(i):
            def strip(j):
                if j == fold - 1:
                    return lambda t: place(strips[j], i * grid, j * grid, t)
                return lambda t: join(
                    lambda t: place(strips[j], i * grid, j * grid, t), strip(j + 1), (j + 1) * grid, t
                )

            return jnp.concatenate([strip(0)(t) for t in range(tiles)], axis=1)

        far = None
        partner = bank[right, at]
        for i in range(2):
            field = potential(i)
            terms[i, at] = field * partner
            term = field * bank[left[i], at]
            far = term if far is None else far + term
        terms[2, at] = far
        both(sends_back(chunk), lambda copy: copy.start())

    with jax.named_scope("w_in1"):
        for part, count in enumerate(early_chunks):
            spread_in(early(part, count))
    each(plan.chunks, inverse_z, even)

    weight = [-1.0 / s for s in scale]

    def result(chunk):
        rows = quads * tiles * 2
        at = aligned(chunk * (per * rows), plan.sizes(chunk) * rows)
        return pltpu.make_async_copy(raw.at[at], out_hbm.at[at], put_sem.at[0])

    def finish(chunk):
        with jax.named_scope("w_back"):
            at = block(chunk)
            pl.when(owner)(lambda: await_bytes(back.at[:, at], rr.at[chunk]))
            heard = back.at[:, at] if quad else back.at[0, at]
            pl.when(helper)(lambda: await_bytes(heard, rr.at[chunk]))

        def put(i, value):
            for n in range(plan.sizes(chunk)):
                for r in range(tiles):
                    raw[cells(chunk * per + n, i, r), :] = (
                        value[n * quads : (n + 1) * quads, r * LANE : (r + 1) * LANE] * weight[i]
                    )

        @pl.when(owner)
        def _():
            for i in range(2):
                put(i, terms[i, block(chunk)] + back[i, block(chunk)])

        @pl.when(helper)
        def _():
            put(0, back[0, block(chunk)])
            put(1, back[1, block(chunk)] if quad else terms[2, block(chunk)])

        result(chunk).start()

    with jax.named_scope("p_drain"):
        pl.when(owner)(lambda: await_bytes(bank.at[0:2], zs.at[0]))
        pl.when(helper)(lambda: await_bytes(bank.at[0:2] if quad else bank.at[0], zs.at[0]))
        for source, sem in ((going, fs), (leaving, bs)):
            await_bytes(source.at[:, :, 0 : slabs - 1], sem.at[0])
    each(plan.chunks, finish, even)
    with jax.named_scope("p_drain2"):
        pl.when(owner)(lambda: await_bytes(terms.at[2], rs.at[0]))
        pl.when(helper)(lambda: await_bytes(terms.at[0:3] if quad else terms.at[0:2], rs.at[0]))
        await_bytes(raw, put_sem.at[0])


def run_core(plan, mask, occupation, orbitals, kernel, tables):
    operands = [orbitals, kernel] + [tables[name] for name in NAMES]
    out = jax.ShapeDtypeStruct(orbitals.shape, F32)
    wire = pltpu.VMEM((plan.chunks, plan.parts, plan.slabs, SUB, plan.lanes), F32)
    dma = pltpu.SemaphoreType.DMA
    return pl.pallas_call(
        lambda *refs: core(plan, mask, *refs),
        out_shape=out,
        in_specs=[pl.BlockSpec(memory_space=pltpu.SMEM)]
        + [pl.BlockSpec(memory_space=pl.ANY)] * len(operands),
        out_specs=pl.BlockSpec(memory_space=pl.ANY),
        scratch_shapes=[pltpu.VMEM(op.shape, op.dtype) for op in operands]
        + [
            pltpu.VMEM((5, plan.rows, plan.group), F32),
            pltpu.VMEM((3, plan.rows, plan.group), F32),
            pltpu.VMEM((2, plan.rows, plan.group), F32),
            pltpu.VMEM((plan.freqs // 2, plan.period, 2 * plan.period), F32),
            pltpu.VMEM((plan.lanes, plan.columns), F32),
            wire,
            wire,
            wire,
            wire,
            pltpu.VMEM((plan.wide // LANE, plan.parts * plan.line_rows, LANE), F32),
            dma((len(operands),)),
            dma((1,)),
            dma((plan.chunks,)),
            dma((1,)),
            dma((plan.chunks + plan.parts,)),
            dma((1,)),
            dma((plan.chunks + plan.parts,)),
            dma((1,)),
            dma((plan.chunks,)),
            dma((1,)),
        ],
        compiler_params=pltpu.CompilerParams(
            collective_id=mask, has_side_effects=True, vmem_limit_bytes=62 * 2**20
        ),
    )(occupation, *operands)


def put_out(value):
    def copy(source, dest, sem):
        move = pltpu.make_async_copy(source, dest, sem.at[0])
        move.start()
        move.wait()

    return pl.pallas_call(
        copy,
        out_shape=jax.ShapeDtypeStruct(value.shape, value.dtype),
        in_specs=[pl.BlockSpec(memory_space=pl.ANY)],
        out_specs=pl.BlockSpec(memory_space=pl.ANY),
        scratch_shapes=[pltpu.SemaphoreType.DMA((1,))],
        compiler_params=pltpu.CompilerParams(vmem_limit_bytes=2 * 2**20),
    )(value)


def local(orbitals, occupation, kernel_hat, pair_mask):
    orbit_count, planes, plane_cells = orbitals.shape
    assert orbit_count == 2 and plane_cells % LANE == 0
    slabs = lax.axis_size("slab")
    groups = lax.axis_size("grp")
    freqs, columns = kernel_hat.shape
    plan = Plan(planes, plane_cells, slabs, freqs)
    tables = {name: jnp.asarray(t) for name, t in plan.tables().items()}
    tiles = plane_cells // LANE
    flat = orbitals.reshape(2, planes, tiles, LANE).transpose(1, 2, 0, 3).reshape(-1, LANE)
    if freqs % SUB == 0:
        kernel = kernel_hat.reshape(freqs // SUB, SUB, columns // LANE, LANE)
        kernel = kernel.transpose(0, 2, 1, 3).reshape(-1, LANE)
    else:
        kernel = kernel_hat.reshape(freqs, columns // LANE, LANE)
        kernel = kernel.transpose(1, 0, 2).reshape(-1, LANE)

    def branch(mask):
        return lambda *args: run_core(plan, mask, *args, tables)

    branches = [branch(mask) for mask in range(1, groups)]
    out = lax.switch(pair_mask[0] - 1, branches, occupation, flat, kernel)
    out = put_out(out)
    return out.reshape(planes, tiles, 2, LANE).transpose(2, 0, 1, 3).reshape(2, planes, plane_cells)


def solution(mesh):
    return jax.shard_map(
        local,
        mesh=mesh,
        in_specs=(P("grp", "slab", None), P("grp"), P("slab", None), P()),
        out_specs=P("grp", "slab", None),
        check_vma=False,
    )
```

```python
import math

import jax
import jax.numpy as jnp
import ml_dtypes
import numpy as np
from jax import lax
from jax.experimental import pallas as pl
from jax.experimental.pallas import tpu as pltpu
from jax.sharding import PartitionSpec as P

LANE = 128
EARLY = (3, 2)
LATER = 3
SUB = 8
F32 = jnp.float32


def halves(table):
    high = table.astype(np.float32).astype(ml_dtypes.bfloat16)
    low = (table - high.astype(np.float64)).astype(ml_dtypes.bfloat16)
    return np.stack([high, low])


def padded(size, unit):
    return -(-size // unit) * unit


class Plan:
    def __init__(self, planes, plane_cells, slabs, freqs):
        self.planes, self.slabs, self.freqs = planes, slabs, freqs
        self.grid = math.isqrt(plane_cells)
        self.period = 2 * self.grid
        self.group = math.lcm(self.grid, LANE)
        self.fold = self.group // self.grid
        self.quads = self.grid // self.fold
        self.tiles = self.group // LANE
        self.rows = planes * self.quads
        self.per = math.lcm(self.period, LANE) // self.period
        self.chunks = -(-planes // self.per)
        self.wide = padded(self.period, LANE)
        self.lanes = self.per * self.period
        self.parts = -(-freqs // SUB)
        self.columns = padded(self.parts * slabs * SUB, LANE)
        self.line_rows = planes * 2 * slabs * SUB
        self.pair_starts = self.windows(self.per, self.period, self.lanes)
        assert self.period % LANE == LANE // 2 and LANE % (slabs * SUB) == 0

    def windows(self, count, step, lanes):
        return [min(j * step // LANE * LANE, lanes - self.wide) for j in range(count)]

    def sizes(self, chunk):
        even = self.planes % self.per == 0
        return self.per if even else min(self.per, self.planes - chunk * self.per)

    def wave(self, left, right):
        angle = 2.0 * math.pi / self.period * (np.outer(left, right) % self.period)
        return np.cos(angle), np.sin(angle)

    def tables(self):
        grid, period, fold, wide = self.grid, self.period, self.fold, self.wide
        columns = self.columns
        freq = np.zeros(columns, int)
        live = np.zeros(columns, bool)
        for n in range(self.parts * self.slabs * SUB):
            part, rest = divmod(n, self.slabs * SUB)
            own = part * SUB + rest % SUB
            freq[n] = rest // SUB * self.freqs + own
            live[n] = own < self.freqs
        cells = np.arange(grid)
        zc, zs = self.wave(cells, np.where(live, freq, 0))
        zc, zs = zc * live, zs * live
        zf = np.zeros((wide, 2 * columns))
        zf[:grid, :columns], zf[:grid, columns:] = zc, -zs
        zf[grid:period, :columns], zf[grid:period, columns:] = zs, zc
        zi = np.zeros((2 * columns, wide))
        zi[:columns, :grid], zi[:columns, grid:period] = zc.T / period, zs.T / period
        zi[columns:, :grid], zi[columns:, grid:period] = -zs.T / period, zc.T / period
        y_order = np.array([fold * q + j for j in range(fold) for q in range(self.quads)])
        ky_order = np.concatenate([np.arange(0, period, 2), np.arange(1, period, 2)])
        yc, ys = self.wave(y_order, ky_order)
        offsets = [j * period - self.pair_starts[j] for j in range(self.per)]
        reach = max(offsets)
        self.pair_slides = [reach - offset for offset in offsets]
        self.pair_kinds = sorted(set(offsets))
        self.pair_kind = [self.pair_kinds.index(offset) for offset in offsets]
        yf = np.zeros((reach + wide, 2 * wide))
        re, im = slice(reach, reach + grid), slice(reach + grid, reach + period)
        yf[re, :period], yf[re, wide : wide + period] = yc, -ys
        yf[im, :period], yf[im, wide : wide + period] = ys, yc
        yi = np.zeros((len(self.pair_kinds), 2 * wide, wide))
        for n, offset in enumerate(self.pair_kinds):
            re, im = slice(offset, offset + grid), slice(offset + grid, offset + period)
            yi[n, :period, re], yi[n, :period, im] = yc.T / period, ys.T / period
            yi[n, wide : wide + period, re] = -ys.T / period
            yi[n, wide : wide + period, im] = yc.T / period
        row = [
            (c, s * self.planes + x)
            for x in range(self.planes)
            for c in range(2)
            for s in range(self.slabs)
        ]
        side = np.array([r[0] for r in row])
        cos, sin = self.wave(np.arange(period), np.array([r[1] for r in row]))
        xf = np.concatenate([np.where(side == 0, cos, sin), np.where(side == 0, -sin, cos)])
        xi = np.concatenate([np.where(side == 0, cos, sin), np.where(side == 0, -sin, cos)])
        return {
            "zf": halves(zf),
            "zi": halves(zi),
            "yf": halves(yf),
            "yi": halves(yi),
            "xf": halves(xf),
            "xi": np.concatenate([halves(xi.T / period)[n] for n in (0, 1, 0)], axis=1),
        }


def mm(left, right):
    return jnp.dot(left, right, preferred_element_type=F32)


def split(value):
    high = value.astype(jnp.bfloat16)
    low = (value - high.astype(F32)).astype(jnp.bfloat16)
    return high, low


def right_mul(value, high, low):
    vh, vl = value
    return mm(vh, high) + mm(vh, low) + mm(vl, high)


def left_mul(high, low, value):
    vh, vl = value
    return mm(high, vh) + mm(low, vh) + mm(high, vl)


def each(count, body, looped):
    if looped and count > 1:
        lax.fori_loop(0, count, lambda n, carry: (body(n), carry)[1], 0)
    else:
        for n in range(count):
            body(n)


def lane_of(value):
    return lax.broadcasted_iota(jnp.int32, value.shape, 1)


def place(tiles, start, dest, index):
    shift = (dest - start) % LANE
    base = index + (start - dest + shift) // LANE
    if shift == 0:
        return tiles[base]
    below, above = (
        pltpu.roll(tiles[n], shift, 1) if 0 <= n < len(tiles) else None for n in (base - 1, base)
    )
    if below is None or above is None:
        return above if below is None else below
    return jnp.where(lane_of(above) < shift, below, above)


def join(first, second, at, index):
    low, high = index * LANE, (index + 1) * LANE
    if at <= low:
        return second(index)
    if at >= high:
        return first(index)
    value = first(index)
    return jnp.where(lane_of(value) < at - low, value, second(index))


NAMES = ("zf", "yf", "xf", "xi", "yi", "zi")


def core(plan, mask, *refs):
    occ_ref, orb_hbm, kern_hbm, *table_hbm = refs[:9]
    out_ref = refs[9]
    raw, flat, zf, yf, xf, xi, yi, zi = refs[10:18]
    bank, terms, back, cube, turned, going, coming, leaving, landing, lines = refs[18:28]
    load_sem, zs, zr, fs, fr, bs, br, rs, rr = refs[28:]
    slabs, parts, planes, period = plan.slabs, plan.parts, plan.planes, plan.period
    grid, quads, fold, wide, tiles = plan.grid, plan.quads, plan.fold, plan.wide, plan.tiles
    columns = plan.columns

    loads = [
        pltpu.make_async_copy(source, dest, load_sem.at[n])
        for n, (source, dest) in enumerate(
            zip([orb_hbm, kern_hbm, *table_hbm], [raw, flat, zf, yf, xf, xi, yi, zi])
        )
    ]
    loads[0].start()

    me = lax.axis_index("slab")
    g = lax.axis_index("grp")
    top = 1 << (mask.bit_length() - 1)
    quad = mask % 2 == 0
    owner = (g % 2) == ((g // top) % 2 if quad else 0)
    helper = jnp.logical_not(owner)
    mate = 1 if quad else mask
    steps = sorted(range(1, slabs), key=lambda step: -step)
    others = sorted({mate, mask, mask ^ 1} if quad else {mask})
    barrier = pltpu.get_barrier_semaphore()
    mesh_id = pl.DeviceIdType.MESH
    for other in others:
        pl.semaphore_signal(barrier, 1, device_id={"grp": g ^ other}, device_id_type=mesh_id)
    for step in steps:
        pl.semaphore_signal(barrier, 1, device_id={"slab": me ^ step}, device_id_type=mesh_id)

    def hop(source, dest, send_sem, recv_sem, other):
        return pltpu.make_async_remote_copy(
            src_ref=source,
            dst_ref=dest,
            send_sem=send_sem,
            recv_sem=recv_sem,
            device_id={"grp": g ^ other},
            device_id_type=mesh_id,
        )

    per = plan.per
    even = planes % per == 0
    last_chunk, last_part = plan.chunks - 1, parts - 1

    def aligned(start, size):
        return pl.ds(start if isinstance(start, int) else pl.multiple_of(start, SUB), size)

    def block(chunk):
        return aligned(chunk * (per * quads), plan.sizes(chunk) * quads)

    def when(condition, act):
        if isinstance(condition, bool):
            if condition:
                act()
        else:
            pl.when(condition)(act)

    def ahead(chunk, source, slot, other):
        at = block(chunk)
        return hop(bank.at[source, at], bank.at[slot, at], zs.at[0], zr.at[chunk], other)

    def answer(chunk, source, slot, other):
        at = block(chunk)
        return hop(terms.at[source, at], back.at[slot, at], rs.at[0], rr.at[chunk], other)

    def await_bytes(ref, sem):
        pltpu.make_async_copy(ref, ref, sem).wait()

    def sends_ahead(chunk):
        mine = [ahead(chunk, 0, 2, mate), ahead(chunk, 1, 3, mate)]
        theirs = [ahead(chunk, 0, 4, mask)] + ([ahead(chunk, 1, 4, mask ^ 1)] if quad else [])
        return mine, theirs

    crossing = False

    def sends_ahead_now(chunk):
        mine, theirs = sends_ahead(chunk)
        return mine, ([] if crossing else theirs)

    def sends_ahead_later(chunk):
        if not crossing:
            return

        @pl.when(helper)
        def _():
            when(chunk >= LATER, lambda: ahead(chunk - LATER, 0, 4, mask).start())

            def others_left():
                for n in range(max(0, plan.chunks - LATER), plan.chunks):
                    ahead(n, 0, 4, mask).start()

            when(chunk == last_chunk, others_left)

    def sends_back(chunk):
        mine = [answer(chunk, 2, 0, mask)]
        theirs = [answer(chunk, 0, 0, mate), answer(chunk, 1, 1, mate)]
        return mine, theirs + ([answer(chunk, 2, 1, mask ^ 1)] if quad else [])

    def both(pair, act):
        for role, copies in zip((owner, helper), pair):

            @pl.when(role)
            def _(copies=copies):
                for copy in copies:
                    act(copy)

    every = slice(None)
    ways = ((going, coming, fs, fr), (leaving, landing, bs, br))

    def whole(chunk):
        return 0, chunk, every, chunk

    def tail(part):
        return 0, last_chunk, part, last_chunk + part

    early_chunks = [max(1, plan.chunks * EARLY[min(p, 1)] // 6) for p in range(last_part)]
    kept = [sum(chunk < count for count in early_chunks) for chunk in range(plan.chunks)]

    def early(part, count):
        return 1, slice(0, count), part, part

    def late(chunk, done):
        return 1, chunk, slice(done, parts), last_part + chunk

    hold = last_chunk - 1
    held = (0, hold, 0, hold), (0, hold, slice(1, parts), last_chunk + parts)
    def with_kept(chunk, act):
        for done in sorted(set(kept)):
            own = [n for n in range(plan.chunks) if kept[n] == done]
            if isinstance(chunk, int):
                if chunk in own:
                    act(late(chunk, done))
            else:
                inside = jnp.logical_and(chunk >= own[0], chunk <= own[-1])
                pl.when(inside)(lambda done=done: act(late(chunk, done)))

    def spread(piece, step):
        way, chunk, part, sem = piece
        source, dest, ss, sr = ways[way]
        peer = me ^ step
        return pltpu.make_async_remote_copy(
            src_ref=source.at[chunk, part, peer],
            dst_ref=dest.at[chunk, part, me],
            send_sem=ss.at[0],
            recv_sem=sr.at[sem],
            device_id={"slab": peer},
            device_id_type=mesh_id,
        )

    def spread_out(piece):
        for step in steps:
            spread(piece, step).start()
        way, chunk, part, _ = piece
        source, dest = ways[way][:2]
        dest[chunk, part, pl.ds(me, 1)] = source[chunk, part, pl.ds(me, 1)]

    def spread_in(piece):
        way, chunk, part, sem = piece
        _, dest, _, sr = ways[way]
        await_bytes(dest.at[chunk, part, 0 : slabs - 1], sr.at[sem])

    scale = [jnp.sqrt(0.25 * jnp.full((1, LANE), occ_ref[i], jnp.int32).astype(F32)) for i in range(2)]

    def cells(x, i, r):
        return pl.ds((x * quads * tiles + r) * 2 + i, quads, stride=2 * tiles)

    with jax.named_scope("w_raw"):
        loads[0].wait()

    def own_chunk(chunk):
        for n in range(plan.sizes(chunk)):
            x = chunk * per + n
            for i in range(2):
                for r in range(tiles):
                    bank[i, aligned(x * quads, quads), r * LANE : (r + 1) * LANE] = (
                        raw[cells(x, i, r), :] * scale[i]
                    )

        def meet():
            with jax.named_scope("w_barrier"):
                pl.semaphore_wait(barrier, len(others) + len(steps))

        when(chunk == 0, meet)
        both(sends_ahead_now(chunk), lambda copy: copy.start())

    own_chunk(0)
    for load in loads[1:]:
        load.start()
    for chunk in range(1, plan.chunks):
        own_chunk(chunk)

    with jax.named_scope("w_kern"):
        loads[1].wait()
    pairs = period // 2
    pitch = 2 * period // LANE
    if plan.freqs % SUB == 0:
        unit = SUB
        plane_start = lambda k: k // SUB * (period * period // LANE * SUB) + k % SUB
    else:
        unit = plan.freqs
        plane_start = lambda k: k

    def cube_side(k, side):
        first = plane_start(k)
        got = [flat[pl.ds(first + m * unit, pairs, stride=pitch * unit), :] for m in range(pitch)]
        n = pitch // 2
        swapped = [pltpu.roll(v, LANE // 2, 1) for v in got[n:]]
        spare = jnp.zeros((wide - period, LANE), F32)
        result = []
        for t in range(n + 1):
            odd = swapped[t]
            if t < n:
                odd = jnp.where(lane_of(odd) < LANE // 2, odd, swapped[t + 1])
            rows = [got[t], odd, spare] if side == 0 else [spare, got[t], odd]
            result.append(jnp.concatenate(rows, axis=0).T[: min(LANE, period - t * LANE)])
        return result

    def cube_pair(pair, carry):
        low, high = cube_side(2 * pair, 0), cube_side(2 * pair + 1, 1)
        meet = period // LANE * LANE
        for t, (one, two) in enumerate(zip(low, high)):
            rows = slice(t * LANE, t * LANE + one.shape[0])
            cube[pair, rows, :meet] = one[:, :meet]
            cube[pair, rows, meet:wide] = one[:, meet:] + two[:, :LANE]
            cube[pair, rows, wide:] = two[:, LANE:]
        return carry

    with jax.named_scope("p_cube"):
        lax.fori_loop(0, plan.freqs // 2, cube_pair, 0)

    left = [jnp.where(owner, i, 2 + i) for i in range(2)]
    right = jnp.where(owner, 4, 4 if quad else 1)
    for load in loads[2:]:
        load.wait()

    share = LANE // (slabs * SUB)

    def forward_z(chunk):
        with jax.named_scope("w_ahead"):
            at = block(chunk)
            pl.when(owner)(lambda: await_bytes(bank.at[4, at], zr.at[chunk]))
            heard = bank.at[2:5, at] if quad else bank.at[2:4, at]
            pl.when(helper)(lambda: await_bytes(heard, zr.at[chunk]))
        sends_ahead_later(chunk)
        at, count = block(chunk), plan.sizes(chunk)
        partner = bank[right, at]
        densities = [bank[left[i], at] * partner for i in range(2)]
        if count < per:
            turned[count * period :, :] = jnp.zeros(((per - count) * period, columns), F32)
        fields = []
        for j in range(fold):
            one, two = ([d[:, t * LANE : (t + 1) * LANE] for t in range(tiles)] for d in densities)
            fields.append(
                jnp.concatenate(
                    [
                        join(
                            lambda n: place(one, j * grid, 0, n),
                            lambda n: place(two, j * grid, grid, n),
                            grid,
                            n,
                        )
                        for n in range(wide // LANE)
                    ],
                    axis=1,
                )
            )
        total = right_mul(split(jnp.concatenate(fields, axis=0)), zf[0], zf[1])
        for j in range(fold):
            for x in range(count):
                for c in range(2):
                    first = x * period + c * grid + j * quads
                    row = (j * count + x) * quads
                    turned[first : first + quads, :] = total[
                        row : row + quads, c * columns : (c + 1) * columns
                    ]
        for col in range(0, columns, LANE):
            for r in range(0, plan.lanes, LANE):
                flip = turned[r : r + LANE, col : col + LANE].T.reshape(share, slabs, SUB, LANE)
                for n in range(min(share, parts - col // LANE * share)):
                    going[chunk, col // LANE * share + n, :, :, r : r + LANE] = flip[n]

        def by_part():
            spread_out(tail(0))
            spread_out(held[1])
            each(last_part, lambda part: spread_out(tail(part + 1)), True)

        when(chunk < hold, lambda: spread_out(whole(chunk)))
        when(chunk == hold, lambda: spread_out(held[0]))
        when(chunk == last_chunk, by_part)

    each(plan.chunks, forward_z, even)

    size = slabs * SUB
    halves_of = range(wide // LANE)

    def line(part, x, c):
        return aligned(part * plan.line_rows + (x * 2 + c) * size, size)

    def forward_y(some_chunks, some):
        for kind, offset in enumerate(plan.pair_kinds):
            own = [
                (chunk, j, part)
                for chunk in some_chunks
                for j in range(plan.sizes(chunk))
                if plan.pair_kind[j] == kind
                for part in some
            ]
            piece = []
            for chunk, j, part in own:
                lane = slice(plan.pair_starts[j], plan.pair_starts[j] + wide)
                piece.append(coming[chunk, part, :, :, lane].reshape(size, wide))
            slide = plan.pair_kinds[-1] - offset
            rows = slice(slide, slide + wide)
            piece = jnp.concatenate(piece, axis=0) if len(piece) > 1 else piece[0]
            field = right_mul(split(piece), yf[0, rows], yf[1, rows])
            for n, (chunk, j, part) in enumerate(own):
                for c in range(2):
                    for t in halves_of:
                        spot = c * wide + t * LANE
                        lines[t, line(part, chunk * per + j, c), :] = field[
                            n * size : (n + 1) * size, spot : spot + LANE
                        ]

    def some_planes(part, k, count):
        rows = [
            pl.ds(part * plan.line_rows + k + n, planes * 2 * slabs, stride=SUB)
            for n in range(count)
        ]
        two_planes = 2 * period // LANE
        field = []
        for n in range(0, count, 2):
            one, two = ([lines[t, r, :] for t in halves_of] for r in rows[n : n + 2])
            field += [
                join(lambda t: one[t], lambda t: place(two, 0, period, t), period, t)
                for t in range(two_planes)
            ]
        pair = (part * SUB + k) // 2
        kernel = []
        for n in range(count // 2):
            kernel += [
                cube[pair + n, :, t * LANE : (t + 1) * LANE] for t in range(two_planes)
            ]
        stretches = []
        for t in range(0, len(field), 2):
            some = jnp.concatenate(kernel[t : t + 2], axis=1)
            spectra = left_mul(xf[0], xf[1], split(jnp.concatenate(field[t : t + 2], axis=1)))
            spectra = [spectra[:period] * some, spectra[period:] * some]
            stretches.append(split(jnp.concatenate(spectra, axis=0)))
        field = []
        for high, low in stretches:
            done = mm(xi[...], jnp.concatenate([high, high, low], axis=0))
            field += [done[:, t : t + LANE] for t in range(0, done.shape[1], LANE)]
        for n, r in enumerate(rows):
            own = field[n // 2 * two_planes : (n // 2 + 1) * two_planes]
            for t in halves_of:
                lines[t, r, :] = own[t] if n % 2 == 0 else place(own, period, 0, t)

    def inverse_y(items):
        total = {}
        for kind in range(len(plan.pair_kinds)):
            own = [
                (part, chunk, j)
                for part, chunk in items
                for j in range(plan.sizes(chunk))
                if plan.pair_kind[j] == kind
            ]
            if not own:
                continue
            field = [
                jnp.concatenate(
                    [
                        lines[t, line(part, chunk * per + j, c), :]
                        for c in range(2)
                        for t in halves_of
                    ],
                    axis=1,
                )
                for part, chunk, j in own
            ]
            field = jnp.concatenate(field, axis=0) if len(field) > 1 else field[0]
            field = right_mul(split(field), yi[0, kind], yi[1, kind])
            for n, (part, chunk, j) in enumerate(own):
                for t in halves_of:
                    spot = (part, chunk, plan.pair_starts[j] // LANE + t)
                    term = field[n * size : (n + 1) * size, t * LANE : (t + 1) * LANE]
                    total[spot] = total[spot] + term if spot in total else term
        for part, chunk in items:
            for t in range(plan.lanes // LANE):
                term = total.get((part, chunk, t))
                if term is None:
                    term = jnp.zeros((size, LANE), F32)
                leaving[chunk, part, :, :, t * LANE : (t + 1) * LANE] = term.reshape(
                    slabs, SUB, LANE
                )

    def y_chunk(chunk):
        with jax.named_scope("w_in0"):
            spread_in(whole(chunk))
        with jax.named_scope("p_y"):
            forward_y([chunk], range(parts))

    def one_part(part):
        with jax.named_scope("w_in0p"):
            when(part == 0, lambda: spread_in(held[0]))
            when(part == 1, lambda: spread_in(held[1]))
            spread_in(tail(part))
        with jax.named_scope("p_y1"):
            forward_y([hold, last_chunk], [part])
        with jax.named_scope("p_x"):
            live = SUB if plan.freqs % SUB == 0 else min(SUB, plan.freqs - part * SUB)
            some_planes(part, 0, live)
        with jax.named_scope("p_yi"):
            for p, count in enumerate(early_chunks):

                def leave(p=p, count=count):
                    inverse_y([(p, chunk) for chunk in range(count)])
                    spread_out(early(p, count))

                when(part == p, leave)

    each(hold, y_chunk, even)
    each(parts, one_part, plan.freqs % SUB == 0)
    with jax.named_scope("p_yl"):
        for first, end in ((0, 1), (1, 3), (3, plan.chunks)):
            some = range(first, min(end, plan.chunks))
            if some:
                inverse_y([(p, chunk) for chunk in some for p in range(kept[chunk], parts)])
                each(len(some), lambda n: with_kept(first + n, spread_out), False)

    def inverse_z(chunk):
        with jax.named_scope("w_in1"):
            with_kept(chunk, spread_in)
        at, count = block(chunk), plan.sizes(chunk)
        for col in range(0, columns, LANE):
            for r in range(0, plan.lanes, LANE):
                got = []
                for n in range(share):
                    part = col // LANE * share + n
                    if part < parts:
                        one = landing[chunk, part, :, :, r : r + LANE].reshape(slabs * SUB, LANE)
                    else:
                        one = jnp.zeros((slabs * SUB, LANE), F32)
                    got.append(one)
                got = jnp.concatenate(got, axis=0) if share > 1 else got[0]
                turned[r : r + LANE, col : col + LANE] = got.T
        rows = []
        for j in range(fold):
            for x in range(count):
                firsts = [x * period + c * grid + j * quads for c in range(2)]
                rows.append(jnp.concatenate([turned[f : f + quads, :] for f in firsts], axis=1))
        total = right_mul(split(jnp.concatenate(rows, axis=0)), zi[0], zi[1])
        strips = [
            [
                total[j * count * quads : (j + 1) * count * quads, t * LANE : (t + 1) * LANE]
                for t in range(wide // LANE)
            ]
            for j in range(fold)
        ]

        def potential(i):
            def strip(j):
                if j == fold - 1:
                    return lambda t: place(strips[j], i * grid, j * grid, t)
                return lambda t: join(
                    lambda t: place(strips[j], i * grid, j * grid, t), strip(j + 1), (j + 1) * grid, t
                )

            return jnp.concatenate([strip(0)(t) for t in range(tiles)], axis=1)

        far = None
        partner = bank[right, at]
        for i in range(2):
            field = potential(i)
            terms[i, at] = field * partner
            term = field * bank[left[i], at]
            far = term if far is None else far + term
        terms[2, at] = far
        both(sends_back(chunk), lambda copy: copy.start())

    with jax.named_scope("w_in1"):
        for part, count in enumerate(early_chunks):
            spread_in(early(part, count))
    each(plan.chunks, inverse_z, even)

    weight = [-1.0 / s for s in scale]

    def finish(chunk):
        with jax.named_scope("w_back"):
            at = block(chunk)
            pl.when(owner)(lambda: await_bytes(back.at[:, at], rr.at[chunk]))
            heard = back.at[:, at] if quad else back.at[0, at]
            pl.when(helper)(lambda: await_bytes(heard, rr.at[chunk]))

        def put(i, value):
            for n in range(plan.sizes(chunk)):
                for r in range(tiles):
                    out_ref[cells(chunk * per + n, i, r), :] = (
                        value[n * quads : (n + 1) * quads, r * LANE : (r + 1) * LANE] * weight[i]
                    )

        @pl.when(owner)
        def _():
            for i in range(2):
                put(i, terms[i, block(chunk)] + back[i, block(chunk)])

        @pl.when(helper)
        def _():
            put(0, back[0, block(chunk)])
            put(1, back[1, block(chunk)] if quad else terms[2, block(chunk)])

    with jax.named_scope("p_drain"):
        pl.when(owner)(lambda: await_bytes(bank.at[0:2], zs.at[0]))
        pl.when(helper)(lambda: await_bytes(bank.at[0:2] if quad else bank.at[0], zs.at[0]))
        for source, sem in ((going, fs), (leaving, bs)):
            await_bytes(source.at[:, :, 0 : slabs - 1], sem.at[0])
    each(plan.chunks, finish, even)
    with jax.named_scope("p_drain2"):
        pl.when(owner)(lambda: await_bytes(terms.at[2], rs.at[0]))
        pl.when(helper)(lambda: await_bytes(terms.at[0:3] if quad else terms.at[0:2], rs.at[0]))


def run_core(plan, mask, occupation, orbitals, kernel, tables):
    operands = [orbitals, kernel] + [tables[name] for name in NAMES]
    out = jax.ShapeDtypeStruct(orbitals.shape, F32)
    wire = pltpu.VMEM((plan.chunks, plan.parts, plan.slabs, SUB, plan.lanes), F32)
    dma = pltpu.SemaphoreType.DMA
    return pl.pallas_call(
        lambda *refs: core(plan, mask, *refs),
        out_shape=out,
        in_specs=[pl.BlockSpec(memory_space=pltpu.SMEM)]
        + [pl.BlockSpec(memory_space=pl.ANY)] * len(operands),
        out_specs=pl.BlockSpec(memory_space=pltpu.VMEM),
        scratch_shapes=[pltpu.VMEM(op.shape, op.dtype) for op in operands]
        + [
            pltpu.VMEM((5, plan.rows, plan.group), F32),
            pltpu.VMEM((3, plan.rows, plan.group), F32),
            pltpu.VMEM((2, plan.rows, plan.group), F32),
            pltpu.VMEM((plan.freqs // 2, plan.period, 2 * plan.period), F32),
            pltpu.VMEM((plan.lanes, plan.columns), F32),
            wire,
            wire,
            wire,
            wire,
            pltpu.VMEM((plan.wide // LANE, plan.parts * plan.line_rows, LANE), F32),
            dma((len(operands),)),
            dma((1,)),
            dma((plan.chunks,)),
            dma((1,)),
            dma((plan.chunks + plan.parts,)),
            dma((1,)),
            dma((plan.chunks + plan.parts,)),
            dma((1,)),
            dma((plan.chunks,)),
        ],
        compiler_params=pltpu.CompilerParams(
            collective_id=mask, has_side_effects=True, vmem_limit_bytes=62 * 2**20
        ),
    )(occupation, *operands)


def put_out(value):
    count = next(n for n in (4, 2, 1) if value.shape[0] % (n * SUB) == 0)

    def copy(source, dest, sem):
        step = value.shape[0] // count
        moves = [
            pltpu.make_async_copy(
                source.at[n * step : (n + 1) * step], dest.at[n * step : (n + 1) * step], sem.at[n]
            )
            for n in range(count)
        ]
        for move in moves:
            move.start()
        for move in moves:
            move.wait()

    return pl.pallas_call(
        copy,
        out_shape=jax.ShapeDtypeStruct(value.shape, value.dtype),
        in_specs=[pl.BlockSpec(memory_space=pl.ANY)],
        out_specs=pl.BlockSpec(memory_space=pl.ANY),
        scratch_shapes=[pltpu.SemaphoreType.DMA((count,))],
        compiler_params=pltpu.CompilerParams(vmem_limit_bytes=2 * 2**20),
    )(value)


def local(orbitals, occupation, kernel_hat, pair_mask):
    orbit_count, planes, plane_cells = orbitals.shape
    assert orbit_count == 2 and plane_cells % LANE == 0
    slabs = lax.axis_size("slab")
    groups = lax.axis_size("grp")
    freqs, columns = kernel_hat.shape
    plan = Plan(planes, plane_cells, slabs, freqs)
    tables = {name: jnp.asarray(t) for name, t in plan.tables().items()}
    tiles = plane_cells // LANE
    flat = orbitals.reshape(2, planes, tiles, LANE).transpose(1, 2, 0, 3).reshape(-1, LANE)
    if freqs % SUB == 0:
        kernel = kernel_hat.reshape(freqs // SUB, SUB, columns // LANE, LANE)
        kernel = kernel.transpose(0, 2, 1, 3).reshape(-1, LANE)
    else:
        kernel = kernel_hat.reshape(freqs, columns // LANE, LANE)
        kernel = kernel.transpose(1, 0, 2).reshape(-1, LANE)

    def branch(mask):
        return lambda *args: run_core(plan, mask, *args, tables)

    branches = [branch(mask) for mask in range(1, groups)]
    out = lax.switch(pair_mask[0] - 1, branches, occupation, flat, kernel)
    out = put_out(out)
    return out.reshape(planes, tiles, 2, LANE).transpose(2, 0, 1, 3).reshape(2, planes, plane_cells)


def solution(mesh):
    return jax.shard_map(
        local,
        mesh=mesh,
        in_specs=(P("grp", "slab", None), P("grp"), P("slab", None), P()),
        out_specs=P("grp", "slab", None),
        check_vma=False,
    )
```
